64 devices in a mesh: rep: 4 (over x, y), kv: 16 (over z, core).
Axes of the slice: x: 2, y: 2, z: 8, core: 2. Of those that a mesh axis runs over, the one named last changes fastest.
The devices are a block of a 4x4x8 slice.
Arguments:
- embeds: bfloat16 [2, 2048, 2048], P(None, ('rep', 'kv')), parts along dimension 1
- w_query: bfloat16 [2, 2048, 2048], replicated
- w_key: bfloat16 [2, 2048, 256], replicated
- w_value: bfloat16 [2, 2048, 256], replicated
- w_out: bfloat16 [2, 2048, 2048], replicated
- w_up: bfloat16 [2, 2048, 5632], replicated
- w_down: bfloat16 [2, 5632, 2048], replicated
- k_pool: bfloat16 [5120, 2, 64, 4, 64], P(('rep', 'kv')), parts along dimension 0
- v_pool: bfloat16 [5120, 2, 64, 4, 64], P(('rep', 'kv')), parts along dimension 0
- new_table: int32 [2048, 2], P('rep'), parts along dimension 0
- seq_lens: int32 [2048], P('rep'), parts along dimension 0
- mig_src: int32 [64], P('rep'), parts along dimension 0
- mig_dst: int32 [64], P('rep'), parts along dimension 0
Outputs:
- output 1: bfloat16 [2, 2048, 2048], P(None, ('rep', 'kv')), parts along dimension 1
- output 2: bfloat16 [5120, 2, 64, 4, 64], P(('rep', 'kv')), parts along dimension 0
- output 3: bfloat16 [5120, 2, 64, 4, 64], P(('rep', 'kv')), parts along dimension 0
There are 4 independent parts. The reference program is written for one: setup_inputs(seed, part) draws one part's arguments, and reference() takes and returns one part's arrays. A program takes and returns all parts, laid end to end along the dimension named above; an argument that names none is the same for every part.
All inputs are finite; a program needn't handle non-finite values.
Results may differ from the reference program's by a relative error of at most 0.0153616.
Values are sent between devices in bfloat16 or wider.
A program may use at most 768 MiB of HBM per device.

```python
import jax
import jax.numpy as jnp
from jax import lax

D = 2048
HEADS = 32
KV_HEADS = 4
HEAD = 64
FF = 5632
PAGE = 64
LAYERS = 2
GROUP = 16
SEQ_DEV = 32
PAGES_SEQ = 2
MIG = 16
BATCH = GROUP * SEQ_DEV
SLOTS = PAGES_SEQ * SEQ_DEV + MIG


def draw_layout(layout_key):
    key_hot, key_shift, key_perm, key_rank, key_len = jax.random.split(layout_key, 5)
    hot_dev = jax.random.randint(key_hot, (), 0, GROUP)
    alt_dev = (hot_dev + GROUP // 2) % GROUP
    dev_shift = jax.random.randint(key_shift, (), 0, GROUP)
    slot_perm = jax.vmap(lambda sub_key: jax.random.permutation(sub_key, SLOTS))(jax.random.split(key_perm, GROUP))
    seq_ids = jnp.arange(BATCH)[:, None]
    page_ids = jnp.arange(PAGES_SEQ)[None, :]
    home_dev = seq_ids // SEQ_DEV
    base_dev = (home_dev + page_ids + dev_shift) % GROUP
    base_local = slot_perm[base_dev, page_ids * SEQ_DEV + seq_ids % SEQ_DEV]
    new_table = (base_dev * SLOTS + base_local).astype(jnp.int32)
    eligible = (base_dev != hot_dev) & (base_dev != alt_dev)
    is_last = jnp.broadcast_to(page_ids == PAGES_SEQ - 1, (BATCH, PAGES_SEQ))
    total_pages = BATCH * PAGES_SEQ
    rank_ids = jax.random.permutation(key_rank, total_pages).reshape(BATCH, PAGES_SEQ)
    priority = jnp.where(eligible, jnp.where(is_last, 0, total_pages), 2 * total_pages) + rank_ids
    chosen = jnp.argsort(priority.reshape(-1))[:MIG]
    entry_ids = jnp.arange(MIG)
    src_dev = jnp.where(entry_ids % 8 == 7, alt_dev, hot_dev)
    src_local = slot_perm[src_dev, PAGES_SEQ * SEQ_DEV + entry_ids]
    mig_src = (src_dev * SLOTS + src_local).astype(jnp.int32)
    mig_dst = new_table.reshape(-1)[chosen]
    len_offsets = jax.random.randint(key_len, (BATCH,), 0, PAGE - 1)
    len_offsets = len_offsets.at[0].set(PAGE - 2).at[1].set(0)
    seq_lens = ((PAGES_SEQ - 1) * PAGE + len_offsets).astype(jnp.int32)
    return new_table, seq_lens, mig_src, mig_dst


def setup_inputs(seed: int = 0, part: int = 0) -> dict:
    base_key = jax.random.key(seed)
    part_key = jax.random.fold_in(base_key, part)
    w_keys = jax.random.split(base_key, 6)
    p_keys = jax.random.split(part_key, 5)
    new_table, seq_lens, mig_src, mig_dst = draw_layout(p_keys[0])
    embeds = jax.random.normal(p_keys[1], (2, BATCH, D), jnp.float32).astype(jnp.bfloat16)
    out_scale = (PAGES_SEQ / (HEADS * HEAD)) ** 0.5
    w_query = (jax.random.normal(w_keys[0], (LAYERS, D, HEADS * HEAD), jnp.float32) * 0.5 * D ** -0.5).astype(jnp.bfloat16)
    w_key = (jax.random.normal(w_keys[1], (LAYERS, D, KV_HEADS * HEAD), jnp.float32) * D ** -0.5).astype(jnp.bfloat16)
    w_value = (jax.random.normal(w_keys[2], (LAYERS, D, KV_HEADS * HEAD), jnp.float32) * D ** -0.5).astype(jnp.bfloat16)
    w_out = (jax.random.normal(w_keys[3], (LAYERS, HEADS * HEAD, D), jnp.float32) * out_scale).astype(jnp.bfloat16)
    w_up = (jax.random.normal(w_keys[4], (LAYERS, D, FF), jnp.float32) * D ** -0.5).astype(jnp.bfloat16)
    w_down = (jax.random.normal(w_keys[5], (LAYERS, FF, D), jnp.float32) * FF ** -0.5).astype(jnp.bfloat16)
    pool_shape = (GROUP * SLOTS, LAYERS, PAGE, KV_HEADS, HEAD)
    k_pool = jax.random.normal(p_keys[2], pool_shape, jnp.float32).astype(jnp.bfloat16)
    slot_mean = jax.random.normal(p_keys[3], (GROUP * SLOTS, LAYERS, 1, KV_HEADS, HEAD), jnp.float32)
    v_pool = (0.5 * jax.random.normal(p_keys[4], pool_shape, jnp.float32) + slot_mean).astype(jnp.bfloat16)
    return {'embeds': embeds, 'w_query': w_query, 'w_key': w_key, 'w_value': w_value, 'w_out': w_out, 'w_up': w_up, 'w_down': w_down, 'k_pool': k_pool, 'v_pool': v_pool, 'new_table': new_table, 'seq_lens': seq_lens, 'mig_src': mig_src, 'mig_dst': mig_dst}


def attend_all(queries, k_layer, v_layer, new_table, seq_lens, step_idx):
    group_heads = HEADS // KV_HEADS
    positions = jnp.arange(PAGES_SEQ)[:, None] * PAGE + jnp.arange(PAGE)[None, :]

    def one_seq(args):
        q_row, row_slots, seq_len = args
        keys_f = k_layer[row_slots].astype(jnp.float32)
        vals_f = v_layer[row_slots].astype(jnp.float32)
        q_grp = q_row.astype(jnp.float32).reshape(KV_HEADS, group_heads, HEAD)
        scores = jnp.einsum('kgd,pikd->kgpi', q_grp, keys_f) * HEAD ** -0.5
        scores = jnp.where(positions <= seq_len + step_idx, scores, -jnp.inf)
        flat_scores = scores.reshape(KV_HEADS, group_heads, PAGES_SEQ * PAGE)
        probs_f = jax.nn.softmax(flat_scores, axis=-1).reshape(scores.shape)
        attn_f = jnp.einsum('kgpi,pikd->kgd', probs_f, vals_f)
        return attn_f.reshape(HEADS * HEAD).astype(jnp.bfloat16)

    return lax.map(one_seq, (queries, new_table, seq_lens))


def reference(embeds, w_query, w_key, w_value, w_out, w_up, w_down, k_pool, v_pool, new_table, seq_lens, mig_src, mig_dst):
    k_pool = k_pool.at[mig_dst].set(k_pool[mig_src]).at[mig_src].set(0)
    v_pool = v_pool.at[mig_dst].set(v_pool[mig_src]).at[mig_src].set(0)
    batch_rows = embeds.shape[1]
    step_outs = []
    for step_idx in range(2):
        hidden = embeds[step_idx]
        positions = seq_lens + step_idx
        slot_ids = jnp.take_along_axis(new_table, (positions // PAGE)[:, None], axis=1)[:, 0]
        offsets = positions % PAGE
        for layer_idx in range(LAYERS):
            queries = jnp.dot(hidden, w_query[layer_idx], preferred_element_type=jnp.float32).astype(jnp.bfloat16)
            new_keys = jnp.dot(hidden, w_key[layer_idx], preferred_element_type=jnp.float32).astype(jnp.bfloat16).reshape(batch_rows, KV_HEADS, HEAD)
            new_vals = jnp.dot(hidden, w_value[layer_idx], preferred_element_type=jnp.float32).astype(jnp.bfloat16).reshape(batch_rows, KV_HEADS, HEAD)
            k_pool = k_pool.at[slot_ids, layer_idx, offsets].set(new_keys)
            v_pool = v_pool.at[slot_ids, layer_idx, offsets].set(new_vals)
            attn_out = attend_all(queries.reshape(batch_rows, HEADS, HEAD), k_pool[:, layer_idx], v_pool[:, layer_idx], new_table, seq_lens, step_idx)
            hidden = (hidden.astype(jnp.float32) + jnp.dot(attn_out, w_out[layer_idx], preferred_element_type=jnp.float32)).astype(jnp.bfloat16)
            up_proj = jnp.dot(hidden, w_up[layer_idx], preferred_element_type=jnp.float32).astype(jnp.bfloat16)
            act_vals = jax.nn.gelu(up_proj.astype(jnp.float32), approximate=True).astype(jnp.bfloat16)
            hidden = (hidden.astype(jnp.float32) + jnp.dot(act_vals, w_down[layer_idx], preferred_element_type=jnp.float32)).astype(jnp.bfloat16)
        step_outs.append(hidden)
    return jnp.stack(step_outs), k_pool, v_pool
```

```python
import functools

import jax
import jax.numpy as jnp
from jax import lax
from jax.experimental import pallas as pl
from jax.experimental.pallas import tpu as pltpu
from jax.sharding import PartitionSpec as P

MESH = pl.DeviceIdType.MESH
F32 = jnp.float32
BF16 = jnp.bfloat16
NEG = -1e30
HOPS = 4


def dot(a, b):
    return jnp.dot(a, b, preferred_element_type=F32)


def split3(x):
    hi = x.astype(BF16)
    rest = x - hi.astype(F32)
    mid = rest.astype(BF16)
    low = (rest - mid.astype(F32)).astype(BF16)
    return jnp.concatenate([hi, mid, low], axis=0)


def exact_dot(x, onehot):
    rows = x.shape[0]
    out = dot(split3(x), onehot)
    return out[:rows] + out[rows : 2 * rows] + out[2 * rows :]


def takes(way, hop, half):
    return hop < HOPS or way == half


def main_kernel(
    dims,
    x_ref, wq, wk, wv, wo, wu, wd, kp, vp, oh_ref, e0_ref, e1_ref, et_ref, pres_ref, lane_ref,
    y_ref, knew_ref,
    h_all, hsel, wbig, wk_v, wv_v, wo_v, wu_v, kv_v, q_ref, kn_ref, s_ref, oa, ob, a_ref, ms_ref, pd, rd,
    olhs, pf, rf, hm, act,
    ag_send, ag_recv, dd_send, dd_recv, own_send, own_recv, rs_send, rs_recv, x_send, x_recv, f_send, f_recv, m_send, m_recv,
    w_sem,
):
    layers, d_model, ff, chips, seqs, slots, kv_heads, head, page, rep_heads = dims
    lanes = 128
    me = lax.axis_index("kv")
    z = me // 2
    c = lax.rem(me, 2)
    peer = {"kv": z * 2 + 1 - c}
    pair = 2 * seqs
    half_d = d_model // 2
    own_rows = rep_heads * head
    sub = own_rows // 2
    d_cols = 256

    def chip(step):
        return lax.rem(z + step + 2 * chips, chips)

    def ring_to(way):
        return {"kv": 2 * chip(1 if way == 0 else -1) + c}

    barrier = pltpu.get_barrier_semaphore()
    for target in (peer, ring_to(0), ring_to(1)):
        pl.semaphore_signal(barrier, inc=1, device_id=target, device_id_type=MESH)
    pl.semaphore_wait(barrier, 3)

    heads_cols = 2 * rep_heads * head
    ff_half = ff // 2

    def load(name, l):
        src, dst, i = {
            "q": (lambda: wq.at[l], lambda: wbig.at[pl.ds(0, d_model), :], 0),
            "k": (lambda: wk.at[l], lambda: wk_v, 1),
            "v": (lambda: wv.at[l], lambda: wv_v, 2),
            "o": (lambda: wo.at[l, pl.ds(pl.multiple_of(c * heads_cols, heads_cols), heads_cols), :], lambda: wo_v, 3),
            "u": (lambda: wu.at[l, :, pl.ds(pl.multiple_of(c * ff_half, ff_half), ff_half)], lambda: wu_v, 4),
            "d": (lambda: wd.at[l, pl.ds(pl.multiple_of(c * ff_half, ff_half), ff_half), :], lambda: wbig.at[pl.ds(0, ff_half), :], 5),
            "K": (lambda: kp.at[l], lambda: kv_v.at[0], 6),
            "V": (lambda: vp.at[l], lambda: kv_v.at[1], 7),
        }[name]
        return pltpu.make_async_copy(src(), dst(), w_sem.at[i])

    def block(t, zz, cc, half):
        return h_all.at[t, pl.ds(pl.multiple_of(zz * pair + cc * seqs, seqs), seqs), pl.ds(half * half_d, half_d)]

    def ag_copy(t, way, hop, half):
        sgn = 1 if way == 0 else -1
        ref = block(t, chip(-sgn * (hop - 1)), c, half)
        return pltpu.make_async_remote_copy(
            src_ref=ref, dst_ref=ref, send_sem=ag_send.at[t, way, hop - 1, half], recv_sem=ag_recv.at[t, way, hop - 1, half],
            device_id=ring_to(way), device_id_type=MESH)

    def dd_copy(t, way, hop, half):
        sgn = 1 if way == 0 else -1
        ref = block(t, chip(-sgn * hop), c, half)
        return pltpu.make_async_remote_copy(
            src_ref=ref, dst_ref=ref, send_sem=dd_send.at[t, way, hop - 1, half], recv_sem=dd_recv.at[t, way, hop - 1, half],
            device_id=peer, device_id_type=MESH)

    def own_copy(t, half):
        ref = block(t, z, c, half)
        return pltpu.make_async_remote_copy(
            src_ref=ref, dst_ref=ref, send_sem=own_send.at[t, half], recv_sem=own_recv.at[t, half],
            device_id=peer, device_id_type=MESH)

    def ag_start(t):
        for half in range(2):
            for way in range(2):
                ag_copy(t, way, 1, half).start()
        for half in range(2):
            own_copy(t, half).start()

    def ag_hop(t, hop):
        for half in range(2):
            for way in range(2):
                if takes(way, hop, half):
                    ag_copy(t, way, hop, half).wait_recv()
                    if hop < HOPS and takes(way, hop + 1, half):
                        ag_copy(t, way, hop + 1, half).start()
                    dd_copy(t, way, hop, half).start()

    def ag_finish(t):
        for half in range(2):
            own_copy(t, half).wait_recv()
            own_copy(t, half).wait_send()
            for way in range(2):
                for hop in range(1, HOPS + 1):
                    if takes(way, hop, half):
                        dd_copy(t, way, hop, half).wait_recv()
                        dd_copy(t, way, hop, half).wait_send()
                        ag_copy(t, way, hop, half).wait_send()

    def rs_copy(t, way, k, half):
        sgn = 1 if way == 0 else -1
        return pltpu.make_async_remote_copy(
            src_ref=pd.at[t, chip(sgn * k), half], dst_ref=rd.at[t, way, k - 1, half],
            send_sem=rs_send.at[t, way, k - 1, half], recv_sem=rs_recv.at[t, way, k - 1, half],
            device_id=ring_to(way), device_id_type=MESH)

    def merge(t, way, k, half):
        sgn = 1 if way == 0 else -1
        zz = chip(sgn * (k - 1))
        got = rd.at[t, way, k - 1, half]
        mine = pd.at[t, zz, half]
        m1, l1 = got[pl.ds(sub, 8), :], got[pl.ds(sub + 8, 8), :]
        m2, l2 = mine[pl.ds(sub, 8), :], mine[pl.ds(sub + 8, 8), :]
        m = jnp.maximum(m1, m2)
        a1, a2 = jnp.exp(m1 - m), jnp.exp(m2 - m)
        mine[pl.ds(sub, 8), :] = m
        mine[pl.ds(sub + 8, 8), :] = a1 * l1 + a2 * l2
        for i in range(rep_heads // 2):
            r = half * (rep_heads // 2) + i
            at = pl.ds(i * head, head)
            mine[at, :] = a1[r : r + 1] * got[at, :] + a2[r : r + 1] * mine[at, :]

    def rs_start(t):
        for half in range(2):
            for way in range(2):
                rs_copy(t, way, HOPS if takes(way, HOPS, half) else HOPS - 1, half).start()

    def rs_step(t, k):
        for half in range(2):
            for way in range(2):
                if takes(way, k, half):
                    rs_copy(t, way, k, half).wait_recv()
                    merge(t, way, k, half)
                    if k > 1:
                        rs_copy(t, way, k - 1, half).start()

    def rs_finish(t):
        for half in range(2):
            for way in range(2):
                for k in range(1, HOPS + 1):
                    if takes(way, k, half):
                        rs_copy(t, way, k, half).wait_send()

    def select(t):
        def body(nb, _):
            cols = pl.ds(pl.multiple_of(nb * d_cols, d_cols), d_cols)
            hsel[:, cols] = dot(oh_ref[...], h_all[t, :, cols]).astype(BF16)
            return 0

        lax.fori_loop(0, d_model // d_cols, body, 0)

    def turned(w):
        return dot(hsel[...], w).astype(BF16).astype(F32).T

    def project(t):
        per = d_cols // head

        def body(nb, _):
            cols = pl.ds(pl.multiple_of(nb * d_cols, d_cols), d_cols)
            q_ref[pl.ds(nb * per, per)] = turned(wbig[pl.ds(0, d_model), cols]).reshape(per, head, lanes)
            return 0

        lax.fori_loop(0, kv_heads * rep_heads // per, body, 0)
        for i, w in enumerate((wk_v, wv_v)):
            kn_ref[t, i] = turned(w[...])

    def attend(t, kvh):
        rows = pl.ds(pl.multiple_of(kvh * head, head), head)
        live = pl.ds(0, slots)
        scale = head ** -0.5
        owner, which = kvh // 2, lax.rem(kvh, 2)
        out = oa.at[t, owner, which]

        def scores(keys):
            parts = [
                jnp.concatenate(
                    [jnp.sum(q_ref[kvh * rep_heads + h, :, live] * key, axis=0, keepdims=True) for h in range(rep_heads)], axis=0)
                for key in keys
            ]
            return parts

        def qk(pb, _):
            keys = [kv_v[0, pb * 4 + i, rows, :].astype(F32) for i in range(4)]
            for i, part in enumerate(scores(keys)):
                s_ref[pb * 4 + i, :, live] = part
            return 0

        lax.fori_loop(0, page // 4, qk, 0)
        fresh = list(range(t + 1))
        news = scores([kn_ref[i, 0, rows, live] for i in fresh])
        lim = lane_ref[0:1, live]
        has_new = lane_ref[1:2, live] > 0
        news = [jnp.where(has_new, s * scale, NEG) for s in news]
        pos = lax.broadcasted_iota(jnp.int32, (page, rep_heads, slots), 0)
        valid = pos < lim[None]
        old = jnp.where(valid, s_ref[:, :, live] * scale, NEG)
        m = jnp.max(old, axis=0)
        for s in news:
            m = jnp.maximum(m, s)
        probs = jnp.where(valid, jnp.exp(old - m[None]), 0.0)
        s_ref[:, :, live] = probs
        news = [jnp.where(has_new, jnp.exp(s - m), 0.0) for s in news]
        total = jnp.sum(probs, axis=0)
        for p in news:
            total = total + p
        out[pl.ds(own_rows, rep_heads), live] = m
        out[pl.ds(own_rows + 8, rep_heads), live] = total
        vals = [kn_ref[i, 1, rows, live] for i in fresh]
        for h in range(rep_heads):
            acc = news[0][h : h + 1] * vals[0]
            for p, v in zip(news[1:], vals[1:], strict=True):
                acc = acc + p[h : h + 1] * v
            out[pl.ds(h * head, head), live] = acc

        def pv(pb, _):
            vals = [kv_v[1, pb * 4 + i, rows, :].astype(F32) for i in range(4)]
            ps = [s_ref[pb * 4 + i, :, live] for i in range(4)]
            for h in range(rep_heads):
                at = pl.ds(h * head, head)
                acc = out[at, live]
                for p, v in zip(ps, vals, strict=True):
                    acc = acc + p[h : h + 1] * v
                out[at, live] = acc
            return 0

        lax.fori_loop(0, page // 4, pv, 0)

    def exchange(t):
        return pltpu.make_async_remote_copy(
            src_ref=oa.at[t, 1 - c], dst_ref=ob.at[t], send_sem=x_send.at[t], recv_sem=x_recv.at[t],
            device_id=peer, device_id_type=MESH)

    lane = lax.broadcasted_iota(jnp.int32, (1, lanes), 1)
    low_lanes = lane < pair

    def by_chip(parts, put):
        for zp in range(chips // 2):
            a, b = (p[:, zp * lanes : (zp + 1) * lanes] for p in parts)
            put(2 * zp, jnp.where(low_lanes, a, pltpu.roll(b, pair, 1)))
            put(2 * zp + 1, jnp.where(low_lanes, pltpu.roll(a, pair, 1), b))

    def scatter(t):
        both = [e0_ref[...], e1_ref[...]]
        tops, sums = [], []
        for hh in range(2):
            stat = [
                jnp.concatenate([oa[t, c, hh, pl.ds(own_rows + o, 8), :], ob[t, hh, pl.ds(own_rows + o, 8), :]], axis=1)
                for o in (0, 8)
            ]
            tops.append(stat[0])
            sums.append(stat[1])
        dense_m, dense_l = [], []
        for hh in range(2):
            m_page = [jnp.where(pres_ref[i : i + 1, :] > 0, exact_dot(tops[hh], both[i]), NEG) for i in range(2)]
            m_seq = jnp.maximum(m_page[0], m_page[1])
            back = exact_dot(m_seq, et_ref[...])
            a = jnp.exp(jnp.minimum(tops[hh] - back, 0.0))
            a_ref[hh] = a
            dense_m.append(m_seq)
            dense_l.append(exact_dot(sums[hh] * a, e0_ref[...] + e1_ref[...]))
        for dense, at in ((dense_m, sub), (dense_l, sub + 8)):
            def put(zz, v, at=at):
                for half in range(2):
                    pd[t, zz, half, pl.ds(at, 8), :] = v

            by_chip(dense, put)

        def body(i, _):
            half, r = i // (rep_heads // 2), lax.rem(i, rep_heads // 2)
            at = pl.ds(pl.multiple_of(i * head, head), head)
            parts = []
            for hh in range(2):
                o = jnp.concatenate([oa[t, c, hh, at, :], ob[t, hh, at, :]], axis=1)
                parts.append(exact_dot(o * a_ref[hh, pl.ds(i, 1), :], e0_ref[...] + e1_ref[...]))

            def put(zz, v):
                pd[t, zz, half, pl.ds(pl.multiple_of(r * head, head), head), :] = v

            by_chip(parts, put)
            return 0

        lax.fori_loop(0, rep_heads, body, 0)

    def finalize(t):
        for half in range(2):
            mine = pd.at[t, z, half]
            inv = 1.0 / mine[pl.ds(sub + 8, 8), :]
            rows = []
            for i in range(rep_heads // 2):
                r = half * (rep_heads // 2) + i
                rows.append(mine[pl.ds(i * head, head), :] * inv[r : r + 1])
            turned_o = jnp.concatenate(rows, axis=0).T.astype(BF16)
            for hh in range(2):
                olhs[:, pl.ds(hh * own_rows + half * sub, sub)] = turned_o[hh * pair : (hh + 1) * pair]

    def f_copy(t, stage):
        return pltpu.make_async_remote_copy(
            src_ref=pf.at[stage, 1 - c], dst_ref=rf.at[t, stage], send_sem=f_send.at[t, stage], recv_sem=f_recv.at[t, stage],
            device_id=peer, device_id_type=MESH)

    def m_copy(t):
        return pltpu.make_async_remote_copy(
            src_ref=hm.at[t, c], dst_ref=hm.at[t, c], send_sem=m_send.at[t], recv_sem=m_recv.at[t],
            device_id=peer, device_id_type=MESH)

    def own_block(t):
        return pl.ds(pl.multiple_of(z * pair + c * seqs, seqs), seqs)

    def spread(stage, cols, val):
        pf[stage, 0, :, cols] = val[:seqs]
        pf[stage, 1, :, cols] = val[seqs:]

    def out_proj(t):
        def body(nb, _):
            cols = pl.ds(pl.multiple_of(nb * d_cols, d_cols), d_cols)
            spread(0, cols, dot(olhs[...], wo_v[:, cols]))
            return 0

        lax.fori_loop(0, d_model // d_cols, body, 0)
        f_copy(t, 0).start()
        f_copy(t, 0).wait()
        hm[t, c] = (h_all[t, own_block(t), :].astype(F32) + (pf[0, c] + rf[t, 0])).astype(BF16)
        m_copy(t).start()
        m_copy(t).wait()

    def up(t):
        def body(nb, _):
            cols = pl.ds(pl.multiple_of(nb * d_cols, d_cols), d_cols)
            lhs = hm[t].reshape(pair, d_model)
            u = dot(lhs, wu_v[:, cols]).astype(BF16).astype(F32)
            act[:, cols] = jax.nn.gelu(u, approximate=True).astype(BF16)
            return 0

        lax.fori_loop(0, ff_half // d_cols, body, 0)

    def down(t):
        def body(nb, _):
            cols = pl.ds(pl.multiple_of(nb * d_cols, d_cols), d_cols)
            spread(1, cols, dot(act[...], wbig[pl.ds(0, ff_half), cols]))
            return 0

        lax.fori_loop(0, d_model // d_cols, body, 0)
        f_copy(t, 1).start()
        f_copy(t, 1).wait()
        new = (hm[t, c].astype(F32) + (pf[1, c] + rf[t, 1])).astype(BF16)
        h_all[t, own_block(t), :] = new
        y_ref[t] = new

    for name in ("q", "k", "v", "K", "V", "o", "u"):
        load(name, 0).start()
    oa[...] = jnp.zeros_like(oa)
    for t in range(2):
        h_all[t, own_block(t), :] = x_ref[t]
        ag_start(t)

    def layer(l, _):
        more = l + 1 < layers

        def refill(*names):
            @pl.when(more)
            def _():
                for name in names:
                    load(name, l + 1).start()

        for t in range(2):
            for hop in range(1, HOPS + 1):
                ag_hop(t, hop)
            ag_finish(t)
        for name in ("q", "k", "v", "K", "V"):
            load(name, l).wait()
        for t in range(2):
            select(t)
            project(t)
            for i in range(2):
                knew_ref[l, t, i] = kn_ref[t, i].astype(BF16)
            if t == 1:
                load("d", l).start()
                refill("k", "v")

            def heads(kvh, _, t=t):
                attend(t, kvh)
                return 0

            lax.fori_loop(0, kv_heads, heads, 0)
            if t == 1:
                refill("K", "V")
            exchange(t).start()
            exchange(t).wait()
            scatter(t)
            rs_start(t)
        load("o", l).wait()
        load("u", l).wait()
        load("d", l).wait()
        for t in range(2):
            for k in range(HOPS, 0, -1):
                rs_step(t, k)
            rs_finish(t)
            finalize(t)
            out_proj(t)
            if t == 1:
                refill("o")
            up(t)
            if t == 1:
                refill("u")
            down(t)
            if t == 1:
                refill("q")

            @pl.when(more)
            def _(t=t):
                ag_start(t)

        return 0

    lax.fori_loop(0, layers, layer, 0)


def pool_kernel(vec_ref, move_ref, mig_ref, new_ref, pool_ref, out_ref):
    rows, slots = pool_ref.shape[2], pool_ref.shape[3]
    live = slice(0, slots)
    at0, at1, keep = vec_ref[0:1, live], vec_ref[1:2, live], vec_ref[2:3, live] > 0
    base = pl.program_id(1) * pool_ref.shape[1]
    new0, new1 = new_ref[0, 0, 0, :, live].astype(F32), new_ref[0, 1, 0, :, live].astype(F32)
    for i in range(pool_ref.shape[1]):
        moved = lax.dot_general(
            mig_ref[0, :, i * rows : (i + 1) * rows], move_ref[...], (((0,), (0,)), ((), ())), preferred_element_type=F32)
        val = jnp.where(keep, pool_ref[0, i].astype(F32), moved)
        val = jnp.where(at0 == base + i, new0, val)
        val = jnp.where(at1 == base + i, new1, val)
        out_ref[0, i] = val.astype(BF16)


def new_pool(pool, mig, knew, which, vec, move):
    layers, page, rows, slots = pool.shape
    step = 8
    entries = mig.shape[1]
    return pl.pallas_call(
        pool_kernel,
        out_shape=jax.ShapeDtypeStruct(pool.shape, BF16),
        grid=(layers, page // step),
        in_specs=[
            pl.BlockSpec(vec.shape, lambda l, i: (0, 0)),
            pl.BlockSpec(move.shape, lambda l, i: (0, 0)),
            pl.BlockSpec((1, entries, step * rows), lambda l, i: (which, 0, l * (page // step) + i)),
            pl.BlockSpec((1, 2, 1, rows, 128), lambda l, i: (l, 0, which, 0, 0)),
            pl.BlockSpec((1, step, rows, slots), lambda l, i: (l, i, 0, 0)),
        ],
        out_specs=pl.BlockSpec((1, step, rows, slots), lambda l, i: (l, i, 0, 0)),
        compiler_params=pltpu.CompilerParams(dimension_semantics=("arbitrary", "arbitrary"), vmem_limit_bytes=32 << 20),
        name="new_pool",
    )(vec, move, mig, knew, pool)


def slot_tables(table, lens, src, dst, dev, slots, page):
    ids = dev * slots + jnp.arange(slots, dtype=jnp.int32)
    from_src = ids[:, None] == src[None, :]
    is_src = jnp.any(from_src, axis=1)
    is_dst = jnp.any(ids[:, None] == dst[None, :], axis=1)
    target = jnp.where(is_src, jnp.sum(jnp.where(from_src, dst[None, :], 0), axis=1), ids)
    hit = [table[None, :, p] == target[:, None] for p in range(2)]
    live = [h & ~is_dst[:, None] for h in hit]
    return ids, is_src, is_dst, hit, live


def pad_rows(a, rows):
    return jnp.pad(a, ((0, rows - a.shape[0]), (0, 0)))


def solution(mesh):
    devs = mesh.shape["kv"]
    chips = devs // 2
    pool_spec = P(("rep", "kv"))
    tok_spec = P(None, ("rep", "kv"), None)

    def device_fn(embeds, w_query, w_key, w_value, w_out, w_up, w_down, k_pool, v_pool, new_table, seq_lens, mig_src, mig_dst):
        slots, layers, page, kv_heads, head = k_pool.shape
        seqs, d_model = embeds.shape[1:]
        ff = w_up.shape[2]
        rep_heads = w_query.shape[2] // head // kv_heads
        total = seqs * devs
        dev = lax.axis_index("kv")
        peer = dev + 1 - 2 * lax.rem(dev, 2)
        pools = [jnp.transpose(p, (1, 2, 3, 4, 0)).reshape(layers, page, kv_heads * head, slots) for p in (k_pool, v_pool)]

        ids, is_src, is_dst, hit, live = slot_tables(new_table, seq_lens, mig_src, mig_dst, dev, slots, page)
        peer_live = slot_tables(new_table, seq_lens, mig_src, mig_dst, peer, slots, page)[4]
        onehot = pad_rows((hit[0] | hit[1]).astype(BF16), 128)
        e_page = [jnp.concatenate([pad_rows(live[p].astype(BF16), 128), pad_rows(peer_live[p].astype(BF16), 128)]) for p in range(2)]
        e_back = (e_page[0] + e_page[1]).T
        pres = pad_rows(jnp.stack([jnp.sum(e.astype(F32), axis=0) for e in e_page]), 8)
        length = jnp.sum(jnp.where(hit[0] | hit[1], seq_lens[None, :], 0), axis=1)
        first, last = jnp.any(live[0], axis=1), jnp.any(live[1], axis=1)
        limit = jnp.where(first, jnp.minimum(length, page), jnp.where(last, length - page, 0))
        lane_tab = jnp.pad(jnp.stack([limit, last.astype(jnp.int32)]).astype(jnp.int32), ((0, 6), (0, 128 - slots)))
        on_last = jnp.any(hit[1], axis=1) & ~is_src
        at = [jnp.where(on_last, length - page + t, -1) for t in range(2)]
        keep = ~(is_src | is_dst)
        vec = jnp.pad(jnp.stack(at + [keep.astype(jnp.int32)]).astype(jnp.int32), ((0, 5), (0, 128 - slots)))
        move = (mig_dst[:, None] == ids[None, :]).astype(BF16)
        pick = (mig_src[:, None] == ids[None, :]).astype(BF16)

        mig = jnp.stack([
            lax.dot_general(pick, p.reshape(-1, slots), (((1,), (1,)), ((), ())), preferred_element_type=F32).astype(BF16)
            for p in pools
        ])
        mig = lax.psum(mig, "kv")

        dims = (layers, d_model, ff, chips, seqs, slots, kv_heads, head, page, rep_heads)
        own_rows = rep_heads * head
        sub = own_rows // 2
        kv_cols = kv_heads * head
        big = max(d_model, ff // 2)
        vm, dma = pltpu.VMEM, pltpu.SemaphoreType.DMA
        any_spec, vmem_spec = pl.BlockSpec(memory_space=pl.ANY), pl.BlockSpec(memory_space=pltpu.VMEM)
        flops = 2 * layers * 2 * (128 * d_model * (total + heads_all(w_query, kv_cols)) + 64 * d_model * (d_model + ff) * 2)
        y, knew = pl.pallas_call(
            functools.partial(main_kernel, dims),
            out_shape=[
                jax.ShapeDtypeStruct((2, seqs, d_model), BF16),
                jax.ShapeDtypeStruct((layers, 2, 2, kv_cols, 128), BF16),
            ],
            in_specs=[vmem_spec] + [any_spec] * 8 + [vmem_spec] * 6,
            out_specs=[vmem_spec] * 2,
            scratch_shapes=[
                vm((2, total, d_model), BF16),
                vm((128, d_model), BF16),
                vm((big, d_model), BF16),
                vm((d_model, kv_cols), BF16),
                vm((d_model, kv_cols), BF16),
                vm((2 * own_rows, d_model), BF16),
                vm((d_model, ff // 2), BF16),
                vm((2, page, kv_cols, slots), BF16),
                vm((kv_heads * rep_heads, head, 128), F32),
                vm((2, 2, kv_cols, 128), F32),
                vm((page, rep_heads, 128), F32),
                vm((2, 2, 2, own_rows + 16, 128), F32),
                vm((2, 2, own_rows + 16, 128), F32),
                vm((2, rep_heads, 256), F32),
                vm((2, rep_heads, 256), F32),
                vm((2, chips, 2, sub + 16, 128), F32),
                vm((2, 2, HOPS, 2, sub + 16, 128), F32),
                vm((2 * seqs, 2 * own_rows), BF16),
                vm((2, 2, seqs, d_model), F32),
                vm((2, 2, seqs, d_model), F32),
                vm((2, 2, seqs, d_model), BF16),
                vm((2 * seqs, ff // 2), BF16),
                dma((2, 2, HOPS, 2)), dma((2, 2, HOPS, 2)),
                dma((2, 2, HOPS, 2)), dma((2, 2, HOPS, 2)),
                dma((2, 2)), dma((2, 2)),
                dma((2, 2, HOPS, 2)), dma((2, 2, HOPS, 2)),
                dma((2,)), dma((2,)),
                dma((2, 2)), dma((2, 2)),
                dma((2,)), dma((2,)),
                dma((8,)),
            ],
            compiler_params=pltpu.CompilerParams(collective_id=0, has_side_effects=True, vmem_limit_bytes=67043328),
            cost_estimate=pl.CostEstimate(flops=int(flops), bytes_accessed=int(90e6), transcendentals=0),
            name="decode",
        )(embeds, w_query, w_key, w_value, w_out, w_up, w_down, *pools, onehot, *e_page, e_back, pres, lane_tab)

        outs = [
            jnp.transpose(new_pool(p, mig, knew, i, vec, move).reshape(layers, page, kv_heads, head, slots), (4, 0, 1, 2, 3))
            for i, p in enumerate(pools)
        ]
        return y, outs[0], outs[1]

    def heads_all(w_query, kv_cols):
        return w_query.shape[2] + 2 * kv_cols

    return jax.shard_map(
        device_fn, mesh=mesh,
        in_specs=(tok_spec, P(), P(), P(), P(), P(), P(), pool_spec, pool_spec, P("rep", None), P("rep"), P("rep"), P("rep")),
        out_specs=(tok_spec, pool_spec, pool_spec), check_vma=False)
```

```python
import functools

import jax
import jax.numpy as jnp
from jax import lax
from jax.experimental import pallas as pl
from jax.experimental.pallas import tpu as pltpu
from jax.sharding import PartitionSpec as P

MESH = pl.DeviceIdType.MESH
F32 = jnp.float32
BF16 = jnp.bfloat16
NEG = -1e30
HOPS = 4


def dot(a, b):
    return jnp.dot(a, b, preferred_element_type=F32)


def split3(x):
    hi = x.astype(BF16)
    rest = x - hi.astype(F32)
    mid = rest.astype(BF16)
    low = (rest - mid.astype(F32)).astype(BF16)
    return jnp.concatenate([hi, mid, low], axis=0)


def exact_dot(x, onehot, across=False):
    rows = x.shape[0]
    dims = (((1,), (1 if across else 0,)), ((), ()))
    out = lax.dot_general(split3(x), onehot, dims, preferred_element_type=F32)
    return out[:rows] + out[rows : 2 * rows] + out[2 * rows :]


def sums_to_rows(parts):
    sub = lax.broadcasted_iota(jnp.int32, parts[0].shape, 0)
    for shift in (4, 2, 1):
        half = len(parts) // 2
        high = (sub & shift) != 0
        parts = [
            jnp.where(high, a + pltpu.roll(a, shift, 0), b + pltpu.roll(b, 8 - shift, 0))
            for a, b in zip(parts[half:], parts[:half], strict=True)
        ]
    return parts[0]


def takes(way, hop, half):
    return hop < HOPS or way == half


def main_kernel(
    dims,
    x_ref, wq, wk, wv, wo, wu, wd, kp, vp, oh_ref, e0_ref, e1_ref, es_ref, pres_ref, lane_ref,
    y_ref, knew_ref,
    h_all, hsel, wbig, wk_v, wv_v, wo_v, wu_v, kv_v, q_ref, kn_ref, s_ref, oa, ob, a_ref, ms_ref, pd, rd,
    olhs, pf, rf, hm, act,
    ag_send, ag_recv, dd_send, dd_recv, own_send, own_recv, rs_send, rs_recv, x_send, x_recv, f_send, f_recv, m_send, m_recv,
    w_sem,
):
    layers, d_model, ff, chips, seqs, slots, kv_heads, head, page, rep_heads = dims
    lanes = 128
    me = lax.axis_index("kv")
    z = me // 2
    c = lax.rem(me, 2)
    peer = {"kv": z * 2 + 1 - c}
    pair = 2 * seqs
    half_d = d_model // 2
    own_rows = rep_heads * head
    sub = own_rows // 2
    d_cols = 256

    def chip(step):
        return lax.rem(z + step + 2 * chips, chips)

    def ring_to(way):
        return {"kv": 2 * chip(1 if way == 0 else -1) + c}

    barrier = pltpu.get_barrier_semaphore()
    for target in (peer, ring_to(0), ring_to(1)):
        pl.semaphore_signal(barrier, inc=1, device_id=target, device_id_type=MESH)
    pl.semaphore_wait(barrier, 3)

    heads_cols = 2 * rep_heads * head
    ff_half = ff // 2

    def load(name, l):
        src, dst, i = {
            "q": (lambda: wq.at[l], lambda: wbig.at[pl.ds(0, d_model), :], 0),
            "k": (lambda: wk.at[l], lambda: wk_v, 1),
            "v": (lambda: wv.at[l], lambda: wv_v, 2),
            "o": (lambda: wo.at[l, pl.ds(pl.multiple_of(c * heads_cols, heads_cols), heads_cols), :], lambda: wo_v, 3),
            "u": (lambda: wu.at[l, :, pl.ds(pl.multiple_of(c * ff_half, ff_half), ff_half)], lambda: wu_v, 4),
            "d": (lambda: wd.at[l, pl.ds(pl.multiple_of(c * ff_half, ff_half), ff_half), :], lambda: wbig.at[pl.ds(0, ff_half), :], 5),
            "K": (lambda: kp.at[l], lambda: kv_v.at[0], 6),
            "V": (lambda: vp.at[l], lambda: kv_v.at[1], 7),
        }[name]
        return pltpu.make_async_copy(src(), dst(), w_sem.at[i])

    def block(t, zz, cc, half):
        return h_all.at[t, pl.ds(pl.multiple_of(zz * pair + cc * seqs, seqs), seqs), pl.ds(half * half_d, half_d)]

    def ag_copy(t, way, hop, half):
        sgn = 1 if way == 0 else -1
        ref = block(t, chip(-sgn * (hop - 1)), c, half)
        return pltpu.make_async_remote_copy(
            src_ref=ref, dst_ref=ref, send_sem=ag_send.at[t, way, hop - 1, half], recv_sem=ag_recv.at[t, way, hop - 1, half],
            device_id=ring_to(way), device_id_type=MESH)

    def dd_copy(t, way, hop, half):
        sgn = 1 if way == 0 else -1
        ref = block(t, chip(-sgn * hop), c, half)
        return pltpu.make_async_remote_copy(
            src_ref=ref, dst_ref=ref, send_sem=dd_send.at[t, way, hop - 1, half], recv_sem=dd_recv.at[t, way, hop - 1, half],
            device_id=peer, device_id_type=MESH)

    def own_copy(t, half):
        ref = block(t, z, c, half)
        return pltpu.make_async_remote_copy(
            src_ref=ref, dst_ref=ref, send_sem=own_send.at[t, half], recv_sem=own_recv.at[t, half],
            device_id=peer, device_id_type=MESH)

    def ag_start(t):
        for half in range(2):
            for way in range(2):
                ag_copy(t, way, 1, half).start()
        for half in range(2):
            own_copy(t, half).start()

    def ag_hop(t, hop):
        for half in range(2):
            for way in range(2):
                if takes(way, hop, half):
                    ag_copy(t, way, hop, half).wait_recv()
                    if hop < HOPS and takes(way, hop + 1, half):
                        ag_copy(t, way, hop + 1, half).start()
                    dd_copy(t, way, hop, half).start()

    def ag_finish(t):
        for half in range(2):
            own_copy(t, half).wait_recv()
            own_copy(t, half).wait_send()
            for way in range(2):
                for hop in range(1, HOPS + 1):
                    if takes(way, hop, half):
                        dd_copy(t, way, hop, half).wait_recv()
                        dd_copy(t, way, hop, half).wait_send()
                        ag_copy(t, way, hop, half).wait_send()

    def rs_copy(t, way, k, half):
        sgn = 1 if way == 0 else -1
        return pltpu.make_async_remote_copy(
            src_ref=pd.at[t, chip(sgn * k), half], dst_ref=rd.at[t, way, k - 1, half],
            send_sem=rs_send.at[t, way, k - 1, half], recv_sem=rs_recv.at[t, way, k - 1, half],
            device_id=ring_to(way), device_id_type=MESH)

    def merge(t, way, k, half):
        sgn = 1 if way == 0 else -1
        zz = chip(sgn * (k - 1))
        got = rd.at[t, way, k - 1, half]
        mine = pd.at[t, zz, half]
        m1, l1 = got[pl.ds(sub, 8), :], got[pl.ds(sub + 8, 8), :]
        m2, l2 = mine[pl.ds(sub, 8), :], mine[pl.ds(sub + 8, 8), :]
        m = jnp.maximum(m1, m2)
        a1, a2 = jnp.exp(m1 - m), jnp.exp(m2 - m)
        mine[pl.ds(sub, 8), :] = m
        mine[pl.ds(sub + 8, 8), :] = a1 * l1 + a2 * l2
        for i in range(rep_heads // 2):
            r = half * (rep_heads // 2) + i
            at = pl.ds(i * head, head)
            mine[at, :] = a1[r : r + 1] * got[at, :] + a2[r : r + 1] * mine[at, :]

    def rs_start(t):
        for half in range(2):
            for way in range(2):
                rs_copy(t, way, HOPS if takes(way, HOPS, half) else HOPS - 1, half).start()

    def rs_step(t, k, late):
        for way in range(2):
            half = way if late else 1 - way
            rs_copy(t, way, k, half).wait_recv()
            merge(t, way, k, half)
            if k > 1:
                rs_copy(t, way, k - 1, half).start()

    def rs_finish(t):
        for half in range(2):
            for way in range(2):
                for k in range(1, HOPS + 1):
                    if takes(way, k, half):
                        rs_copy(t, way, k, half).wait_send()

    def select(t):
        def body(nb, _):
            cols = pl.ds(pl.multiple_of(nb * d_cols, d_cols), d_cols)
            hsel[:, cols] = dot(oh_ref[...], h_all[t, :, cols]).astype(BF16)
            return 0

        lax.fori_loop(0, d_model // d_cols, body, 0)

    def turned(w):
        return dot(hsel[...], w).astype(BF16).astype(F32).T

    def project(t):
        per = d_cols // head

        def body(nb, _):
            cols = pl.ds(pl.multiple_of(nb * d_cols, d_cols), d_cols)
            q_ref[pl.ds(nb * per, per)] = turned(wbig[pl.ds(0, d_model), cols]).reshape(per, head, lanes)
            return 0

        lax.fori_loop(0, kv_heads * rep_heads // per, body, 0)
        for i, w in enumerate((wk_v, wv_v)):
            kn_ref[t, i] = turned(w[...])

    def attend(t, kvh):
        rows = pl.ds(pl.multiple_of(kvh * head, head), head)
        live = pl.ds(0, slots)
        scale = head ** -0.5
        owner, which = kvh // 2, lax.rem(kvh, 2)
        out = oa.at[t, owner, which]

        def scores(keys):
            sums = []
            for h in range(rep_heads):
                q = q_ref[kvh * rep_heads + h, :, live]
                sums.append([jnp.sum((q * key).reshape(head // 8, 8, slots), axis=0) for key in keys])
            return [sums_to_rows([part[i] for part in sums]) for i in range(len(keys))]

        def qk(pb, _):
            keys = [kv_v[0, pb * 4 + i, rows, :].astype(F32) for i in range(4)]
            for i, part in enumerate(scores(keys)):
                s_ref[pb * 4 + i, :, live] = part
            return 0

        lax.fori_loop(0, page // 4, qk, 0)
        fresh = list(range(t + 1))
        news = scores([kn_ref[i, 0, rows, live] for i in fresh])
        lim = lane_ref[0:1, live]
        has_new = lane_ref[1:2, live] > 0
        news = [jnp.where(has_new, s * scale, NEG) for s in news]
        pos = lax.broadcasted_iota(jnp.int32, (page, rep_heads, slots), 0)
        valid = pos < lim[None]
        old = jnp.where(valid, s_ref[:, :, live] * scale, NEG)
        m = jnp.max(old, axis=0)
        for s in news:
            m = jnp.maximum(m, s)
        probs = jnp.where(valid, jnp.exp(old - m[None]), 0.0)
        s_ref[:, :, live] = probs
        news = [jnp.where(has_new, jnp.exp(s - m), 0.0) for s in news]
        total = jnp.sum(probs, axis=0)
        for p in news:
            total = total + p
        out[pl.ds(own_rows, rep_heads), live] = m
        out[pl.ds(own_rows + 8, rep_heads), live] = total
        vals = [kn_ref[i, 1, rows, live] for i in fresh]
        for h in range(rep_heads):
            acc = news[0][h : h + 1] * vals[0]
            for p, v in zip(news[1:], vals[1:], strict=True):
                acc = acc + p[h : h + 1] * v
            out[pl.ds(h * head, head), live] = acc

        def pv(pb, _):
            vals = [kv_v[1, pb * 4 + i, rows, :].astype(F32) for i in range(4)]
            ps = [s_ref[pb * 4 + i, :, live] for i in range(4)]
            for h in range(rep_heads):
                at = pl.ds(h * head, head)
                acc = out[at, live]
                for p, v in zip(ps, vals, strict=True):
                    acc = acc + p[h : h + 1] * v
                out[at, live] = acc
            return 0

        lax.fori_loop(0, page // 4, pv, 0)

    def exchange(t):
        return pltpu.make_async_remote_copy(
            src_ref=oa.at[t, 1 - c], dst_ref=ob.at[t], send_sem=x_send.at[t], recv_sem=x_recv.at[t],
            device_id=peer, device_id_type=MESH)

    lane = lax.broadcasted_iota(jnp.int32, (1, lanes), 1)
    low_lanes = lane < pair

    def by_chip(parts, put):
        for zp in range(chips // 2):
            a, b = (p[:, zp * lanes : (zp + 1) * lanes] for p in parts)
            put(2 * zp, jnp.where(low_lanes, a, pltpu.roll(b, pair, 1)))
            put(2 * zp + 1, jnp.where(low_lanes, pltpu.roll(a, pair, 1), b))

    def scatter(t):
        both = [e0_ref[...], e1_ref[...]]
        tops, sums = [], []
        for hh in range(2):
            stat = [
                jnp.concatenate([oa[t, c, hh, pl.ds(own_rows + o, 8), :], ob[t, hh, pl.ds(own_rows + o, 8), :]], axis=1)
                for o in (0, 8)
            ]
            tops.append(stat[0])
            sums.append(stat[1])
        dense_m, dense_l = [], []
        for hh in range(2):
            m_page = [jnp.where(pres_ref[i : i + 1, :] > 0, exact_dot(tops[hh], both[i]), NEG) for i in range(2)]
            m_seq = jnp.maximum(m_page[0], m_page[1])
            back = exact_dot(m_seq, es_ref[...], across=True)
            a = jnp.exp(jnp.minimum(tops[hh] - back, 0.0))
            a_ref[hh] = a
            dense_m.append(m_seq)
            dense_l.append(exact_dot(sums[hh] * a, es_ref[...]))
        for dense, at in ((dense_m, sub), (dense_l, sub + 8)):
            def put(zz, v, at=at):
                for half in range(2):
                    pd[t, zz, half, pl.ds(at, 8), :] = v

            by_chip(dense, put)

        def body(i, _):
            half, r = i // (rep_heads // 2), lax.rem(i, rep_heads // 2)
            at = pl.ds(pl.multiple_of(i * head, head), head)
            parts = []
            for hh in range(2):
                o = jnp.concatenate([oa[t, c, hh, at, :], ob[t, hh, at, :]], axis=1)
                parts.append(exact_dot(o * a_ref[hh, pl.ds(i, 1), :], es_ref[...]))

            def put(zz, v):
                pd[t, zz, half, pl.ds(pl.multiple_of(r * head, head), head), :] = v

            by_chip(parts, put)
            return 0

        lax.fori_loop(0, rep_heads, body, 0)

    def finalize(t):
        for half in range(2):
            mine = pd.at[t, z, half]
            inv = 1.0 / mine[pl.ds(sub + 8, 8), :]
            rows = []
            for i in range(rep_heads // 2):
                r = half * (rep_heads // 2) + i
                rows.append(mine[pl.ds(i * head, head), :] * inv[r : r + 1])
            turned_o = jnp.concatenate(rows, axis=0).T.astype(BF16)
            for hh in range(2):
                olhs[:, pl.ds(hh * own_rows + half * sub, sub)] = turned_o[hh * pair : (hh + 1) * pair]

    def f_copy(t, stage):
        return pltpu.make_async_remote_copy(
            src_ref=pf.at[stage, 1 - c], dst_ref=rf.at[t, stage], send_sem=f_send.at[t, stage], recv_sem=f_recv.at[t, stage],
            device_id=peer, device_id_type=MESH)

    def m_copy(t):
        return pltpu.make_async_remote_copy(
            src_ref=hm.at[t, c], dst_ref=hm.at[t, c], send_sem=m_send.at[t], recv_sem=m_recv.at[t],
            device_id=peer, device_id_type=MESH)

    def own_block(t):
        return pl.ds(pl.multiple_of(z * pair + c * seqs, seqs), seqs)

    def spread(stage, cols, val):
        pf[stage, 0, :, cols] = val[:seqs]
        pf[stage, 1, :, cols] = val[seqs:]

    def out_proj(t):
        def body(nb, _):
            cols = pl.ds(pl.multiple_of(nb * d_cols, d_cols), d_cols)
            spread(0, cols, dot(olhs[...], wo_v[:, cols]))
            return 0

        lax.fori_loop(0, d_model // d_cols, body, 0)
        f_copy(t, 0).start()

    def mid(t):
        f_copy(t, 0).wait()
        hm[t, c] = (h_all[t, own_block(t), :].astype(F32) + (pf[0, c] + rf[t, 0])).astype(BF16)
        m_copy(t).start()

    def up(t, halfway):
        def body(nb, _):
            cols = pl.ds(pl.multiple_of(nb * d_cols, d_cols), d_cols)
            lhs = hm[t].reshape(pair, d_model)
            u = dot(lhs, wu_v[:, cols]).astype(BF16).astype(F32)
            act[:, cols] = jax.nn.gelu(u, approximate=True).astype(BF16)

            @pl.when(nb == ff_half // d_cols // 2)
            def _():
                halfway()

            return 0

        m_copy(t).wait()
        lax.fori_loop(0, ff_half // d_cols, body, 0)

    def down(t):
        def body(nb, _):
            cols = pl.ds(pl.multiple_of(nb * d_cols, d_cols), d_cols)
            spread(1, cols, dot(act[...], wbig[pl.ds(0, ff_half), cols]))
            return 0

        lax.fori_loop(0, d_model // d_cols, body, 0)
        f_copy(t, 1).start()

    def new_h(t):
        f_copy(t, 1).wait()
        new = (hm[t, c].astype(F32) + (pf[1, c] + rf[t, 1])).astype(BF16)
        h_all[t, own_block(t), :] = new
        y_ref[t] = new

    def attend_all(t, between):
        mine = kv_heads // 2

        def body(i, _):
            attend(t, jnp.where(i < mine, (1 - c) * mine + i, c * mine + i - mine))

            @pl.when(i == mine - 1)
            def _():
                exchange(t).start()

            for at, work in between.items():
                pl.when(i == at)(work)
            return 0

        lax.fori_loop(0, kv_heads, body, 0)

    for name in ("q", "k", "v", "K", "V", "o", "u"):
        load(name, 0).start()
    h_all[0, own_block(0), :] = x_ref[0]
    ag_start(0)
    h_all[1, own_block(1), :] = x_ref[1]
    oa[...] = jnp.zeros_like(oa)
    ag_hop(0, 1)
    ag_hop(0, 2)
    ag_start(1)
    ag_hop(0, 3)
    ag_hop(0, 4)
    ag_finish(0)

    def layer(l, _):
        more = l + 1 < layers

        def if_more(work, *args):
            @pl.when(more)
            def _():
                work(*args)

        def refill(*names):
            @pl.when(more)
            def _():
                for name in names:
                    load(name, l + 1).start()

        def keep_new(t):
            for i in range(2):
                knew_ref[l, t, i] = kn_ref[t, i].astype(BF16)

        for name in ("q", "k", "v"):
            load(name, l).wait()
        select(0)
        project(0)
        keep_new(0)
        ag_hop(1, 1)
        for name in ("K", "V"):
            load(name, l).wait()
        attend_all(0, {0: lambda: ag_hop(1, 2), 1: lambda: ag_hop(1, 3), 2: lambda: ag_hop(1, 4)})
        exchange(0).wait()
        scatter(0)
        rs_start(0)
        ag_finish(1)
        select(1)
        project(1)
        keep_new(1)
        load("d", l).start()
        refill("k", "v")
        rs_step(0, 4, True)
        attend_all(1, {
            0: lambda: rs_step(0, 3, False), 1: lambda: rs_step(0, 3, True),
            2: lambda: rs_step(0, 2, False), 3: lambda: rs_step(0, 2, True)})
        refill("K", "V")
        exchange(1).wait()
        scatter(1)
        rs_start(1)
        rs_step(0, 1, False)
        rs_step(0, 1, True)
        rs_finish(0)
        load("o", l).wait()
        load("u", l).wait()
        load("d", l).wait()
        finalize(0)
        out_proj(0)
        rs_step(1, 4, True)
        mid(0)
        rs_step(1, 3, False)
        up(0, lambda: rs_step(1, 3, True))
        down(0)
        rs_step(1, 2, False)
        new_h(0)
        if_more(ag_start, 0)
        rs_step(1, 2, True)
        rs_step(1, 1, False)
        if_more(ag_hop, 0, 1)
        rs_step(1, 1, True)
        rs_finish(1)
        finalize(1)
        out_proj(1)
        if_more(ag_hop, 0, 2)
        mid(1)
        refill("o")
        if_more(ag_hop, 0, 3)
        up(1, lambda: if_more(ag_hop, 0, 4))
        refill("u")
        down(1)
        refill("q")
        if_more(ag_finish, 0)
        new_h(1)
        if_more(ag_start, 1)
        return 0

    lax.fori_loop(0, layers, layer, 0)


def pool_kernel(vec_ref, move_ref, mig_ref, new_ref, pool_ref, out_ref):
    rows, slots = pool_ref.shape[2], pool_ref.shape[3]
    live = slice(0, slots)
    at0, at1, keep = vec_ref[0:1, live], vec_ref[1:2, live], vec_ref[2:3, live] > 0
    base = pl.program_id(1) * pool_ref.shape[1]
    new0, new1 = new_ref[0, 0, 0, :, live].astype(F32), new_ref[0, 1, 0, :, live].astype(F32)
    for i in range(pool_ref.shape[1]):
        moved = lax.dot_general(
            mig_ref[0, :, i * rows : (i + 1) * rows], move_ref[...], (((0,), (0,)), ((), ())), preferred_element_type=F32)
        val = jnp.where(keep, pool_ref[0, i].astype(F32), moved)
        val = jnp.where(at0 == base + i, new0, val)
        val = jnp.where(at1 == base + i, new1, val)
        out_ref[0, i] = val.astype(BF16)


def new_pool(pool, mig, knew, which, vec, move):
    layers, page, rows, slots = pool.shape
    step = 8
    entries = mig.shape[1]
    return pl.pallas_call(
        pool_kernel,
        out_shape=jax.ShapeDtypeStruct(pool.shape, BF16),
        grid=(layers, page // step),
        in_specs=[
            pl.BlockSpec(vec.shape, lambda l, i: (0, 0)),
            pl.BlockSpec(move.shape, lambda l, i: (0, 0)),
            pl.BlockSpec((1, entries, step * rows), lambda l, i: (which, 0, l * (page // step) + i)),
            pl.BlockSpec((1, 2, 1, rows, 128), lambda l, i: (l, 0, which, 0, 0)),
            pl.BlockSpec((1, step, rows, slots), lambda l, i: (l, i, 0, 0)),
        ],
        out_specs=pl.BlockSpec((1, step, rows, slots), lambda l, i: (l, i, 0, 0)),
        compiler_params=pltpu.CompilerParams(dimension_semantics=("arbitrary", "arbitrary"), vmem_limit_bytes=67043328),
        name="new_pool",
    )(vec, move, mig, knew, pool)


def slot_tables(table, lens, src, dst, dev, slots, page):
    ids = dev * slots + jnp.arange(slots, dtype=jnp.int32)
    from_src = ids[:, None] == src[None, :]
    is_src = jnp.any(from_src, axis=1)
    is_dst = jnp.any(ids[:, None] == dst[None, :], axis=1)
    target = jnp.where(is_src, jnp.sum(jnp.where(from_src, dst[None, :], 0), axis=1), ids)
    hit = [table[None, :, p] == target[:, None] for p in range(2)]
    live = [h & ~is_dst[:, None] for h in hit]
    return ids, is_src, is_dst, hit, live


def pad_rows(a, rows):
    return jnp.pad(a, ((0, rows - a.shape[0]), (0, 0)))


def solution(mesh):
    devs = mesh.shape["kv"]
    chips = devs // 2
    pool_spec = P(("rep", "kv"))
    tok_spec = P(None, ("rep", "kv"), None)

    def device_fn(embeds, w_query, w_key, w_value, w_out, w_up, w_down, k_pool, v_pool, new_table, seq_lens, mig_src, mig_dst):
        slots, layers, page, kv_heads, head = k_pool.shape
        seqs, d_model = embeds.shape[1:]
        ff = w_up.shape[2]
        rep_heads = w_query.shape[2] // head // kv_heads
        total = seqs * devs
        dev = lax.axis_index("kv")
        peer = dev + 1 - 2 * lax.rem(dev, 2)
        pools = [jnp.transpose(p, (1, 2, 3, 4, 0)).reshape(layers, page, kv_heads * head, slots) for p in (k_pool, v_pool)]

        ids, is_src, is_dst, hit, live = slot_tables(new_table, seq_lens, mig_src, mig_dst, dev, slots, page)
        peer_live = slot_tables(new_table, seq_lens, mig_src, mig_dst, peer, slots, page)[4]
        onehot = pad_rows((hit[0] | hit[1]).astype(BF16), 128)
        e_page = [jnp.concatenate([pad_rows(live[p].astype(BF16), 128), pad_rows(peer_live[p].astype(BF16), 128)]) for p in range(2)]
        e_sum = e_page[0] + e_page[1]
        pres = pad_rows(jnp.stack([jnp.sum(e.astype(F32), axis=0) for e in e_page]), 8)
        length = jnp.sum(jnp.where(hit[0] | hit[1], seq_lens[None, :], 0), axis=1)
        first, last = jnp.any(live[0], axis=1), jnp.any(live[1], axis=1)
        limit = jnp.where(first, jnp.minimum(length, page), jnp.where(last, length - page, 0))
        lane_tab = jnp.pad(jnp.stack([limit, last.astype(jnp.int32)]).astype(jnp.int32), ((0, 6), (0, 128 - slots)))
        on_last = jnp.any(hit[1], axis=1) & ~is_src
        at = [jnp.where(on_last, length - page + t, -1) for t in range(2)]
        keep = ~(is_src | is_dst)
        vec = jnp.pad(jnp.stack(at + [keep.astype(jnp.int32)]).astype(jnp.int32), ((0, 5), (0, 128 - slots)))
        move = (mig_dst[:, None] == ids[None, :]).astype(BF16)
        pick = (mig_src[:, None] == ids[None, :]).astype(BF16)

        mig = jnp.stack([
            lax.dot_general(pick, p.reshape(-1, slots), (((1,), (1,)), ((), ())), preferred_element_type=F32).astype(BF16)
            for p in pools
        ])
        mig = lax.psum(mig, "kv")

        dims = (layers, d_model, ff, chips, seqs, slots, kv_heads, head, page, rep_heads)
        own_rows = rep_heads * head
        sub = own_rows // 2
        kv_cols = kv_heads * head
        big = max(d_model, ff // 2)
        vm, dma = pltpu.VMEM, pltpu.SemaphoreType.DMA
        any_spec, vmem_spec = pl.BlockSpec(memory_space=pl.ANY), pl.BlockSpec(memory_space=pltpu.VMEM)
        flops = 2 * layers * 2 * (128 * d_model * (total + heads_all(w_query, kv_cols)) + 64 * d_model * (d_model + ff) * 2)
        y, knew = pl.pallas_call(
            functools.partial(main_kernel, dims),
            out_shape=[
                jax.ShapeDtypeStruct((2, seqs, d_model), BF16),
                jax.ShapeDtypeStruct((layers, 2, 2, kv_cols, 128), BF16),
            ],
            in_specs=[vmem_spec] + [any_spec] * 8 + [vmem_spec] * 6,
            out_specs=[vmem_spec] * 2,
            scratch_shapes=[
                vm((2, total, d_model), BF16),
                vm((128, d_model), BF16),
                vm((big, d_model), BF16),
                vm((d_model, kv_cols), BF16),
                vm((d_model, kv_cols), BF16),
                vm((2 * own_rows, d_model), BF16),
                vm((d_model, ff // 2), BF16),
                vm((2, page, kv_cols, slots), BF16),
                vm((kv_heads * rep_heads, head, 128), F32),
                vm((2, 2, kv_cols, 128), F32),
                vm((page, rep_heads, 128), F32),
                vm((2, 2, 2, own_rows + 16, 128), F32),
                vm((2, 2, own_rows + 16, 128), F32),
                vm((2, rep_heads, 256), F32),
                vm((2, rep_heads, 256), F32),
                vm((2, chips, 2, sub + 16, 128), F32),
                vm((2, 2, HOPS, 2, sub + 16, 128), F32),
                vm((2 * seqs, 2 * own_rows), BF16),
                vm((2, 2, seqs, d_model), F32),
                vm((2, 2, seqs, d_model), F32),
                vm((2, 2, seqs, d_model), BF16),
                vm((2 * seqs, ff // 2), BF16),
                dma((2, 2, HOPS, 2)), dma((2, 2, HOPS, 2)),
                dma((2, 2, HOPS, 2)), dma((2, 2, HOPS, 2)),
                dma((2, 2)), dma((2, 2)),
                dma((2, 2, HOPS, 2)), dma((2, 2, HOPS, 2)),
                dma((2,)), dma((2,)),
                dma((2, 2)), dma((2, 2)),
                dma((2,)), dma((2,)),
                dma((8,)),
            ],
            compiler_params=pltpu.CompilerParams(collective_id=0, has_side_effects=True, vmem_limit_bytes=67043328),
            cost_estimate=pl.CostEstimate(flops=int(flops), bytes_accessed=int(90e6), transcendentals=0),
            name="decode",
        )(embeds, w_query, w_key, w_value, w_out, w_up, w_down, *pools, onehot, *e_page, e_sum, pres, lane_tab)

        outs = [
            jnp.transpose(new_pool(p, mig, knew, i, vec, move).reshape(layers, page, kv_heads, head, slots), (4, 0, 1, 2, 3))
            for i, p in enumerate(pools)
        ]
        return y, outs[0], outs[1]

    def heads_all(w_query, kv_cols):
        return w_query.shape[2] + 2 * kv_cols

    return jax.shard_map(
        device_fn, mesh=mesh,
        in_specs=(tok_spec, P(), P(), P(), P(), P(), P(), pool_spec, pool_spec, P("rep", None), P("rep"), P("rep"), P("rep")),
        out_specs=(tok_spec, pool_spec, pool_spec), check_vma=False)
```

```python
import functools

import jax
import jax.numpy as jnp
from jax import lax
from jax.experimental import pallas as pl
from jax.experimental.pallas import tpu as pltpu
from jax.sharding import PartitionSpec as P

MESH = pl.DeviceIdType.MESH
F32 = jnp.float32
BF16 = jnp.bfloat16
NEG = -1e30
HOPS = 4


def dot(a, b):
    return jnp.dot(a, b, preferred_element_type=F32)


def split3(x):
    hi = x.astype(BF16)
    rest = x - hi.astype(F32)
    mid = rest.astype(BF16)
    low = (rest - mid.astype(F32)).astype(BF16)
    return jnp.concatenate([hi, mid, low], axis=0)


def exact_dot(x, onehot, across=False):
    rows = x.shape[0]
    dims = (((1,), (1 if across else 0,)), ((), ()))
    out = lax.dot_general(split3(x), onehot, dims, preferred_element_type=F32)
    return out[:rows] + out[rows : 2 * rows] + out[2 * rows :]


def sums_to_rows(parts):
    sub = lax.broadcasted_iota(jnp.int32, parts[0].shape, 0)
    for shift in (4, 2, 1):
        half = len(parts) // 2
        high = (sub & shift) != 0
        parts = [
            jnp.where(high, a + pltpu.roll(a, shift, 0), b + pltpu.roll(b, 8 - shift, 0))
            for a, b in zip(parts[half:], parts[:half], strict=True)
        ]
    return parts[0]


def takes(way, hop, half):
    return hop < HOPS or way == half


def main_kernel(
    dims,
    x_ref, wq, wk, wv, wo, wu, wd, kp, vp, oh_ref, e0_ref, e1_ref, es_ref, pres_ref, lane_ref,
    y_ref, knew_ref,
    h_all, hsel, wbig, wk_v, wv_v, wo_v, wu_v, kv_v, q_ref, kn_ref, s_ref, oa, ob, a_ref, ms_ref, pd, rd,
    olhs, pf, rf, hm, act,
    ag_send, ag_recv, dd_send, dd_recv, own_send, own_recv, rs_send, rs_recv, x_send, x_recv, f_send, f_recv, m_send, m_recv,
    w_sem,
):
    layers, d_model, ff, chips, seqs, slots, kv_heads, head, page, rep_heads = dims
    lanes = 128
    me = lax.axis_index("kv")
    z = me // 2
    c = lax.rem(me, 2)
    peer = {"kv": z * 2 + 1 - c}
    pair = 2 * seqs
    half_d = d_model // 2
    own_rows = rep_heads * head
    sub = own_rows // 2
    d_cols = 512
    s_cols = 1024
    o_cols = 512
    u_cols = ff // 2 // 2

    def chip(step):
        return lax.rem(z + step + 2 * chips, chips)

    def ring_to(way):
        return {"kv": 2 * chip(1 if way == 0 else -1) + c}

    barrier = pltpu.get_barrier_semaphore()
    for target in (peer, ring_to(0), ring_to(1)):
        pl.semaphore_signal(barrier, inc=1, device_id=target, device_id_type=MESH)
    pl.semaphore_wait(barrier, 3)

    heads_cols = 2 * rep_heads * head
    ff_half = ff // 2

    def load(name, l):
        src, dst, i = {
            "q": (lambda: wq.at[l], lambda: wbig.at[pl.ds(0, d_model), :], 0),
            "k": (lambda: wk.at[l], lambda: wk_v, 1),
            "v": (lambda: wv.at[l], lambda: wv_v, 2),
            "o": (lambda: wo.at[l, pl.ds(pl.multiple_of(c * heads_cols, heads_cols), heads_cols), :], lambda: wo_v, 3),
            "u": (lambda: wu.at[l, :, pl.ds(pl.multiple_of(c * ff_half, ff_half), ff_half)], lambda: wu_v, 4),
            "d": (lambda: wd.at[l, pl.ds(pl.multiple_of(c * ff_half, ff_half), ff_half), :], lambda: wbig.at[pl.ds(0, ff_half), :], 5),
            "K": (lambda: kp.at[l], lambda: kv_v.at[0], 6),
            "V": (lambda: vp.at[l], lambda: kv_v.at[1], 7),
        }[name]
        return pltpu.make_async_copy(src(), dst(), w_sem.at[i])

    def block(t, zz, cc, half):
        return h_all.at[t, pl.ds(pl.multiple_of(zz * pair + cc * seqs, seqs), seqs), pl.ds(half * half_d, half_d)]

    def ag_copy(t, way, hop, half):
        sgn = 1 if way == 0 else -1
        ref = block(t, chip(-sgn * (hop - 1)), c, half)
        return pltpu.make_async_remote_copy(
            src_ref=ref, dst_ref=ref, send_sem=ag_send.at[t, way, hop - 1, half], recv_sem=ag_recv.at[t, way, hop - 1, half],
            device_id=ring_to(way), device_id_type=MESH)

    def dd_copy(t, way, hop, half):
        sgn = 1 if way == 0 else -1
        ref = block(t, chip(-sgn * hop), c, half)
        return pltpu.make_async_remote_copy(
            src_ref=ref, dst_ref=ref, send_sem=dd_send.at[t, way, hop - 1, half], recv_sem=dd_recv.at[t, way, hop - 1, half],
            device_id=peer, device_id_type=MESH)

    def own_copy(t, half):
        ref = block(t, z, c, half)
        return pltpu.make_async_remote_copy(
            src_ref=ref, dst_ref=ref, send_sem=own_send.at[t, half], recv_sem=own_recv.at[t, half],
            device_id=peer, device_id_type=MESH)

    def ag_start(t):
        for half in range(2):
            for way in range(2):
                ag_copy(t, way, 1, half).start()
        for half in range(2):
            own_copy(t, half).start()

    def ag_hop(t, hop):
        for half in range(2):
            for way in range(2):
                if takes(way, hop, half):
                    ag_copy(t, way, hop, half).wait_recv()
                    if hop < HOPS and takes(way, hop + 1, half):
                        ag_copy(t, way, hop + 1, half).start()
                    dd_copy(t, way, hop, half).start()

    def ag_finish(t):
        for half in range(2):
            own_copy(t, half).wait_recv()
            own_copy(t, half).wait_send()
            for way in range(2):
                for hop in range(1, HOPS + 1):
                    if takes(way, hop, half):
                        dd_copy(t, way, hop, half).wait_recv()
                        dd_copy(t, way, hop, half).wait_send()
                        ag_copy(t, way, hop, half).wait_send()

    def rs_copy(t, way, k, half):
        sgn = 1 if way == 0 else -1
        return pltpu.make_async_remote_copy(
            src_ref=pd.at[t, chip(sgn * k), half], dst_ref=rd.at[t, way, k - 1, half],
            send_sem=rs_send.at[t, way, k - 1, half], recv_sem=rs_recv.at[t, way, k - 1, half],
            device_id=ring_to(way), device_id_type=MESH)

    def merge(t, way, k, half):
        sgn = 1 if way == 0 else -1
        zz = chip(sgn * (k - 1))
        got = rd.at[t, way, k - 1, half]
        mine = pd.at[t, zz, half]
        m1, l1 = got[pl.ds(sub, 8), :], got[pl.ds(sub + 8, 8), :]
        m2, l2 = mine[pl.ds(sub, 8), :], mine[pl.ds(sub + 8, 8), :]
        m = jnp.maximum(m1, m2)
        a1, a2 = jnp.exp(m1 - m), jnp.exp(m2 - m)
        mine[pl.ds(sub, 8), :] = m
        mine[pl.ds(sub + 8, 8), :] = a1 * l1 + a2 * l2
        for i in range(rep_heads // 2):
            r = half * (rep_heads // 2) + i
            at = pl.ds(i * head, head)
            mine[at, :] = a1[r : r + 1] * got[at, :] + a2[r : r + 1] * mine[at, :]

    def rs_start(t):
        for half in range(2):
            for way in range(2):
                rs_copy(t, way, HOPS if takes(way, HOPS, half) else HOPS - 1, half).start()

    def rs_step(t, k, late):
        for way in range(2):
            half = way if late else 1 - way
            rs_copy(t, way, k, half).wait_recv()
            merge(t, way, k, half)
            if k > 1:
                rs_copy(t, way, k - 1, half).start()

    def rs_finish(t):
        for half in range(2):
            for way in range(2):
                for k in range(1, HOPS + 1):
                    if takes(way, k, half):
                        rs_copy(t, way, k, half).wait_send()

    def select(t):
        def body(nb, _):
            cols = pl.ds(pl.multiple_of(nb * s_cols, s_cols), s_cols)
            hsel[:, cols] = dot(oh_ref[pl.ds(0, slots), :], h_all[t, :, cols]).astype(BF16)
            return 0

        lax.fori_loop(0, d_model // s_cols, body, 0)

    def turned(w):
        rows = dot(hsel[...], w).astype(BF16).astype(F32)
        return jnp.concatenate([rows, jnp.zeros((lanes - slots, rows.shape[1]), F32)], axis=0).T

    def project(t):
        per = d_cols // head

        def body(nb, _):
            cols = pl.ds(pl.multiple_of(nb * d_cols, d_cols), d_cols)
            q_ref[pl.ds(nb * per, per)] = turned(wbig[pl.ds(0, d_model), cols]).reshape(per, head, lanes)
            return 0

        lax.fori_loop(0, kv_heads * rep_heads // per, body, 0)
        for i, w in enumerate((wk_v, wv_v)):
            kn_ref[t, i] = turned(w[...])

    def attend(t, kvh):
        rows = pl.ds(pl.multiple_of(kvh * head, head), head)
        live = pl.ds(0, slots)
        scale = head ** -0.5
        owner, which = kvh // 2, lax.rem(kvh, 2)
        out = oa.at[t, owner, which]

        def scores(keys):
            sums = []
            for h in range(rep_heads):
                q = [q_ref[kvh * rep_heads + h, pl.ds(d, 8), live] for d in range(0, head, 8)]
                parts = []
                for key in keys:
                    acc = q[0] * key[:8]
                    for i in range(1, head // 8):
                        acc = acc + q[i] * key[8 * i : 8 * i + 8]
                    parts.append(acc)
                sums.append(parts)
            return [sums_to_rows([part[i] for part in sums]) for i in range(len(keys))]

        def qk(pb, _):
            keys = [kv_v[0, pb * 4 + i, rows, :].astype(F32) for i in range(4)]
            for i, part in enumerate(scores(keys)):
                s_ref[pb * 4 + i, :, live] = part
            return 0

        lax.fori_loop(0, page // 4, qk, 0)
        fresh = list(range(t + 1))
        news = scores([kn_ref[i, 0, rows, live] for i in fresh])
        lim = lane_ref[0:1, live]
        has_new = lane_ref[1:2, live] > 0
        news = [jnp.where(has_new, s * scale, NEG) for s in news]
        pos = lax.broadcasted_iota(jnp.int32, (page, rep_heads, slots), 0)
        valid = pos < lim[None]
        old = jnp.where(valid, s_ref[:, :, live] * scale, NEG)
        m = jnp.max(old, axis=0)
        for s in news:
            m = jnp.maximum(m, s)
        probs = jnp.where(valid, jnp.exp(old - m[None]), 0.0)
        s_ref[:, :, live] = probs
        news = [jnp.where(has_new, jnp.exp(s - m), 0.0) for s in news]
        total = jnp.sum(probs, axis=0)
        for p in news:
            total = total + p
        out[pl.ds(own_rows, rep_heads), live] = m
        out[pl.ds(own_rows + 8, rep_heads), live] = total
        vals = [kn_ref[i, 1, rows, live] for i in fresh]
        for h in range(rep_heads):
            acc = news[0][h : h + 1] * vals[0]
            for p, v in zip(news[1:], vals[1:], strict=True):
                acc = acc + p[h : h + 1] * v
            out[pl.ds(h * head, head), live] = acc

        def pv(pb, _):
            vals = [kv_v[1, pb * 4 + i, rows, :].astype(F32) for i in range(4)]
            ps = [s_ref[pb * 4 + i, :, live] for i in range(4)]
            for h in range(rep_heads):
                at = pl.ds(h * head, head)
                acc = out[at, live]
                for p, v in zip(ps, vals, strict=True):
                    acc = acc + p[h : h + 1] * v
                out[at, live] = acc
            return 0

        lax.fori_loop(0, page // 4, pv, 0)

    def exchange(t):
        return pltpu.make_async_remote_copy(
            src_ref=oa.at[t, 1 - c], dst_ref=ob.at[t], send_sem=x_send.at[t], recv_sem=x_recv.at[t],
            device_id=peer, device_id_type=MESH)

    lane = lax.broadcasted_iota(jnp.int32, (1, lanes), 1)
    low_lanes = lane < pair

    def by_chip(parts, put):
        for zp in range(chips // 2):
            a, b = (p[:, zp * lanes : (zp + 1) * lanes] for p in parts)
            put(2 * zp, jnp.where(low_lanes, a, pltpu.roll(b, pair, 1)))
            put(2 * zp + 1, jnp.where(low_lanes, pltpu.roll(a, pair, 1), b))

    def scatter(t):
        def stat(o):
            return jnp.concatenate([
                jnp.concatenate([oa[t, c, hh, pl.ds(own_rows + o, 8), :], ob[t, hh, pl.ds(own_rows + o, 8), :]], axis=1)
                for hh in range(2)
            ], axis=0)

        top = stat(0)
        m_page = [jnp.where(pres_ref[i : i + 1, :] > 0, exact_dot(top, e[...]), NEG) for i, e in enumerate((e0_ref, e1_ref))]
        m_seq = jnp.maximum(m_page[0], m_page[1])
        a = jnp.exp(jnp.minimum(top - exact_dot(m_seq, es_ref[...], across=True), 0.0))
        a_ref[0], a_ref[1] = a[:8], a[8:]
        l_seq = exact_dot(stat(8) * a, es_ref[...])
        for dense, at in ((m_seq, sub), (l_seq, sub + 8)):
            def put(zz, v, at=at):
                for half in range(2):
                    pd[t, zz, half, pl.ds(at, 8), :] = v

            by_chip([dense[:8], dense[8:]], put)

        def body(n, _):
            for half in range(2):
                i = half * (rep_heads // 2) + n
                at = pl.ds(pl.multiple_of(i * head, head), head)
                parts = []
                for hh in range(2):
                    o = jnp.concatenate([oa[t, c, hh, at, :], ob[t, hh, at, :]], axis=1)
                    parts.append(exact_dot(o * a_ref[hh, pl.ds(i, 1), :], es_ref[...]))

                def put(zz, v, half=half):
                    pd[t, zz, half, pl.ds(pl.multiple_of(n * head, head), head), :] = v

                by_chip(parts, put)
            return 0

        lax.fori_loop(0, rep_heads // 2, body, 0)

    def finalize(t):
        for half in range(2):
            mine = pd.at[t, z, half]
            inv = 1.0 / mine[pl.ds(sub + 8, 8), :]
            rows = []
            for i in range(rep_heads // 2):
                r = half * (rep_heads // 2) + i
                rows.append(mine[pl.ds(i * head, head), :] * inv[r : r + 1])
            turned_o = jnp.concatenate(rows, axis=0).T.astype(BF16)
            for hh in range(2):
                olhs[:, pl.ds(hh * own_rows + half * sub, sub)] = turned_o[hh * pair : (hh + 1) * pair]

    def f_copy(t, stage):
        return pltpu.make_async_remote_copy(
            src_ref=pf.at[stage, 1 - c], dst_ref=rf.at[t, stage], send_sem=f_send.at[t, stage], recv_sem=f_recv.at[t, stage],
            device_id=peer, device_id_type=MESH)

    def m_copy(t):
        return pltpu.make_async_remote_copy(
            src_ref=hm.at[t, c], dst_ref=hm.at[t, c], send_sem=m_send.at[t], recv_sem=m_recv.at[t],
            device_id=peer, device_id_type=MESH)

    def own_block(t):
        return pl.ds(pl.multiple_of(z * pair + c * seqs, seqs), seqs)

    def spread(stage, cols, val):
        pf[stage, 0, :, cols] = val[:seqs]
        pf[stage, 1, :, cols] = val[seqs:]

    def out_proj(t):
        def body(nb, _):
            cols = pl.ds(pl.multiple_of(nb * o_cols, o_cols), o_cols)
            spread(0, cols, dot(olhs[...], wo_v[:, cols]))
            return 0

        lax.fori_loop(0, d_model // o_cols, body, 0)
        f_copy(t, 0).start()

    def mid(t):
        f_copy(t, 0).wait()
        hm[t, c] = (h_all[t, own_block(t), :].astype(F32) + (pf[0, c] + rf[t, 0])).astype(BF16)
        m_copy(t).start()

    def up(t, halfway):
        def body(nb, _):
            cols = pl.ds(pl.multiple_of(nb * u_cols, 128), u_cols)
            u = dot(hm[t].reshape(pair, d_model), wu_v[:, cols]).astype(BF16).astype(F32)
            act[:, cols] = jax.nn.gelu(u, approximate=True).astype(BF16)

            @pl.when(nb == ff_half // u_cols // 2 - 1)
            def _():
                halfway()

            return 0

        m_copy(t).wait()
        lax.fori_loop(0, ff_half // u_cols, body, 0)

    def down(t):
        def body(nb, _):
            cols = pl.ds(pl.multiple_of(nb * o_cols, o_cols), o_cols)
            spread(1, cols, dot(act[...], wbig[pl.ds(0, ff_half), cols]))
            return 0

        lax.fori_loop(0, d_model // o_cols, body, 0)
        f_copy(t, 1).start()

    def new_h(t):
        f_copy(t, 1).wait()
        new = (hm[t, c].astype(F32) + (pf[1, c] + rf[t, 1])).astype(BF16)
        h_all[t, own_block(t), :] = new
        y_ref[t] = new

    def attend_all(t, between):
        mine = kv_heads // 2

        def body(i, _):
            attend(t, jnp.where(i < mine, (1 - c) * mine + i, c * mine + i - mine))

            @pl.when(i == mine - 1)
            def _():
                exchange(t).start()

            for at, work in between.items():
                pl.when(i == at)(work)
            return 0

        lax.fori_loop(0, kv_heads, body, 0)

    for name in ("q", "k", "v", "K", "V", "o", "u"):
        load(name, 0).start()
    h_all[0, own_block(0), :] = x_ref[0]
    ag_start(0)
    h_all[1, own_block(1), :] = x_ref[1]
    oa[...] = jnp.zeros_like(oa)
    ag_hop(0, 1)
    ag_hop(0, 2)
    ag_start(1)
    ag_hop(0, 3)
    ag_hop(0, 4)
    ag_finish(0)

    def layer(l, _):
        more = l + 1 < layers

        def if_more(work, *args):
            @pl.when(more)
            def _():
                work(*args)

        def refill(*names):
            @pl.when(more)
            def _():
                for name in names:
                    load(name, l + 1).start()

        def keep_new(t):
            for i in range(2):
                knew_ref[l, t, i] = kn_ref[t, i].astype(BF16)

        for name in ("q", "k", "v"):
            load(name, l).wait()
        select(0)
        project(0)
        keep_new(0)
        ag_hop(1, 1)
        for name in ("K", "V"):
            load(name, l).wait()
        attend_all(0, {0: lambda: ag_hop(1, 2), 1: lambda: ag_hop(1, 3), 2: lambda: ag_hop(1, 4)})
        exchange(0).wait()
        scatter(0)
        rs_start(0)
        ag_finish(1)
        select(1)
        project(1)
        keep_new(1)
        load("d", l).start()
        refill("k", "v")
        rs_step(0, 4, True)
        attend_all(1, {
            0: lambda: rs_step(0, 3, False), 1: lambda: rs_step(0, 3, True),
            2: lambda: rs_step(0, 2, False), 3: lambda: rs_step(0, 2, True)})
        refill("K", "V")
        exchange(1).wait()
        scatter(1)
        rs_start(1)
        rs_step(0, 1, False)
        rs_step(0, 1, True)
        rs_finish(0)
        load("o", l).wait()
        load("u", l).wait()
        load("d", l).wait()
        finalize(0)
        out_proj(0)
        rs_step(1, 4, True)
        mid(0)
        rs_step(1, 3, False)
        up(0, lambda: rs_step(1, 3, True))
        down(0)
        rs_step(1, 2, False)
        new_h(0)
        if_more(ag_start, 0)
        rs_step(1, 2, True)
        rs_step(1, 1, False)
        if_more(ag_hop, 0, 1)
        rs_step(1, 1, True)
        rs_finish(1)
        finalize(1)
        out_proj(1)
        if_more(ag_hop, 0, 2)
        mid(1)
        refill("o")
        if_more(ag_hop, 0, 3)
        up(1, lambda: if_more(ag_hop, 0, 4))
        refill("u")
        down(1)
        refill("q")
        if_more(ag_finish, 0)
        new_h(1)
        if_more(ag_start, 1)
        return 0

    lax.fori_loop(0, layers, layer, 0)


def pool_kernel(vec_ref, move_ref, mig_ref, new_ref, k_ref, v_ref, ko_ref, vo_ref, moved):
    step, rows, slots = k_ref.shape[1:]
    live = slice(0, slots)
    group = moved.shape[1] // rows
    tab = vec_ref[...].astype(F32)
    at0, at1, keep = (tab[i : i + 1, live].astype(BF16) for i in range(3))
    keep = keep > 0
    base = pl.program_id(1) * step
    turns = [(which, g) for which in range(2) for g in range(step // group)]

    def move(which, g, slot):
        moved[slot] = lax.dot_general(
            mig_ref[which, :, g * group * rows : (g + 1) * group * rows], move_ref[...], (((0,), (0,)), ((), ())),
            preferred_element_type=F32).astype(BF16)

    move(0, 0, 0)
    for n, (which, g) in enumerate(turns):
        if n + 1 < len(turns):
            move(*turns[n + 1], (n + 1) % 2)
        pool_ref, out_ref = ((k_ref, ko_ref), (v_ref, vo_ref))[which]
        for j in range(group):
            i = g * group + j
            pos = jnp.full((1, slots), (base + i).astype(F32), F32).astype(BF16)
            for r in range(0, rows, 64):
                cut = slice(r, r + 64)
                val = jnp.where(keep, pool_ref[0, i, cut], moved[n % 2, j * rows + r : j * rows + r + 64, :])
                val = jnp.where(at0 == pos, new_ref[0, 0, which, cut, live], val)
                out_ref[0, i, cut] = jnp.where(at1 == pos, new_ref[0, 1, which, cut, live], val)


def new_pools(pools, mig, knew, vec, move):
    layers, page, rows, slots = pools[0].shape
    step = 16
    entries = mig.shape[1]
    block = pl.BlockSpec((1, step, rows, slots), lambda l, i: (l, i, 0, 0))
    return pl.pallas_call(
        pool_kernel,
        out_shape=[jax.ShapeDtypeStruct(pools[0].shape, BF16)] * 2,
        grid=(layers, page // step),
        in_specs=[
            pl.BlockSpec(vec.shape, lambda l, i: (0, 0)),
            pl.BlockSpec(move.shape, lambda l, i: (0, 0)),
            pl.BlockSpec((2, entries, step * rows), lambda l, i: (0, 0, l * (page // step) + i)),
            pl.BlockSpec((1, 2, 2, rows, 128), lambda l, i: (l, 0, 0, 0, 0)),
            block, block,
        ],
        out_specs=[block, block],
        scratch_shapes=[pltpu.VMEM((2, 4 * rows, slots), BF16)],
        compiler_params=pltpu.CompilerParams(dimension_semantics=("arbitrary", "arbitrary"), vmem_limit_bytes=67043328),
        name="new_pools",
    )(vec, move, mig, knew, *pools)


def slot_tables(table, lens, src, dst, dev, slots, page):
    ids = dev * slots + jnp.arange(slots, dtype=jnp.int32)
    from_src = ids[:, None] == src[None, :]
    is_src = jnp.any(from_src, axis=1)
    is_dst = jnp.any(ids[:, None] == dst[None, :], axis=1)
    target = jnp.where(is_src, jnp.sum(jnp.where(from_src, dst[None, :], 0), axis=1), ids)
    hit = [table[None, :, p] == target[:, None] for p in range(2)]
    live = [h & ~is_dst[:, None] for h in hit]
    return ids, is_src, is_dst, hit, live


def pad_rows(a, rows):
    return jnp.pad(a, ((0, rows - a.shape[0]), (0, 0)))


def solution(mesh):
    devs = mesh.shape["kv"]
    chips = devs // 2
    pool_spec = P(("rep", "kv"))
    tok_spec = P(None, ("rep", "kv"), None)

    def device_fn(embeds, w_query, w_key, w_value, w_out, w_up, w_down, k_pool, v_pool, new_table, seq_lens, mig_src, mig_dst):
        slots, layers, page, kv_heads, head = k_pool.shape
        seqs, d_model = embeds.shape[1:]
        ff = w_up.shape[2]
        rep_heads = w_query.shape[2] // head // kv_heads
        total = seqs * devs
        dev = lax.axis_index("kv")
        peer = dev + 1 - 2 * lax.rem(dev, 2)
        pools = [jnp.transpose(p, (1, 2, 3, 4, 0)).reshape(layers, page, kv_heads * head, slots) for p in (k_pool, v_pool)]

        ids, is_src, is_dst, hit, live = slot_tables(new_table, seq_lens, mig_src, mig_dst, dev, slots, page)
        peer_live = slot_tables(new_table, seq_lens, mig_src, mig_dst, peer, slots, page)[4]
        onehot = pad_rows((hit[0] | hit[1]).astype(BF16), 128)
        e_page = [jnp.concatenate([pad_rows(live[p].astype(BF16), 128), pad_rows(peer_live[p].astype(BF16), 128)]) for p in range(2)]
        e_sum = e_page[0] + e_page[1]
        pres = pad_rows(jnp.stack([jnp.sum(e.astype(F32), axis=0) for e in e_page]), 8)
        length = jnp.sum(jnp.where(hit[0] | hit[1], seq_lens[None, :], 0), axis=1)
        first, last = jnp.any(live[0], axis=1), jnp.any(live[1], axis=1)
        limit = jnp.where(first, jnp.minimum(length, page), jnp.where(last, length - page, 0))
        lane_tab = jnp.pad(jnp.stack([limit, last.astype(jnp.int32)]).astype(jnp.int32), ((0, 6), (0, 128 - slots)))
        on_last = jnp.any(hit[1], axis=1) & ~is_src
        at = [jnp.where(on_last, length - page + t, -1) for t in range(2)]
        keep = ~(is_src | is_dst)
        vec = jnp.pad(jnp.stack(at + [keep.astype(jnp.int32)]).astype(jnp.int32), ((0, 5), (0, 128 - slots)))
        move = (mig_dst[:, None] == ids[None, :]).astype(BF16)
        pick = (mig_src[:, None] == ids[None, :]).astype(BF16)

        mig = jnp.stack([
            lax.dot_general(pick, p.reshape(-1, slots), (((1,), (1,)), ((), ())), preferred_element_type=F32).astype(BF16)
            for p in pools
        ])
        mig = lax.psum(mig, "kv")

        dims = (layers, d_model, ff, chips, seqs, slots, kv_heads, head, page, rep_heads)
        own_rows = rep_heads * head
        sub = own_rows // 2
        kv_cols = kv_heads * head
        big = max(d_model, ff // 2)
        vm, dma = pltpu.VMEM, pltpu.SemaphoreType.DMA
        any_spec, vmem_spec = pl.BlockSpec(memory_space=pl.ANY), pl.BlockSpec(memory_space=pltpu.VMEM)
        flops = 2 * layers * 2 * (128 * d_model * (total + heads_all(w_query, kv_cols)) + 64 * d_model * (d_model + ff) * 2)
        y, knew = pl.pallas_call(
            functools.partial(main_kernel, dims),
            out_shape=[
                jax.ShapeDtypeStruct((2, seqs, d_model), BF16),
                jax.ShapeDtypeStruct((layers, 2, 2, kv_cols, 128), BF16),
            ],
            in_specs=[vmem_spec] + [any_spec] * 8 + [vmem_spec] * 6,
            out_specs=[vmem_spec] * 2,
            scratch_shapes=[
                vm((2, total, d_model), BF16),
                vm((slots, d_model), BF16),
                vm((big, d_model), BF16),
                vm((d_model, kv_cols), BF16),
                vm((d_model, kv_cols), BF16),
                vm((2 * own_rows, d_model), BF16),
                vm((d_model, ff // 2), BF16),
                vm((2, page, kv_cols, slots), BF16),
                vm((kv_heads * rep_heads, head, 128), F32),
                vm((2, 2, kv_cols, 128), F32),
                vm((page, rep_heads, 128), F32),
                vm((2, 2, 2, own_rows + 16, 128), F32),
                vm((2, 2, own_rows + 16, 128), F32),
                vm((2, rep_heads, 256), F32),
                vm((2, rep_heads, 256), F32),
                vm((2, chips, 2, sub + 16, 128), F32),
                vm((2, 2, HOPS, 2, sub + 16, 128), F32),
                vm((2 * seqs, 2 * own_rows), BF16),
                vm((2, 2, seqs, d_model), F32),
                vm((2, 2, seqs, d_model), F32),
                vm((2, 2, seqs, d_model), BF16),
                vm((2 * seqs, ff // 2), BF16),
                dma((2, 2, HOPS, 2)), dma((2, 2, HOPS, 2)),
                dma((2, 2, HOPS, 2)), dma((2, 2, HOPS, 2)),
                dma((2, 2)), dma((2, 2)),
                dma((2, 2, HOPS, 2)), dma((2, 2, HOPS, 2)),
                dma((2,)), dma((2,)),
                dma((2, 2)), dma((2, 2)),
                dma((2,)), dma((2,)),
                dma((8,)),
            ],
            compiler_params=pltpu.CompilerParams(collective_id=0, has_side_effects=True, vmem_limit_bytes=67043328),
            cost_estimate=pl.CostEstimate(flops=int(flops), bytes_accessed=int(90e6), transcendentals=0),
            name="decode",
        )(embeds, w_query, w_key, w_value, w_out, w_up, w_down, *pools, onehot, *e_page, e_sum, pres, lane_tab)

        outs = [
            jnp.transpose(p.reshape(layers, page, kv_heads, head, slots), (4, 0, 1, 2, 3))
            for p in new_pools(pools, mig, knew, vec, move)
        ]
        return y, outs[0], outs[1]

    def heads_all(w_query, kv_cols):
        return w_query.shape[2] + 2 * kv_cols

    return jax.shard_map(
        device_fn, mesh=mesh,
        in_specs=(tok_spec, P(), P(), P(), P(), P(), P(), pool_spec, pool_spec, P("rep", None), P("rep"), P("rep"), P("rep")),
        out_specs=(tok_spec, pool_spec, pool_spec), check_vma=False)
```

```python
import functools

import jax
import jax.numpy as jnp
from jax import lax
from jax.experimental import pallas as pl
from jax.experimental.pallas import tpu as pltpu
from jax.sharding import PartitionSpec as P

MESH = pl.DeviceIdType.MESH
F32 = jnp.float32
BF16 = jnp.bfloat16
NEG = -1e30
HOPS = 4


def dot(a, b):
    return jnp.dot(a, b, preferred_element_type=F32)


def split3(x):
    hi = x.astype(BF16)
    rest = x - hi.astype(F32)
    mid = rest.astype(BF16)
    low = (rest - mid.astype(F32)).astype(BF16)
    return jnp.concatenate([hi, mid, low], axis=0)


def exact_dot(x, onehot, across=False):
    rows = x.shape[0]
    dims = (((1,), (1 if across else 0,)), ((), ()))
    out = lax.dot_general(split3(x), onehot, dims, preferred_element_type=F32)
    return out[:rows] + out[rows : 2 * rows] + out[2 * rows :]


def sums_to_rows(parts):
    sub = lax.broadcasted_iota(jnp.int32, parts[0].shape, 0)
    for shift in (4, 2, 1):
        half = len(parts) // 2
        high = (sub & shift) != 0
        parts = [
            jnp.where(high, a + pltpu.roll(a, shift, 0), b + pltpu.roll(b, 8 - shift, 0))
            for a, b in zip(parts[half:], parts[:half], strict=True)
        ]
    return parts[0]


def takes(way, hop, half):
    return hop < HOPS or way == half


def main_kernel(
    dims,
    src_ref, dst_ref, tab_ref, len_ref, x_ref, wq, wk, wv, wo, wu, wd, kp, vp,
    y_ref, knew_ref, vec_ref, mig_out,
    oh_ref, e0_ref, e1_ref, es_ref, pres_ref, lane_ref, pick_ref, mg, mx, mr, mf,
    h_all, hsel, wbig, wk_v, wv_v, wo_v, wu_v, kv_v, q_ref, kn_ref, s_ref, oa, ob, a_ref, ms_ref, pd, rd,
    olhs, pf, rf, hm, act,
    ag_send, ag_recv, dd_send, dd_recv, own_send, own_recv, rs_send, rs_recv, x_send, x_recv, f_send, f_recv, m_send, m_recv,
    gs_send, gs_recv, gg_send, gg_recv, gp_send, gp_recv, go_send, go_recv, go_sem, w_sem,
):
    layers, d_model, ff, chips, seqs, slots, kv_heads, head, page, rep_heads = dims
    lanes = 128
    me = lax.axis_index("kv")
    z = me // 2
    c = lax.rem(me, 2)
    peer = {"kv": z * 2 + 1 - c}
    pair = 2 * seqs
    half_d = d_model // 2
    own_rows = rep_heads * head
    sub = own_rows // 2
    d_cols = 512
    s_cols = 1024
    o_cols = 512
    u_cols = ff // 2 // 2

    def chip(step):
        return lax.rem(z + step + 2 * chips, chips)

    def ring_to(way):
        return {"kv": 2 * chip(1 if way == 0 else -1) + c}

    barrier = pltpu.get_barrier_semaphore()
    for target in (peer, ring_to(0), ring_to(1)):
        pl.semaphore_signal(barrier, inc=1, device_id=target, device_id_type=MESH)
    pl.semaphore_wait(barrier, 3)

    heads_cols = 2 * rep_heads * head
    kv_cols = kv_heads * head
    ff_half = ff // 2

    def load(name, l):
        src, dst, i = {
            "q": (lambda: wq.at[l], lambda: wbig.at[pl.ds(0, d_model), :], 0),
            "k": (lambda: wk.at[l], lambda: wk_v, 1),
            "v": (lambda: wv.at[l], lambda: wv_v, 2),
            "o": (lambda: wo.at[l, pl.ds(pl.multiple_of(c * heads_cols, heads_cols), heads_cols), :], lambda: wo_v, 3),
            "u": (lambda: wu.at[l, :, pl.ds(pl.multiple_of(c * ff_half, ff_half), ff_half)], lambda: wu_v, 4),
            "d": (lambda: wd.at[l, pl.ds(pl.multiple_of(c * ff_half, ff_half), ff_half), :], lambda: wbig.at[pl.ds(0, ff_half), :], 5),
            "K": (lambda: kp.at[l], lambda: kv_v.at[0], 6),
            "V": (lambda: vp.at[l], lambda: kv_v.at[1], 7),
        }[name]
        return pltpu.make_async_copy(src(), dst(), w_sem.at[i])

    def block(t, zz, cc, half):
        return h_all.at[t, pl.ds(pl.multiple_of(zz * pair + cc * seqs, seqs), seqs), pl.ds(half * half_d, half_d)]

    def ag_copy(t, way, hop, half):
        sgn = 1 if way == 0 else -1
        ref = block(t, chip(-sgn * (hop - 1)), c, half)
        return pltpu.make_async_remote_copy(
            src_ref=ref, dst_ref=ref, send_sem=ag_send.at[t, way, hop - 1, half], recv_sem=ag_recv.at[t, way, hop - 1, half],
            device_id=ring_to(way), device_id_type=MESH)

    def dd_copy(t, way, hop, half):
        sgn = 1 if way == 0 else -1
        ref = block(t, chip(-sgn * hop), c, half)
        return pltpu.make_async_remote_copy(
            src_ref=ref, dst_ref=ref, send_sem=dd_send.at[t, way, hop - 1, half], recv_sem=dd_recv.at[t, way, hop - 1, half],
            device_id=peer, device_id_type=MESH)

    def own_copy(t, half):
        ref = block(t, z, c, half)
        return pltpu.make_async_remote_copy(
            src_ref=ref, dst_ref=ref, send_sem=own_send.at[t, half], recv_sem=own_recv.at[t, half],
            device_id=peer, device_id_type=MESH)

    def ag_start(t):
        for half in range(2):
            for way in range(2):
                ag_copy(t, way, 1, half).start()
        for half in range(2):
            own_copy(t, half).start()

    def ag_hop(t, hop):
        for half in range(2):
            for way in range(2):
                if takes(way, hop, half):
                    ag_copy(t, way, hop, half).wait_recv()
                    if hop < HOPS and takes(way, hop + 1, half):
                        ag_copy(t, way, hop + 1, half).start()
                    dd_copy(t, way, hop, half).start()

    def ag_finish(t):
        for half in range(2):
            own_copy(t, half).wait_recv()
            own_copy(t, half).wait_send()
            for way in range(2):
                for hop in range(1, HOPS + 1):
                    if takes(way, hop, half):
                        dd_copy(t, way, hop, half).wait_recv()
                        dd_copy(t, way, hop, half).wait_send()
                        ag_copy(t, way, hop, half).wait_send()

    def rs_copy(t, way, k, half):
        sgn = 1 if way == 0 else -1
        return pltpu.make_async_remote_copy(
            src_ref=pd.at[t, chip(sgn * k), half], dst_ref=rd.at[t, way, k - 1, half],
            send_sem=rs_send.at[t, way, k - 1, half], recv_sem=rs_recv.at[t, way, k - 1, half],
            device_id=ring_to(way), device_id_type=MESH)

    def merge(t, way, k, half):
        sgn = 1 if way == 0 else -1
        zz = chip(sgn * (k - 1))
        got = rd.at[t, way, k - 1, half]
        mine = pd.at[t, zz, half]
        m1, l1 = got[pl.ds(sub, 8), :], got[pl.ds(sub + 8, 8), :]
        m2, l2 = mine[pl.ds(sub, 8), :], mine[pl.ds(sub + 8, 8), :]
        m = jnp.maximum(m1, m2)
        a1, a2 = jnp.exp(m1 - m), jnp.exp(m2 - m)
        mine[pl.ds(sub, 8), :] = m
        mine[pl.ds(sub + 8, 8), :] = a1 * l1 + a2 * l2
        for i in range(rep_heads // 2):
            r = half * (rep_heads // 2) + i
            at = pl.ds(i * head, head)
            mine[at, :] = a1[r : r + 1] * got[at, :] + a2[r : r + 1] * mine[at, :]

    def rs_start(t):
        for half in range(2):
            for way in range(2):
                rs_copy(t, way, HOPS if takes(way, HOPS, half) else HOPS - 1, half).start()

    def rs_step(t, k, late):
        for way in range(2):
            half = way if late else 1 - way
            rs_copy(t, way, k, half).wait_recv()
            merge(t, way, k, half)
            if k > 1:
                rs_copy(t, way, k - 1, half).start()

    def rs_finish(t):
        for half in range(2):
            for way in range(2):
                for k in range(1, HOPS + 1):
                    if takes(way, k, half):
                        rs_copy(t, way, k, half).wait_send()

    def select(t):
        def body(nb, _):
            cols = pl.ds(pl.multiple_of(nb * s_cols, s_cols), s_cols)
            hsel[:, cols] = dot(oh_ref[pl.ds(0, slots), :], h_all[t, :, cols]).astype(BF16)
            return 0

        lax.fori_loop(0, d_model // s_cols, body, 0)

    def turned(w):
        rows = dot(hsel[...], w).astype(BF16).astype(F32)
        return jnp.concatenate([rows, jnp.zeros((lanes - slots, rows.shape[1]), F32)], axis=0).T

    def project(t):
        per = d_cols // head

        def body(nb, _):
            cols = pl.ds(pl.multiple_of(nb * d_cols, d_cols), d_cols)
            q_ref[pl.ds(nb * per, per)] = turned(wbig[pl.ds(0, d_model), cols]).reshape(per, head, lanes)
            return 0

        lax.fori_loop(0, kv_heads * rep_heads // per, body, 0)
        for i, w in enumerate((wk_v, wv_v)):
            kn_ref[t, i] = turned(w[...])

    def attend(t, kvh):
        rows = pl.ds(pl.multiple_of(kvh * head, head), head)
        live = pl.ds(0, slots)
        scale = head ** -0.5
        owner, which = kvh // 2, lax.rem(kvh, 2)
        out = oa.at[t, owner, which]

        def scores(keys):
            sums = []
            for h in range(rep_heads):
                q = [q_ref[kvh * rep_heads + h, pl.ds(d, 8), live] for d in range(0, head, 8)]
                parts = []
                for key in keys:
                    acc = q[0] * key[:8]
                    for i in range(1, head // 8):
                        acc = acc + q[i] * key[8 * i : 8 * i + 8]
                    parts.append(acc)
                sums.append(parts)
            return [sums_to_rows([part[i] for part in sums]) for i in range(len(keys))]

        def qk(pb, _):
            keys = [kv_v[0, pb * 4 + i, rows, :].astype(F32) for i in range(4)]
            for i, part in enumerate(scores(keys)):
                s_ref[pb * 4 + i, :, live] = part
            return 0

        lax.fori_loop(0, page // 4, qk, 0)
        fresh = list(range(t + 1))
        news = scores([kn_ref[i, 0, rows, live] for i in fresh])
        lim = lane_ref[0:1, live]
        has_new = lane_ref[1:2, live] > 0
        news = [jnp.where(has_new, s * scale, NEG) for s in news]
        pos = lax.broadcasted_iota(jnp.int32, (page, rep_heads, slots), 0)
        valid = pos < lim[None]
        old = jnp.where(valid, s_ref[:, :, live] * scale, NEG)
        m = jnp.max(old, axis=0)
        for s in news:
            m = jnp.maximum(m, s)
        probs = jnp.where(valid, jnp.exp(old - m[None]), 0.0)
        s_ref[:, :, live] = probs
        news = [jnp.where(has_new, jnp.exp(s - m), 0.0) for s in news]
        total = jnp.sum(probs, axis=0)
        for p in news:
            total = total + p
        out[pl.ds(own_rows, rep_heads), live] = m
        out[pl.ds(own_rows + 8, rep_heads), live] = total
        vals = [kn_ref[i, 1, rows, live] for i in fresh]
        for h in range(rep_heads):
            acc = news[0][h : h + 1] * vals[0]
            for p, v in zip(news[1:], vals[1:], strict=True):
                acc = acc + p[h : h + 1] * v
            out[pl.ds(h * head, head), live] = acc

        def pv(pb, _):
            vals = [kv_v[1, pb * 4 + i, rows, :].astype(F32) for i in range(4)]
            ps = [s_ref[pb * 4 + i, :, live] for i in range(4)]
            for h in range(rep_heads):
                at = pl.ds(h * head, head)
                acc = out[at, live]
                for p, v in zip(ps, vals, strict=True):
                    acc = acc + p[h : h + 1] * v
                out[at, live] = acc
            return 0

        lax.fori_loop(0, page // 4, pv, 0)

    def exchange(t):
        return pltpu.make_async_remote_copy(
            src_ref=oa.at[t, 1 - c], dst_ref=ob.at[t], send_sem=x_send.at[t], recv_sem=x_recv.at[t],
            device_id=peer, device_id_type=MESH)

    lane = lax.broadcasted_iota(jnp.int32, (1, lanes), 1)
    low_lanes = lane < pair

    def by_chip(parts, put):
        for zp in range(chips // 2):
            a, b = (p[:, zp * lanes : (zp + 1) * lanes] for p in parts)
            put(2 * zp, jnp.where(low_lanes, a, pltpu.roll(b, pair, 1)))
            put(2 * zp + 1, jnp.where(low_lanes, pltpu.roll(a, pair, 1), b))

    def scatter(t):
        def stat(o):
            return jnp.concatenate([
                jnp.concatenate([oa[t, c, hh, pl.ds(own_rows + o, 8), :], ob[t, hh, pl.ds(own_rows + o, 8), :]], axis=1)
                for hh in range(2)
            ], axis=0)

        top = stat(0)
        m_page = [jnp.where(pres_ref[i : i + 1, :] > 0, exact_dot(top, e[...]), NEG) for i, e in enumerate((e0_ref, e1_ref))]
        m_seq = jnp.maximum(m_page[0], m_page[1])
        a = jnp.exp(jnp.minimum(top - exact_dot(m_seq, es_ref[...], across=True), 0.0))
        a_ref[0], a_ref[1] = a[:8], a[8:]
        l_seq = exact_dot(stat(8) * a, es_ref[...])
        for dense, at in ((m_seq, sub), (l_seq, sub + 8)):
            def put(zz, v, at=at):
                for half in range(2):
                    pd[t, zz, half, pl.ds(at, 8), :] = v

            by_chip([dense[:8], dense[8:]], put)

        def body(n, _):
            for half in range(2):
                i = half * (rep_heads // 2) + n
                at = pl.ds(pl.multiple_of(i * head, head), head)
                parts = []
                for hh in range(2):
                    o = jnp.concatenate([oa[t, c, hh, at, :], ob[t, hh, at, :]], axis=1)
                    parts.append(exact_dot(o * a_ref[hh, pl.ds(i, 1), :], es_ref[...]))

                def put(zz, v, half=half):
                    pd[t, zz, half, pl.ds(pl.multiple_of(n * head, head), head), :] = v

                by_chip(parts, put)
            return 0

        lax.fori_loop(0, rep_heads // 2, body, 0)

    def finalize(t):
        for half in range(2):
            mine = pd.at[t, z, half]
            inv = 1.0 / mine[pl.ds(sub + 8, 8), :]
            rows = []
            for i in range(rep_heads // 2):
                r = half * (rep_heads // 2) + i
                rows.append(mine[pl.ds(i * head, head), :] * inv[r : r + 1])
            turned_o = jnp.concatenate(rows, axis=0).T.astype(BF16)
            for hh in range(2):
                olhs[:, pl.ds(hh * own_rows + half * sub, sub)] = turned_o[hh * pair : (hh + 1) * pair]

    def f_copy(t, stage):
        return pltpu.make_async_remote_copy(
            src_ref=pf.at[stage, 1 - c], dst_ref=rf.at[t, stage], send_sem=f_send.at[t, stage], recv_sem=f_recv.at[t, stage],
            device_id=peer, device_id_type=MESH)

    def m_copy(t):
        return pltpu.make_async_remote_copy(
            src_ref=hm.at[t, c], dst_ref=hm.at[t, c], send_sem=m_send.at[t], recv_sem=m_recv.at[t],
            device_id=peer, device_id_type=MESH)

    def own_block(t):
        return pl.ds(pl.multiple_of(z * pair + c * seqs, seqs), seqs)

    def spread(stage, cols, val):
        pf[stage, 0, :, cols] = val[:seqs]
        pf[stage, 1, :, cols] = val[seqs:]

    def out_proj(t):
        def body(nb, _):
            cols = pl.ds(pl.multiple_of(nb * o_cols, o_cols), o_cols)
            spread(0, cols, dot(olhs[...], wo_v[:, cols]))
            return 0

        lax.fori_loop(0, d_model // o_cols, body, 0)
        f_copy(t, 0).start()

    def mid(t):
        f_copy(t, 0).wait()
        hm[t, c] = (h_all[t, own_block(t), :].astype(F32) + (pf[0, c] + rf[t, 0])).astype(BF16)
        m_copy(t).start()

    def up(t, halfway):
        def body(nb, _):
            cols = pl.ds(pl.multiple_of(nb * u_cols, 128), u_cols)
            u = dot(hm[t].reshape(pair, d_model), wu_v[:, cols]).astype(BF16).astype(F32)
            act[:, cols] = jax.nn.gelu(u, approximate=True).astype(BF16)

            @pl.when(nb == ff_half // u_cols // 2 - 1)
            def _():
                halfway()

            return 0

        m_copy(t).wait()
        lax.fori_loop(0, ff_half // u_cols, body, 0)

    def down(t):
        def body(nb, _):
            cols = pl.ds(pl.multiple_of(nb * o_cols, o_cols), o_cols)
            spread(1, cols, dot(act[...], wbig[pl.ds(0, ff_half), cols]))
            return 0

        lax.fori_loop(0, d_model // o_cols, body, 0)
        f_copy(t, 1).start()

    def new_h(t):
        f_copy(t, 1).wait()
        new = (hm[t, c].astype(F32) + (pf[1, c] + rf[t, 1])).astype(BF16)
        h_all[t, own_block(t), :] = new
        y_ref[t] = new

    def attend_all(t, between):
        mine = kv_heads // 2

        def body(i, _):
            attend(t, jnp.where(i < mine, (1 - c) * mine + i, c * mine + i - mine))

            @pl.when(i == mine - 1)
            def _():
                exchange(t).start()

            for at, work in between.items():
                pl.when(i == at)(work)
            return 0

        lax.fori_loop(0, kv_heads, body, 0)

    entries = src_ref.shape[0]

    def ids_of(dev, axis):
        shape = (lanes, 1) if axis == 0 else (1, lanes)
        at = lax.broadcasted_iota(jnp.int32, shape, axis)
        return jnp.where(at < slots, dev * slots + at, -1)

    def tables():
        page_of = [tab_ref[p : p + 1, :] for p in range(2)]
        for g, dev in enumerate((me, z * 2 + 1 - c)):
            ids = ids_of(dev, 0)
            target, stale = ids, jnp.zeros_like(ids)
            for e in range(entries):
                target = jnp.where(ids == src_ref[e], dst_ref[e], target)
                stale = jnp.where(ids == dst_ref[e], 1, stale)
            hit = [jnp.where(p == target, 1.0, 0.0) for p in page_of]
            live = [jnp.where(stale == 0, h, 0.0) for h in hit]
            at = pl.ds(g * lanes, lanes)
            e0_ref[at, :] = live[0].astype(BF16)
            e1_ref[at, :] = live[1].astype(BF16)
            es_ref[at, :] = (live[0] + live[1]).astype(BF16)
            if g == 0:
                oh_ref[...] = (hit[0] + hit[1]).astype(BF16)
                held = [h.astype(BF16) for h in (live[0], live[1], hit[1])]
        for p, e in enumerate((e0_ref, e1_ref)):
            pres_ref[p : p + 1, :] = jnp.sum(e[...].astype(F32), axis=0, keepdims=True)
        lens = len_ref[...].astype(F32)
        rows = jnp.concatenate([lens, jnp.ones_like(lens), jnp.zeros((6, lens.shape[1]), F32)], axis=0).astype(BF16)
        first, last, fresh = (
            lax.dot_general(rows, h, (((1,), (1,)), ((), ())), preferred_element_type=F32) for h in held)
        limit = jnp.where(
            first[1:2] > 0, jnp.minimum(first[0:1], page), jnp.where(last[1:2] > 0, last[0:1] - page, 0.0))
        lane_ref[0:1, :] = limit.astype(jnp.int32)
        lane_ref[1:2, :] = last[1:2].astype(jnp.int32)
        ids = ids_of(me, 1)
        is_src, is_dst = jnp.zeros_like(ids), jnp.zeros_like(ids)
        row = lax.broadcasted_iota(jnp.int32, (entries, lanes), 0)
        pick = jnp.zeros((entries, lanes), F32)
        for e in range(entries):
            is_src = jnp.where(ids == src_ref[e], 1, is_src)
            is_dst = jnp.where(ids == dst_ref[e], 1, is_dst)
            pick = jnp.where(row == e, jnp.where(ids == src_ref[e], 1.0, 0.0), pick)
        pick_ref[...] = pick[:, :slots].astype(BF16)
        on_last = jnp.where(is_src == 0, fresh[1:2], 0.0) > 0
        start = fresh[0:1] - page
        vec_ref[0:1, :] = jnp.where(on_last, start, -1.0)
        vec_ref[1:2, :] = jnp.where(on_last, start + 1, -1.0)
        vec_ref[2:3, :] = jnp.where(is_src + is_dst == 0, 1.0, 0.0)
        vec_ref[3:8, :] = jnp.zeros((5, lanes), F32)

    m_cols = mf.shape[1] // chips // 2

    def extract():
        def body(i, _):
            for w in range(2):
                for j in range(4):
                    n = i * 4 + j
                    mg[w, :, pl.ds(pl.multiple_of(n * kv_cols, kv_cols), kv_cols)] = lax.dot_general(
                        pick_ref[...], kv_v[w, n], (((1,), (1,)), ((), ())), preferred_element_type=F32).astype(BF16)
            return 0

        lax.fori_loop(0, page // 4, body, 0)
        mig_pair().start()

    def mig_pair():
        return pltpu.make_async_remote_copy(
            src_ref=mg.at[1 - c], dst_ref=mx, send_sem=gp_send, recv_sem=gp_recv, device_id=peer, device_id_type=MESH)

    def m_at(zz, half):
        return pl.ds(pl.multiple_of((zz * 2 + half) * m_cols, m_cols), m_cols)

    def ms_copy(way, k, half):
        sgn = 1 if way == 0 else -1
        return pltpu.make_async_remote_copy(
            src_ref=mg.at[c, :, m_at(chip(sgn * k), half)], dst_ref=mr.at[way, k - 1, half],
            send_sem=gs_send.at[way, k - 1, half], recv_sem=gs_recv.at[way, k - 1, half],
            device_id=ring_to(way), device_id_type=MESH)

    def mig_start():
        mig_pair().wait()
        mg[c] = mg[c] + mx[...]
        for half in range(2):
            for way in range(2):
                ms_copy(way, HOPS if takes(way, HOPS, half) else HOPS - 1, half).start()

    def mig_step(k):
        for half in range(2):
            for way in range(2):
                if takes(way, k, half):
                    sgn = 1 if way == 0 else -1
                    ms_copy(way, k, half).wait_recv()
                    at = m_at(chip(sgn * (k - 1)), half)
                    mg[c, :, at] = mg[c, :, at] + mr[way, k - 1, half]
                    if k > 1:
                        ms_copy(way, k - 1, half).start()
        if k == 1:
            for half in range(2):
                mf[:, m_at(z, half)] = mg[c, :, m_at(z, half)]
                for way in range(2):
                    for k2 in range(1, HOPS + 1):
                        if takes(way, k2, half):
                            ms_copy(way, k2, half).wait_send()

    def mgat_copy(way, hop, half):
        sgn = 1 if way == 0 else -1
        ref = mf.at[:, m_at(chip(-sgn * (hop - 1)), half)]
        return pltpu.make_async_remote_copy(
            src_ref=ref, dst_ref=ref, send_sem=gg_send.at[way, hop - 1, half], recv_sem=gg_recv.at[way, hop - 1, half],
            device_id=ring_to(way), device_id_type=MESH)

    def mgat_hop(hop):
        for half in range(2):
            for way in range(2):
                if hop == 0:
                    mgat_copy(way, 1, half).start()
                elif takes(way, hop, half):
                    mgat_copy(way, hop, half).wait_recv()
                    if hop < HOPS and takes(way, hop + 1, half):
                        mgat_copy(way, hop + 1, half).start()

    def mig_out_copies(l):
        return (
            pltpu.make_async_remote_copy(
                src_ref=mf, dst_ref=mig_out.at[l, c], send_sem=go_send, recv_sem=go_recv, device_id=peer, device_id_type=MESH),
            pltpu.make_async_copy(mf, mig_out.at[l, c], go_sem),
        )

    def mig_put(l):
        for way in range(2):
            for half in range(2):
                for hop in range(1, HOPS + 1):
                    if takes(way, hop, half):
                        mgat_copy(way, hop, half).wait_send()
        for copy in mig_out_copies(l):
            copy.start()

    def mig_done(l):
        for copy in mig_out_copies(l):
            copy.wait()

    for name in ("q", "k", "v", "K", "V", "o", "u"):
        load(name, 0).start()
    h_all[0, own_block(0), :] = x_ref[0]
    ag_start(0)
    h_all[1, own_block(1), :] = x_ref[1]
    tables()
    ag_hop(0, 1)
    oa[...] = jnp.zeros_like(oa)
    ag_hop(0, 2)
    ag_start(1)
    load("K", 0).wait()
    load("V", 0).wait()
    extract()
    ag_hop(0, 3)
    ag_hop(0, 4)
    ag_finish(0)

    def layer(l, _):
        more = l + 1 < layers

        def if_more(work, *args):
            @pl.when(more)
            def _():
                work(*args)

        def refill(*names):
            @pl.when(more)
            def _():
                for name in names:
                    load(name, l + 1).start()

        def keep_new(t):
            for i in range(2):
                knew_ref[l, t, i] = kn_ref[t, i].astype(BF16)

        for name in ("q", "k", "v"):
            load(name, l).wait()
        select(0)
        mig_start()
        project(0)
        keep_new(0)
        ag_hop(1, 1)
        mig_step(4)

        def also(hop, k):
            def work():
                ag_hop(1, hop)
                mig_step(k)

            return work

        attend_all(0, {0: also(2, 3), 1: also(3, 2), 2: also(4, 1)})
        exchange(0).wait()
        scatter(0)
        rs_start(0)
        ag_finish(1)
        select(1)
        project(1)
        keep_new(1)
        load("d", l).start()
        refill("k", "v")
        rs_step(0, 4, True)
        attend_all(1, {
            0: lambda: rs_step(0, 3, False), 1: lambda: rs_step(0, 3, True),
            2: lambda: rs_step(0, 2, False), 3: lambda: rs_step(0, 2, True)})
        refill("K", "V")
        exchange(1).wait()
        scatter(1)
        rs_start(1)
        rs_step(0, 1, False)
        rs_step(0, 1, True)
        rs_finish(0)
        load("o", l).wait()
        load("u", l).wait()
        load("d", l).wait()
        finalize(0)
        out_proj(0)
        rs_step(1, 4, True)
        mid(0)
        rs_step(1, 3, False)
        up(0, lambda: rs_step(1, 3, True))
        down(0)
        rs_step(1, 2, False)
        new_h(0)
        if_more(ag_start, 0)

        @pl.when(more)
        def _():
            load("K", l + 1).wait()
            load("V", l + 1).wait()
            extract()

        rs_step(1, 2, True)
        rs_step(1, 1, False)
        if_more(ag_hop, 0, 1)
        rs_step(1, 1, True)
        mgat_hop(0)
        rs_finish(1)
        finalize(1)
        out_proj(1)
        if_more(ag_hop, 0, 2)
        mgat_hop(1)
        mid(1)
        refill("o")
        if_more(ag_hop, 0, 3)
        mgat_hop(2)
        up(1, lambda: (if_more(ag_hop, 0, 4), mgat_hop(3)))
        refill("u")
        mgat_hop(4)
        mig_put(l)
        down(1)
        refill("q")
        if_more(ag_finish, 0)
        new_h(1)
        if_more(ag_start, 1)
        mig_done(l)
        return 0

    lax.fori_loop(0, layers, layer, 0)


def pool_kernel(dst_ref, vec_ref, mig_ref, new_ref, y_ref, k_ref, v_ref, ko_ref, vo_ref, yo_ref, moved, move_ref):
    step, rows, slots = k_ref.shape[1:]
    entries = dst_ref.shape[0]
    live = slice(0, slots)
    group = moved.shape[1] // rows
    tab = vec_ref[...]
    at0, at1, keep = (tab[i : i + 1, live].astype(BF16) for i in range(3))
    keep = keep > 0
    base = pl.program_id(1) * step
    turns = [(which, g) for which in range(2) for g in range(step // group)]

    @pl.when((pl.program_id(0) == 0) & (pl.program_id(1) == 0))
    def _():
        yo_ref[...] = y_ref[...]
        ids = lax.axis_index("kv") * slots + lax.broadcasted_iota(jnp.int32, (entries, slots), 1)
        row = lax.broadcasted_iota(jnp.int32, (entries, slots), 0)
        put = jnp.zeros((entries, slots), F32)
        for e in range(entries):
            put = jnp.where(row == e, jnp.where(ids == dst_ref[e], 1.0, 0.0), put)
        move_ref[...] = put.astype(BF16)

    def move(which, g, slot):
        moved[slot] = lax.dot_general(
            mig_ref[0, which, :, g * group * rows : (g + 1) * group * rows], move_ref[...], (((0,), (0,)), ((), ())),
            preferred_element_type=F32).astype(BF16)

    move(0, 0, 0)
    for n, (which, g) in enumerate(turns):
        if n + 1 < len(turns):
            move(*turns[n + 1], (n + 1) % 2)
        pool_ref, out_ref = ((k_ref, ko_ref), (v_ref, vo_ref))[which]
        for j in range(group):
            i = g * group + j
            pos = jnp.full((1, slots), (base + i).astype(F32), F32).astype(BF16)
            val = jnp.where(keep, pool_ref[0, i], moved[n % 2, j * rows : (j + 1) * rows, :])
            val = jnp.where(at0 == pos, new_ref[0, 0, which, :, live], val)
            out_ref[0, i] = jnp.where(at1 == pos, new_ref[0, 1, which, :, live], val)


def new_pools(pools, mig, knew, vec, dst, y):
    layers, page, rows, slots = pools[0].shape
    step = 32
    entries = mig.shape[2]
    block = pl.BlockSpec((1, step, rows, slots), lambda l, i: (l, i, 0, 0))
    whole = pl.BlockSpec(y.shape, lambda l, i: (0, 0, 0))
    return pl.pallas_call(
        pool_kernel,
        out_shape=[jax.ShapeDtypeStruct(pools[0].shape, BF16)] * 2 + [jax.ShapeDtypeStruct(y.shape, BF16)],
        grid=(layers, page // step),
        in_specs=[
            pl.BlockSpec(memory_space=pltpu.SMEM),
            pl.BlockSpec(vec.shape, lambda l, i: (0, 0)),
            pl.BlockSpec((1, 2, entries, step * rows), lambda l, i: (l, 0, 0, i)),
            pl.BlockSpec((1, 2, 2, rows, 128), lambda l, i: (l, 0, 0, 0, 0)),
            whole, block, block,
        ],
        out_specs=[block, block, whole],
        scratch_shapes=[pltpu.VMEM((2, 4 * rows, slots), BF16), pltpu.VMEM((entries, slots), BF16)],
        compiler_params=pltpu.CompilerParams(dimension_semantics=("arbitrary", "arbitrary"), vmem_limit_bytes=67043328),
        name="new_pools",
    )(dst, vec, mig, knew, y, *pools)


def solution(mesh):
    devs = mesh.shape["kv"]
    chips = devs // 2
    pool_spec = P(("rep", "kv"))
    tok_spec = P(None, ("rep", "kv"), None)

    def device_fn(embeds, w_query, w_key, w_value, w_out, w_up, w_down, k_pool, v_pool, new_table, seq_lens, mig_src, mig_dst):
        slots, layers, page, kv_heads, head = k_pool.shape
        seqs, d_model = embeds.shape[1:]
        ff = w_up.shape[2]
        rep_heads = w_query.shape[2] // head // kv_heads
        total = seqs * devs
        entries = mig_src.shape[0]
        pools = [jnp.transpose(p, (1, 2, 3, 4, 0)).reshape(layers, page, kv_heads * head, slots) for p in (k_pool, v_pool)]

        dims = (layers, d_model, ff, chips, seqs, slots, kv_heads, head, page, rep_heads)
        own_rows = rep_heads * head
        sub = own_rows // 2
        kv_cols = kv_heads * head
        big = max(d_model, ff // 2)
        vm, dma = pltpu.VMEM, pltpu.SemaphoreType.DMA
        any_spec, vmem_spec, smem_spec = (pl.BlockSpec(memory_space=m) for m in (pl.ANY, pltpu.VMEM, pltpu.SMEM))
        flops = 2 * layers * 2 * (128 * d_model * (total + heads_all(w_query, kv_cols)) + 64 * d_model * (d_model + ff) * 2)
        y, knew, vec, mig = pl.pallas_call(
            functools.partial(main_kernel, dims),
            out_shape=[
                jax.ShapeDtypeStruct((2, seqs, d_model), BF16),
                jax.ShapeDtypeStruct((layers, 2, 2, kv_cols, 128), BF16),
                jax.ShapeDtypeStruct((8, 128), F32),
                jax.ShapeDtypeStruct((layers, 2, entries, page * kv_cols), BF16),
            ],
            in_specs=[smem_spec] * 2 + [vmem_spec] * 3 + [any_spec] * 8,
            out_specs=[vmem_spec] * 3 + [any_spec],
            scratch_shapes=[
                vm((128, total), BF16),
                vm((256, total), BF16),
                vm((256, total), BF16),
                vm((256, total), BF16),
                vm((8, total), F32),
                vm((8, 128), jnp.int32),
                vm((entries, slots), BF16),
                vm((2, entries, page * kv_cols), BF16),
                vm((entries, page * kv_cols), BF16),
                vm((2, HOPS, 2, entries, page * kv_cols // chips // 2), BF16),
                vm((entries, page * kv_cols), BF16),
                vm((2, total, d_model), BF16),
                vm((slots, d_model), BF16),
                vm((big, d_model), BF16),
                vm((d_model, kv_cols), BF16),
                vm((d_model, kv_cols), BF16),
                vm((2 * own_rows, d_model), BF16),
                vm((d_model, ff // 2), BF16),
                vm((2, page, kv_cols, slots), BF16),
                vm((kv_heads * rep_heads, head, 128), F32),
                vm((2, 2, kv_cols, 128), F32),
                vm((page, rep_heads, 128), F32),
                vm((2, 2, 2, own_rows + 16, 128), F32),
                vm((2, 2, own_rows + 16, 128), F32),
                vm((2, rep_heads, 256), F32),
                vm((2, rep_heads, 256), F32),
                vm((2, chips, 2, sub + 16, 128), F32),
                vm((2, 2, HOPS, 2, sub + 16, 128), F32),
                vm((2 * seqs, 2 * own_rows), BF16),
                vm((2, 2, seqs, d_model), F32),
                vm((2, 2, seqs, d_model), F32),
                vm((2, 2, seqs, d_model), BF16),
                vm((2 * seqs, ff // 2), BF16),
                dma((2, 2, HOPS, 2)), dma((2, 2, HOPS, 2)),
                dma((2, 2, HOPS, 2)), dma((2, 2, HOPS, 2)),
                dma((2, 2)), dma((2, 2)),
                dma((2, 2, HOPS, 2)), dma((2, 2, HOPS, 2)),
                dma((2,)), dma((2,)),
                dma((2, 2)), dma((2, 2)),
                dma((2,)), dma((2,)),
                dma((2, HOPS, 2)), dma((2, HOPS, 2)), dma((2, HOPS, 2)), dma((2, HOPS, 2)),
                dma, dma, dma, dma, dma,
                dma((8,)),
            ],
            compiler_params=pltpu.CompilerParams(collective_id=0, has_side_effects=True, vmem_limit_bytes=67043328),
            cost_estimate=pl.CostEstimate(flops=int(flops), bytes_accessed=int(90e6), transcendentals=0),
            name="decode",
        )(mig_src, mig_dst, new_table.T, seq_lens[None], embeds, w_query, w_key, w_value, w_out, w_up, w_down, *pools)

        *outs, y = new_pools(pools, mig, knew, vec, mig_dst, y)
        outs = [jnp.transpose(p.reshape(layers, page, kv_heads, head, slots), (4, 0, 1, 2, 3)) for p in outs]
        return y, outs[0], outs[1]

    def heads_all(w_query, kv_cols):
        return w_query.shape[2] + 2 * kv_cols

    return jax.shard_map(
        device_fn, mesh=mesh,
        in_specs=(tok_spec, P(), P(), P(), P(), P(), P(), pool_spec, pool_spec, P("rep", None), P("rep"), P("rep"), P("rep")),
        out_specs=(tok_spec, pool_spec, pool_spec), check_vma=False)
```

```python
import functools
from types import SimpleNamespace

import jax
import jax.numpy as jnp
from jax import lax
from jax.experimental import pallas as pl
from jax.experimental.pallas import tpu as pltpu
from jax.sharding import PartitionSpec as P

MESH = pl.DeviceIdType.MESH
F32, BF16, I32 = jnp.float32, jnp.bfloat16, jnp.int32
NEG = -1e30
LANES = 128
SUB = 8
A, B = BOTH = range(2)
PAIR = len(BOTH)
VMEM_BYTES = 67043328
FAR = 4
HOPS = range(1, FAR + 1)


class Names:
    def __getattr__(self, name):
        return name


W = Names()
ORDER = (
    W.AG00s, W.AG01s, W.TAB, W.EXT0, W.AG00h10, W.AG00h11, W.AG01h10, W.AG01h11, W.MS0s, W.AG00h20, W.AG00h21,
    W.AG01h20, W.AG01h21, W.MS0k400, W.MS0k310, W.MS0k301, W.MS0k411, W.AG00h30, W.AG00h31, W.AG01h30, W.AG01h31,
    W.MS0k300, W.MS0k210, W.MS0k201, W.MS0k311, W.AG00h40, W.AG00h41, W.AG01h40, W.SEL00, W.PROJ00, W.AG01h41,
    W.MS0k200, W.MS0k211, W.MS0k110, W.MS0k101, W.ATT000, W.ATT001, W.MS0k100, W.MS0k111, W.MG0s, W.ATT002, W.ATT003,
    W.MG0h10, W.MG0h11, W.SCAT00, W.RS00s, W.SEL01, W.PROJ01, W.MG0h20, W.MG0h21, W.ATT010, W.RS00k400, W.RS00k310,
    W.ATT011, W.RS00k411, W.RS00k301, W.MG0h30, W.MG0h31, W.ATT012, W.RS00k300, W.RS00k210, W.ATT013, W.RS00k311,
    W.RS00k201, W.MG0h41, W.SCAT01, W.RS01s, W.MG0h40, W.RS00k200, W.RS00k110, W.EXT1, W.RS00k211, W.RS00k101,
    W.RS01k400, W.RS01k310, W.MS1s, W.RS01k301, W.RS01k411, W.RS00k100, W.RS00k111, W.FO00, W.RS01k300, W.MS1k400,
    W.RS01k210, W.MS1k301, W.MS1k310, W.MS1k411, W.MID00, W.RS01k201, W.RS01k311, W.UP000, W.UP001, W.DOWN00,
    W.RS01k200, W.RS01k110, W.MS1k300, W.MS1k210, W.MS1k311, W.MS1k201, W.NEWH00, W.AG10s, W.RS01k101, W.RS01k211,
    W.MS1k110, W.MS1k211, W.RS01k100, W.MS1k200, W.MS1k101, W.AG10h10, W.AG10h11, W.RS01k111, W.FO01, W.MS1k111,
    W.MS1k100, W.MG1s, W.MID01, W.AG10h20, W.AG10h21, W.UP010, W.UP011, W.DOWN01, W.MG1h10, W.MG1h11, W.AG10h30,
    W.AG10h31, W.NEWH01, W.AG11s, W.MG1h20, W.MG1h21, W.AG10h40, W.AG10h41, W.AG11h10, W.SEL10, W.AG11h11, W.PROJ10,
    W.MG1h30, W.MG1h31, W.ATT100, W.AG11h20, W.AG11h21, W.ATT101, W.MG1h40, W.MG1h41, W.ATT102, W.AG11h30, W.AG11h31,
    W.ATT103, W.SCAT10, W.RS10s, W.AG11h40, W.AG11h41, W.SEL11, W.PROJ11, W.ATT110, W.RS10k400, W.RS10k310, W.ATT111,
    W.RS10k411, W.RS10k301, W.ATT112, W.RS10k300, W.RS10k210, W.ATT113, W.RS10k311, W.RS10k201, W.SCAT11, W.RS11s,
    W.RS10k200, W.RS10k110, W.RS10k211, W.RS10k101, W.RS11k400, W.RS11k310, W.RS11k301, W.RS11k411, W.RS10k100,
    W.RS10k111, W.FO10, W.RS11k300, W.RS11k210, W.MID10, W.RS11k201, W.RS11k311, W.UP100, W.UP101, W.DOWN10,
    W.RS11k200, W.RS11k110, W.NEWH10, W.RS11k101, W.RS11k211, W.RS11k100, W.RS11k111, W.FO11, W.MID11, W.UP110,
    W.UP111, W.DOWN11, W.NEWH11,
)


def dot(a, b):
    return jnp.dot(a, b, preferred_element_type=F32)


def dot_by(a, b, left, right):
    return lax.dot_general(a, b, (((left,), (right,)), ((), ())), preferred_element_type=F32)


def exact_dot(x, onehot, right=A):
    high = x.astype(BF16)
    rest = x - high.astype(F32)
    mid = rest.astype(BF16)
    low = (rest - mid.astype(F32)).astype(BF16)
    out = dot_by(jnp.concatenate([high, mid, low], axis=A), onehot, B, right).reshape(FAR - 1, x.shape[A], -1)
    return out[A] + out[B] + out[PAIR]


def sums_to_rows(parts):
    axis = parts[A].ndim - PAIR
    sub = lax.broadcasted_iota(I32, parts[A].shape, axis)
    while len(parts) > 1:
        half = len(parts) // PAIR
        high = (sub & half) != 0
        parts = [
            jnp.where(high, a + pltpu.roll(a, half, axis), b + pltpu.roll(b, SUB - half, axis))
            for a, b in zip(parts[half:], parts[:half], strict=True)
        ]
    return parts[A]


def at_block(i, size):
    return pl.ds(pl.multiple_of(i * size, size), size)


def loop(count, body):
    def step(i, carry):
        body(i)
        return carry

    lax.fori_loop(A, count, step, A)


def takes(way, hop, half):
    return hop < FAR or way == half


def taken(hops=HOPS):
    return [(way, hop, half) for half in BOTH for way in BOTH for hop in hops if takes(way, hop, half)]


def mask_rows(ids, values, shape=None):
    out = jnp.zeros(shape or ids.shape, I32)
    for e in range(values.shape[A]):
        out = jnp.where(ids == values[e], 1, out)
    return out


def placed(ids, values, slots):
    entries = values.shape[A]
    row = lax.broadcasted_iota(I32, (entries, slots), A)
    out = jnp.zeros((entries, slots), F32)
    for e in range(entries):
        out = jnp.where(row == e, jnp.where(ids == values[e], 1.0, 0.0), out)
    return out.astype(BF16)


def main_kernel(
    n,
    src_ref, dst_ref, tab_ref, len_ref, x_ref, wq, wk, wv, wo, wu, wd, kp, vp,
    y_ref, knew_ref, vec_ref, mig_out,
    oh_ref, e_ref, es_ref, pres_ref, lane_ref, pick_ref, mg, mx, mr, mf,
    h_all, hsel, wbig, wk_v, wv_v, wo_v, wu_v, kv_v, q_ref, kn_ref, s_ref, oa, ob, a_ref, pd, rd,
    olhs, pf, rf, hm, act, ag_sent, ag_got, dd_sem, rs_sent, rs_got, x_sem, f_sem, m_sem, gs_sent, gs_got, gg_sent, gg_got,
    gp_sem, go_sem, w_sem,
):
    me = lax.axis_index("kv")
    z, c = me // PAIR, lax.rem(me, PAIR)
    group = lax.axis_index("rep")
    peer = (group, z * PAIR + 1 - c)
    live = pl.ds(A, n.slots)
    half_d = n.d_model // PAIR
    heads_half = n.rep_heads // PAIR

    chips = {step: lax.rem(z + step + n.chips, n.chips) for step in range(-FAR, FAR + 1)}
    rings = {step: (group, PAIR * chips[step] + c) for step in (-1, 1)}
    h_rows = {step: (chips[step] * PAIR + c) * n.seqs for step in chips}

    def along(way, steps):
        return steps if way == A else -steps

    def on_ring(way, steps):
        return rings[along(way, steps)]

    def remote_by(src, dst, send, recv, target):
        return pltpu.make_async_remote_copy(
            src_ref=src, dst_ref=dst, send_sem=send, recv_sem=recv, device_id=target, device_id_type=MESH)

    def remote(src, dst, sems, at, target):
        return remote_by(src, dst, sems.at[(A, *at)], sems.at[(B, *at)], target)

    barrier = pltpu.get_barrier_semaphore()
    others = (peer, *rings.values())
    for target in others:
        pl.semaphore_signal(barrier, inc=1, device_id=target, device_id_type=MESH)
    pl.semaphore_wait(barrier, len(others))

    mine_o, mine_f = at_block(c, n.wide), at_block(c, n.ff_half)
    sources = {
        "q": lambda l: (wq.at[l], wbig.at[pl.ds(A, n.d_model), :]), "k": lambda l: (wk.at[l], wk_v), "v": lambda l: (wv.at[l], wv_v),
        "o": lambda l: (wo.at[l, mine_o, :], wo_v), "u": lambda l: (wu.at[l, :, mine_f], wu_v),
        "d": lambda l: (wd.at[l, mine_f, :], wbig.at[pl.ds(A, n.ff_half), :]),
        "K": lambda l: (kp.at[l], kv_v.at[A]), "V": lambda l: (vp.at[l], kv_v.at[B]),
    }
    follows = {"q": ("d", A), "d": ("q", B)} | {name: (name, B) for name in "kvouKV"}
    users = {name: PAIR for name in "qkvoud"} | {name: PAIR + 1 for name in "KV"}
    ready, used = set(), {}

    def load(name, l):
        src, dst = sources[name](l)
        return pltpu.make_async_copy(src, dst, w_sem.at[list(sources).index(name)])

    def need(names, l):
        for name in names:
            if (name, l) not in ready:
                ready.add((name, l))
                load(name, l).wait()

    def release(names, l):
        for name in names:
            used[name, l] = used.get((name, l), A) + 1
            after, more = follows[name]
            if used[name, l] == users[name] and l + more < n.layers:
                load(after, l + more).start()

    def gather(ref_of, sent, got, key):
        def copy(way, hop, half):
            ref = ref_of(along(way, 1 - hop), half)
            return remote_by(ref, ref, sent.at[key], got.at[key, way, hop - 1, half], on_ring(way, 1))

        return copy

    def gather_start(copy):
        for half in BOTH:
            for way in BOTH:
                copy(way, 1, half).start()

    def gather_hop(copy, hop, half, passed_on=None):
        for way in BOTH:
            if takes(way, hop, half):
                copy(way, hop, half).wait_recv()
                if hop < FAR and takes(way, hop + 1, half):
                    copy(way, hop + 1, half).start()
                if passed_on:
                    passed_on(way, hop, half).start()

    def total(src_of, got_of, sent, got, key):
        def copy(way, dist, half):
            return remote_by(
                src_of(along(way, dist), half), got_of(way, dist, half), sent.at[key], got.at[key, way, dist - 1, half],
                on_ring(way, 1))

        return copy

    def total_start(copy):
        for way in BOTH:
            copy(way, FAR, way).start()
        for way in BOTH:
            copy(way, FAR - 1, 1 - way).start()

    def total_hop(copy, add, dist, way, half):
        copy(way, dist, half).wait_recv()
        add(along(way, dist - 1), way, dist, half)
        if dist > 1:
            copy(way, dist - 1, half).start()

    ring_copies = len(taken())

    def all_sent(ref, sem):
        remote_by(ref, ref, sem, sem, peer).wait_send()

    def block(t, step, half):
        return h_all.at[t, pl.ds(pl.multiple_of(h_rows[step], n.seqs), n.seqs), pl.ds(half * half_d, half_d)]

    ag_copies = [gather(lambda step, half, t=t: block(t, step, half), ag_sent, ag_got, t) for t in BOTH]

    def to_peer(t):
        def copy(way, hop, half):
            ref = block(t, along(way, -hop), half)
            return remote(ref, ref, dd_sem, (t,), peer)

        return copy

    def ag_start(l, t):
        gather_start(ag_copies[t])
        for half in BOTH:
            to_peer(t)(A, A, half).start()

    def ag_hop(t, hop, half):
        gather_hop(ag_copies[t], hop, half, to_peer(t))

    def ag_finish(t):
        blocks = ring_copies // PAIR
        from_peer = h_all.at[t, pl.ds(A, (blocks + 1) * n.seqs), :]
        remote(from_peer, from_peer, dd_sem, (t,), peer).wait()
        all_sent(h_all.at[t, pl.ds(A, blocks * n.seqs), :], ag_sent.at[t])

    tops, sums = pl.ds(n.sub, SUB), pl.ds(n.sub + SUB, SUB)
    rs_copies = [
        total(lambda step, half, t=t: pd.at[t, chips[step], half], lambda way, d, half, t=t: rd.at[t, way, d - 1, half], rs_sent, rs_got, t)
        for t in BOTH
    ]

    def merge(t):
        def add(step, way, d, half):
            got, mine = rd.at[t, way, d - 1, half], pd.at[t, chips[step], half]
            m1, m2 = got[tops, :], mine[tops, :]
            m = jnp.maximum(m1, m2)
            a1, a2 = jnp.exp(m1 - m), jnp.exp(m2 - m)
            mine[tops, :] = m
            mine[sums, :] = a1 * got[sums, :] + a2 * mine[sums, :]
            at = pl.ds(A, n.sub)
            by_head = (heads_half, n.head, LANES)
            a1, a2 = (a[half * heads_half : (half + 1) * heads_half][:, None] for a in (a1, a2))
            mine[at, :] = (a1 * got[at, :].reshape(by_head) + a2 * mine[at, :].reshape(by_head)).reshape(n.sub, LANES)

        return add

    def select(l, t):
        ag_finish(t)

        def body(i):
            cols = at_block(i, n.s_cols)
            hsel[:, cols] = dot(oh_ref[live, :], h_all[t, :, cols]).astype(BF16)

        loop(n.d_model // n.s_cols, body)

    def turned(w):
        rows = dot(hsel[...], w).astype(BF16).astype(F32)
        return jnp.concatenate([rows, jnp.zeros((LANES - n.slots, rows.shape[B]), F32)], axis=A).T

    def project(l, t):
        need("qkv", l)
        per = n.d_cols // n.head

        def body(i):
            q_ref[pl.ds(i * per, per)] = turned(wbig[pl.ds(A, n.d_model), at_block(i, n.d_cols)]).reshape(per, n.head, LANES)

        loop(n.kv_heads * n.rep_heads // per, body)
        for i, w in enumerate((wk_v, wv_v)):
            kn_ref[t, i] = turned(w[...])
            knew_ref[l, t, i] = kn_ref[t, i].astype(BF16)
        release("qkv", l)

    def attend(t, kvh):
        rows = at_block(kvh, n.head)
        scale = n.head ** -0.5
        out = oa.at[t, kvh // PAIR, lax.rem(kvh, PAIR)]
        heads = range(n.rep_heads)

        def scores(keys):
            parts = []
            for h in heads:
                prods = q_ref[kvh * n.rep_heads + h, :, live][None] * keys
                acc = prods[:, :SUB]
                for d in range(SUB, n.head, SUB):
                    acc = acc + prods[:, d : d + SUB]
                parts.append(acc)
            return sums_to_rows(parts)

        def qk(i):
            at = pl.ds(i * FAR, FAR)
            s_ref[at, :, live] = scores(kv_v[A, at, rows, :].astype(F32))

        loop(n.page // FAR, qk)
        fresh = range(t + 1)
        news = [scores(kn_ref[i, A, rows, live][None])[A] for i in fresh]
        lim, has_new = lane_ref[pl.ds(A, 1), live], lane_ref[pl.ds(B, 1), live] > 0
        news = [jnp.where(has_new, s * scale, NEG) for s in news]
        valid = lax.broadcasted_iota(I32, (n.page, n.rep_heads, n.slots), A) < lim[None]
        old = jnp.where(valid, s_ref[:, :, live] * scale, NEG)
        m = jnp.max(old, axis=A)
        for s in news:
            m = jnp.maximum(m, s)
        probs = jnp.where(valid, jnp.exp(old - m[None]), 0.0)
        s_ref[:, :, live] = probs
        news = [jnp.where(has_new, jnp.exp(s - m), 0.0) for s in news]
        count = jnp.sum(probs, axis=A)
        for p in news:
            count = count + p
        out[pl.ds(n.own_rows, SUB), live] = m
        out[pl.ds(n.own_rows + SUB, SUB), live] = count
        vals = [kn_ref[i, B, rows, live] for i in fresh]
        for h in heads:
            acc = news[A][h : h + 1] * vals[A]
            for p, v in zip(news[1:], vals[1:], strict=True):
                acc = acc + p[h : h + 1] * v
            out[pl.ds(h * n.head, n.head), live] = acc

        def pv(i):
            vals = [kv_v[B, i * FAR + j, rows, :].astype(F32) for j in range(FAR)]
            ps = [s_ref[i * FAR + j, :, live] for j in range(FAR)]
            for h in heads:
                at = pl.ds(h * n.head, n.head)
                acc = out[at, live]
                for p, v in zip(ps, vals, strict=True):
                    acc = acc + p[h : h + 1] * v
                out[at, live] = acc

        loop(n.page // FAR, pv)

    def exchange(t):
        return remote(oa.at[t, 1 - c], ob.at[t], x_sem, (t,), peer)

    def attend_all(l, t, between):
        mine = n.kv_heads // PAIR
        need("KV", l)

        def body(i):
            attend(t, jnp.where(i < mine, (1 - c) * mine + i, c * mine + i - mine))
            pl.when(i == mine - 1)(lambda: exchange(t).start())
            for at, work in between.items():
                pl.when(i == at)(work)

        loop(n.kv_heads, body)
        release("KV", l)

    low_lanes = lax.broadcasted_iota(I32, (1, LANES), B) < n.pair

    def by_chip(parts, put):
        for zp in range(n.chips // PAIR):
            a, b = (p[:, zp * LANES : (zp + 1) * LANES] for p in parts)
            put(PAIR * zp, jnp.where(low_lanes, a, pltpu.roll(b, n.pair, B)))
            put(PAIR * zp + 1, jnp.where(low_lanes, pltpu.roll(a, n.pair, B), b))

    def scatter(l, t):
        exchange(t).wait()

        def both_cores(hh, at):
            return jnp.concatenate([oa[t, c, hh, at, :], ob[t, hh, at, :]], axis=B)

        top, count = (
            jnp.concatenate([both_cores(hh, pl.ds(n.own_rows + off, SUB)) for hh in BOTH], axis=A) for off in (A, SUB))
        m_page = [jnp.where(pres_ref[pl.ds(p, 1), :] > 0, exact_dot(top, e_ref[p]), NEG) for p in BOTH]
        m_seq = jnp.maximum(*m_page)
        a = jnp.exp(jnp.minimum(top - exact_dot(m_seq, es_ref[...], right=B), 0.0))
        a_ref[A], a_ref[B] = a[:SUB], a[SUB:]
        l_seq = exact_dot(count * a, es_ref[...])
        for dense, at in ((m_seq, tops), (l_seq, sums)):
            def put(zz, v, at=at):
                for half in BOTH:
                    pd[t, zz, half, at, :] = v

            by_chip([dense[:SUB], dense[SUB:]], put)

        def body(i):
            for half in BOTH:
                h = half * heads_half + i
                parts = [
                    exact_dot(both_cores(hh, at_block(h, n.head)) * a_ref[hh, pl.ds(h, 1), :], es_ref[...]) for hh in BOTH]

                def put(zz, v, half=half):
                    pd[t, zz, half, at_block(i, n.head), :] = v

                by_chip(parts, put)

        loop(heads_half, body)

    def f_copy(t, stage):
        return remote(pf.at[t, 1 - c], rf.at[t, stage], f_sem, (t, stage), peer)

    def m_copy(t):
        return remote(hm.at[t, c], hm.at[t, c], m_sem, (t,), peer)

    def product(t, lhs, w):
        def body(i):
            cols = at_block(i, n.d_cols)
            val = dot(lhs(), w(cols))
            pf[t, A, :, cols] = val[: n.seqs]
            pf[t, B, :, cols] = val[n.seqs :]

        loop(n.d_model // n.d_cols, body)

    own = pl.ds(pl.multiple_of(h_rows[A], n.seqs), n.seqs)

    def out_proj(l, t):
        all_sent(pd.at[t, pl.ds(A, ring_copies // PAIR)], rs_sent.at[t])
        for half in BOTH:
            mine = pd.at[t, z, half]
            inv = (1.0 / mine[sums, :])[half * heads_half : (half + 1) * heads_half][:, None]
            flat = (mine[pl.ds(A, n.sub), :].reshape(heads_half, n.head, LANES) * inv).reshape(n.sub, LANES).T.astype(BF16)
            for hh in BOTH:
                olhs[:, pl.ds(hh * n.own_rows + half * n.sub, n.sub)] = flat[hh * n.pair : (hh + 1) * n.pair]
        need("o", l)
        product(t, lambda: olhs[...], lambda cols: wo_v[:, cols])
        release("o", l)
        f_copy(t, A).start()

    def mid(l, t):
        f_copy(t, A).wait()
        hm[t, c] = (h_all[t, own, :].astype(F32) + (pf[t, c] + rf[t, A])).astype(BF16)
        m_copy(t).start()

    def up(l, t, halfway):
        m_copy(t).wait()
        need("u", l)

        def body(i):
            cols = at_block(i, n.u_cols)
            u = dot(hm[t].reshape(n.pair, n.d_model), wu_v[:, cols]).astype(BF16).astype(F32)
            act[t, :, cols] = jax.nn.gelu(u, approximate=True).astype(BF16)
            for at, work in halfway.items():
                pl.when(i == at)(work)

        loop(n.ff_half // n.u_cols, body)
        release("u", l)

    def down(l, t):
        need("d", l)
        product(t, lambda: act[t], lambda cols: wbig[pl.ds(A, n.ff_half), cols])
        release("d", l)
        f_copy(t, B).start()

    def new_h(l, t):
        f_copy(t, B).wait()
        new = (hm[t, c].astype(F32) + (pf[t, c] + rf[t, B])).astype(BF16)
        h_all[t, own, :] = new
        y_ref[t] = new

    def ids_of(dev, axis):
        at = lax.broadcasted_iota(I32, (LANES, 1) if axis == A else (1, LANES), axis)
        return jnp.where(at < n.slots, dev * n.slots + at, -1)

    def tables():
        oa[...] = jnp.zeros_like(oa)
        for g, dev in enumerate((me, z * PAIR + 1 - c)):
            ids = ids_of(dev, A)
            target = ids
            for e in range(n.entries):
                target = jnp.where(ids == src_ref[e], dst_ref[e], target)
            stale = mask_rows(ids, dst_ref)
            hit = [jnp.where(tab_ref[pl.ds(p, 1), :] == target, 1.0, 0.0) for p in BOTH]
            now = [jnp.where(stale == 0, h, 0.0) for h in hit]
            at = pl.ds(g * LANES, LANES)
            for p in BOTH:
                e_ref[p, at, :] = now[p].astype(BF16)
            es_ref[at, :] = (now[A] + now[B]).astype(BF16)
            if g == A:
                oh_ref[...] = (hit[A] + hit[B]).astype(BF16)
                held = [h.astype(BF16) for h in (*now, hit[B])]
        for p in BOTH:
            pres_ref[pl.ds(p, 1), :] = jnp.sum(e_ref[p].astype(F32), axis=A, keepdims=True)
        lens = len_ref[...].astype(F32)
        rows = jnp.concatenate([lens, jnp.ones((SUB - 1, lens.shape[B]), F32)], axis=A).astype(BF16)
        first, last, fresh = (dot_by(rows, h, B, B) for h in held)
        at0, at1 = slice(A, 1), slice(B, PAIR)
        limit = jnp.where(first[at1] > 0, jnp.minimum(first[at0], n.page), jnp.where(last[at1] > 0, last[at0] - n.page, 0.0))
        lane_ref[pl.ds(A, 1), :] = limit.astype(I32)
        lane_ref[pl.ds(B, 1), :] = last[at1].astype(I32)
        ids = ids_of(me, B)
        is_src, is_dst = mask_rows(ids, src_ref), mask_rows(ids, dst_ref)
        pick_ref[...] = placed(ids[:, : n.slots], src_ref, n.slots)
        on_last = jnp.where(is_src == 0, fresh[at1], 0.0) > 0
        start = fresh[at0] - n.page
        vec_ref[...] = jnp.where(is_src + is_dst == 0, 1.0, 0.0) * jnp.ones((SUB, LANES), F32)
        for t in BOTH:
            vec_ref[pl.ds(t, 1), :] = jnp.where(on_last, start + t, -1.0)

    m_cols = mf.shape[B] // n.chips // PAIR

    def mig_pair():
        return remote(mg.at[1 - c], mx, gp_sem, (), peer)

    def m_at(step, half):
        return at_block(chips[step] * PAIR + half, m_cols)

    ms_copies, mg_copies = [], []
    for l in range(n.layers):
        ms_copies.append(total(lambda step, half: mg.at[c, :, m_at(step, half)], lambda way, d, half: mr.at[way, d - 1, half], gs_sent, gs_got, l))
        mg_copies.append(gather(lambda step, half: mf.at[:, m_at(step, half)], gg_sent, gg_got, l))

    def mig_add(step, way, d, half):
        at = m_at(step, half)
        mg[c, :, at] = mg[c, :, at] + mr[way, d - 1, half]

    m_ring = pl.ds(A, ring_copies * m_cols)

    def mig_sent(l):
        all_sent(mg.at[c, :, m_ring], gs_sent.at[l])

    def mig_out_copies(l):
        return remote(mf, mig_out.at[l, c], go_sem, (l,), peer), pltpu.make_async_copy(mf, mig_out.at[l, c], go_sem.at[PAIR, l])

    def extract(l):
        need("KV", l)
        if l > 0:
            mig_sent(l - 1)

        def body(i):
            for w in BOTH:
                for j in range(FAR):
                    r = i * FAR + j
                    mg[w, :, at_block(r, n.kv_cols)] = dot_by(pick_ref[...], kv_v[w, r], B, B).astype(BF16)

        loop(n.page // FAR, body)
        release("KV", l)
        mig_pair().start()

    def mig_start(l):
        if l > 0:
            for copy in mig_out_copies(l - 1):
                copy.wait()
        mig_pair().wait()
        mg[c] = mg[c] + mx[...]
        total_start(ms_copies[l])

    def mig_gather(l):
        for half in BOTH:
            mf[:, m_at(A, half)] = mg[c, :, m_at(A, half)]
        gather_start(mg_copies[l])

    def mig_end(l):
        all_sent(mf.at[:, m_ring], gg_sent.at[l])
        for copy in mig_out_copies(l):
            copy.start()

    steps = {"TAB": tables}
    for l in range(n.layers):
        steps[f"EXT{l}"] = functools.partial(extract, l)
        steps[f"MS{l}s"] = functools.partial(mig_start, l)
        steps[f"MG{l}s"] = functools.partial(mig_gather, l)
        for hop in HOPS:
            for half in BOTH:
                steps[f"MG{l}h{hop}{half}"] = functools.partial(gather_hop, mg_copies[l], hop, half)
                for way in BOTH:
                    steps[f"MS{l}k{hop}{way}{half}"] = functools.partial(total_hop, ms_copies[l], mig_add, hop, way, half)
        for t in BOTH:
            for name, work in (
                ("SEL", select), ("PROJ", project), ("SCAT", scatter), ("FO", out_proj), ("MID", mid), ("DOWN", down), ("NEWH", new_h),
            ):
                steps[f"{name}{l}{t}"] = functools.partial(work, l, t)
            steps[f"AG{l}{t}s"] = functools.partial(ag_start, l, t)
            steps[f"RS{l}{t}s"] = functools.partial(total_start, rs_copies[t])
            for hop in HOPS:
                for half in BOTH:
                    steps[f"AG{l}{t}h{hop}{half}"] = functools.partial(ag_hop, t, hop, half)
                    for way in BOTH:
                        steps[f"RS{l}{t}k{hop}{way}{half}"] = functools.partial(total_hop, rs_copies[t], merge(t), hop, way, half)

    for name in ("q", "k", "v", "K", "V", "o", "u"):
        load(name, A).start()
    for t in BOTH:
        h_all[t, own, :] = x_ref[t]

    todo = list(ORDER)
    on_way = {l: len([name for name in todo if name.startswith(f"MG{l}h")]) for l in range(n.layers)}

    def run(names):
        for name in names:
            steps[name]()
            if name.startswith("MG") and "h" in name:
                l = int(name[PAIR])
                on_way[l] -= 1
                if on_way[l] == 0:
                    mig_end(l)

    loops = {"ATT": (attend_all, n.kv_heads), "UP": (up, n.ff_half // n.u_cols)}
    while todo:
        name = todo.pop(A)
        word = name.rstrip("0123456789")
        if word in loops:
            work, count = loops[word]
            l, t, _ = (int(ch) for ch in name[len(word) :])
            between = {}
            for i in range(count - 1):
                upto = todo.index(f"{word}{l}{t}{i + 1}")
                if upto:
                    between[i] = functools.partial(run, todo[:upto])
                todo = todo[upto + 1 :]
            work(l, t, between)
        else:
            run([name])
    for copy in mig_out_copies(n.layers - 1):
        copy.wait()
    mig_sent(n.layers - 1)


def pool_kernel(dst_ref, vec_ref, mig_ref, new_ref, y_ref, k_ref, v_ref, ko_ref, vo_ref, yo_ref, moved, move_ref):
    step, rows, slots = k_ref.shape[1:]
    live = slice(A, slots)
    group = moved.shape[1] // rows
    tab = vec_ref[...]
    at0, at1, keep = (tab[i : i + 1, live].astype(BF16) for i in range(PAIR + 1))
    keep = keep > 0
    base = pl.program_id(B) * step
    turns = [(which, g) for which in BOTH for g in range(step // group)]

    @pl.when((pl.program_id(A) == 0) & (pl.program_id(B) == 0))
    def _():
        yo_ref[...] = y_ref[...]
        ids = lax.axis_index("kv") * slots + lax.broadcasted_iota(I32, (1, slots), B)
        move_ref[...] = placed(ids, dst_ref, slots)

    def move(which, g, slot):
        moved[slot] = dot_by(mig_ref[A, which, :, g * group * rows : (g + 1) * group * rows], move_ref[...], A, A).astype(BF16)

    move(A, A, A)
    for i, (which, g) in enumerate(turns):
        if i + 1 < len(turns):
            move(*turns[i + 1], (i + 1) % PAIR)
        pool_ref, out_ref = ((k_ref, ko_ref), (v_ref, vo_ref))[which]
        for j in range(group):
            r = g * group + j
            pos = jnp.full((1, slots), (base + r).astype(F32), F32).astype(BF16)
            val = jnp.where(keep, pool_ref[A, r], moved[i % PAIR, j * rows : (j + 1) * rows, :])
            val = jnp.where(at0 == pos, new_ref[A, A, which, :, live], val)
            out_ref[A, r] = jnp.where(at1 == pos, new_ref[A, B, which, :, live], val)


def new_pools(pools, mig, knew, vec, dst, y):
    layers, page, rows, slots = pools[A].shape
    step, group = page // PAIR, FAR
    entries = mig.shape[PAIR]
    block = pl.BlockSpec((1, step, rows, slots), lambda l, i: (l, i, A, A))
    whole = pl.BlockSpec(y.shape, lambda l, i: (A, A, A))
    return pl.pallas_call(
        pool_kernel,
        out_shape=[jax.ShapeDtypeStruct(pools[A].shape, BF16)] * PAIR + [jax.ShapeDtypeStruct(y.shape, BF16)],
        grid=(layers, page // step),
        in_specs=[
            pl.BlockSpec(memory_space=pltpu.SMEM),
            pl.BlockSpec(vec.shape, lambda l, i: (A, A)),
            pl.BlockSpec((1, PAIR, entries, step * rows), lambda l, i: (l, A, A, i)),
            pl.BlockSpec((1, PAIR, PAIR, rows, LANES), lambda l, i: (l, A, A, A, A)),
            whole, block, block,
        ],
        out_specs=[block, block, whole],
        scratch_shapes=[pltpu.VMEM((PAIR, group * rows, slots), BF16), pltpu.VMEM((entries, slots), BF16)],
        compiler_params=pltpu.CompilerParams(dimension_semantics=("arbitrary",) * PAIR, vmem_limit_bytes=VMEM_BYTES),
        name="new_pools",
    )(dst, vec, mig, knew, y, *pools)


def solution(mesh):
    devs = mesh.shape["kv"]
    pool_spec = P(("rep", "kv"))
    tok_spec = P(None, ("rep", "kv"), None)

    def device_fn(embeds, w_query, w_key, w_value, w_out, w_up, w_down, k_pool, v_pool, new_table, seq_lens, mig_src, mig_dst):
        slots, layers, page, kv_heads, head = k_pool.shape
        seqs, d_model = embeds.shape[1:]
        rep_heads = w_query.shape[-1] // head // kv_heads
        own_rows = rep_heads * head
        n = SimpleNamespace(
            layers=layers, d_model=d_model, ff_half=w_up.shape[-1] // PAIR, chips=devs // PAIR, seqs=seqs, pair=PAIR * seqs,
            slots=slots, kv_heads=kv_heads, head=head, page=page, rep_heads=rep_heads, own_rows=own_rows, sub=own_rows // PAIR,
            wide=kv_heads // PAIR * own_rows, kv_cols=kv_heads * head, entries=mig_src.shape[A],
            s_cols=d_model // PAIR, d_cols=d_model // FAR, u_cols=w_up.shape[-1] // FAR)
        total = seqs * devs
        pages = page * n.kv_cols
        pools = [jnp.moveaxis(p, A, -1).reshape(layers, page, n.kv_cols, slots) for p in (k_pool, v_pool)]
        dma, two = pltpu.SemaphoreType.DMA, PAIR
        ring = (two, FAR, two)
        bf = lambda *shape: pltpu.VMEM(shape, BF16)
        f32 = lambda *shape: pltpu.VMEM(shape, F32)
        hbm, vmem, smem = (pl.BlockSpec(memory_space=m) for m in (pl.ANY, pltpu.VMEM, pltpu.SMEM))
        y, knew, vec, mig = pl.pallas_call(
            functools.partial(main_kernel, n),
            out_shape=[
                jax.ShapeDtypeStruct((two, seqs, d_model), BF16),
                jax.ShapeDtypeStruct((layers, two, two, n.kv_cols, LANES), BF16),
                jax.ShapeDtypeStruct((SUB, LANES), F32),
                jax.ShapeDtypeStruct((layers, two, n.entries, pages), BF16),
            ],
            in_specs=[smem] * two + [vmem] * (two + 1) + [hbm] * SUB,
            out_specs=[vmem] * (two + 1) + [hbm],
            scratch_shapes=[
                bf(LANES, total), bf(two, two * LANES, total), bf(two * LANES, total), f32(SUB, total), pltpu.VMEM((SUB, LANES), I32),
                bf(n.entries, slots), bf(two, n.entries, pages), bf(n.entries, pages),
                bf(two, FAR, two, n.entries, pages // devs), bf(n.entries, pages),
                bf(two, total, d_model), bf(slots, d_model), bf(max(d_model, n.ff_half), d_model), bf(d_model, n.kv_cols),
                bf(d_model, n.kv_cols), bf(n.wide, d_model), bf(d_model, n.ff_half), bf(two, page, n.kv_cols, slots),
                f32(kv_heads * rep_heads, head, LANES), f32(two, two, n.kv_cols, LANES), f32(page, rep_heads, LANES),
                f32(two, two, two, own_rows + two * SUB, LANES), f32(two, two, own_rows + two * SUB, LANES),
                f32(two, rep_heads, two * LANES), f32(two, n.chips, two, n.sub + two * SUB, LANES),
                f32(two, two, FAR, two, n.sub + two * SUB, LANES), bf(n.pair, n.wide), f32(two, two, seqs, d_model),
                f32(two, two, seqs, d_model), bf(two, two, seqs, d_model), bf(two, n.pair, n.ff_half),
                dma((two,)), dma((two, *ring)), dma((two, two)), dma((two,)), dma((two, *ring)), dma((two, two)),
                dma((two, two, two)), dma((two, two)), dma((layers,)), dma((layers, *ring)), dma((layers,)), dma((layers, *ring)),
                dma((two,)), dma((two + 1, layers)), dma((SUB,)),
            ],
            compiler_params=pltpu.CompilerParams(collective_id=A, has_side_effects=True, vmem_limit_bytes=VMEM_BYTES),
            name="decode",
        )(mig_src, mig_dst, new_table.T, seq_lens[None], embeds, w_query, w_key, w_value, w_out, w_up, w_down, *pools)
        *outs, y = new_pools(pools, mig, knew, vec, mig_dst, y)
        outs = [jnp.moveaxis(p.reshape(layers, page, kv_heads, head, slots), -1, A) for p in outs]
        return y, *outs

    return jax.shard_map(
        device_fn, mesh=mesh,
        in_specs=(tok_spec, *(P(),) * (SUB - PAIR), pool_spec, pool_spec, P("rep", None), *(P("rep"),) * (FAR - 1)),
        out_specs=(tok_spec, pool_spec, pool_spec), check_vma=False)
```

```python
import functools
from types import SimpleNamespace

import jax
import jax.numpy as jnp
from jax import lax
from jax.experimental import pallas as pl
from jax.experimental.pallas import tpu as pltpu
from jax.sharding import PartitionSpec as P

MESH = pl.DeviceIdType.MESH
F32, BF16, I32 = jnp.float32, jnp.bfloat16, jnp.int32
NEG = -1e30
LANES = 128
SUB = 8
A, B = BOTH = range(2)
PAIR = len(BOTH)
VMEM_BYTES = 67043328
FAR = 4
HOPS = range(1, FAR + 1)


class Names:
    def __getattr__(self, name):
        return name


W = Names()
ORDER = (
    W.AG00s, W.AG01s, W.TAB, W.EXT0, W.AG00h10, W.AG00h11, W.AG01h10, W.AG01h11, W.AG00h20, W.AG00h21, W.AG01h20,
    W.AG01h21, W.AG00h30, W.AG00h31, W.AG01h30, W.AG01h31, W.AG00h40, W.AG00h41, W.SEL00, W.AG01h40, W.PROJ00,
    W.AG01h41, W.ATT000, W.MS0s, W.ATT001, W.ATT002, W.MS0k400, W.MS0k411, W.MS0k310, W.MS0k301, W.SCAT00, W.RS00s,
    W.SEL01, W.MS0k300, W.MS0k311, W.PROJ01, W.MS0k210, W.MS0k201, W.ATT010, W.RS00k400, W.RS00k310, W.ATT011,
    W.RS00k411, W.RS00k301, W.MS0k200, W.MS0k211, W.ATT012, W.RS00k300, W.RS00k210, W.MS0k110, W.MS0k101, W.SCAT01,
    W.RS00k311, W.RS00k201, W.RS01s, W.MS0k100, W.MS0k111, W.EXT1, W.RS00k200, W.RS00k110, W.RS00k211, W.RS00k101,
    W.RS01k310, W.RS01k400, W.RS01k411, W.RS01k301, W.RS00k111, W.RS00k100, W.FO00, W.RS01k210, W.RS01k300, W.MID00,
    W.UP000, W.UP001, W.RS01k311, W.RS01k201, W.DOWN00, W.RS01k200, W.RS01k110, W.NEWH00, W.AG10s, W.RS01k211,
    W.RS01k101, W.RS01k100, W.AG10h10, W.AG10h11, W.RS01k111, W.FO01, W.AG10h20, W.MID01, W.AG10h21, W.UP010, W.UP011,
    W.AG10h30, W.DOWN01, W.AG10h31, W.NEWH01, W.AG11s, W.AG10h40, W.AG10h41, W.MG0s, W.SEL10, W.AG11h10, W.PROJ10,
    W.AG11h11, W.MG0h10, W.ATT100, W.AG11h20, W.MG0h11, W.ATT101, W.AG11h21, W.MG0h20, W.ATT102, W.AG11h30, W.MG0h21,
    W.SCAT10, W.RS10s, W.AG11h31, W.MG0h30, W.AG11h40, W.MG0h31, W.RS10k400, W.RS10k310, W.RS10k301, W.RS10k411,
    W.MG0h40, W.AG11h41, W.MG0h41, W.MS1s, W.SEL11, W.PROJ11, W.RS10k300, W.RS10k210, W.ATT110, W.RS10k311,
    W.RS10k201, W.MS1k400, W.MS1k310, W.MS1k301, W.ATT111, W.RS10k200, W.RS10k110, W.MS1k411, W.ATT112, W.RS10k211,
    W.RS10k101, W.MS1k300, W.MS1k210, W.SCAT11, W.RS11s, W.MS1k311, W.MS1k201, W.RS10k100, W.MS1k200, W.RS10k111,
    W.FO10, W.MS1k110, W.MID10, W.RS11k400, W.RS11k310, W.UP100, W.UP101, W.RS11k411, W.RS11k301, W.MS1k101, W.DOWN10,
    W.MS1k211, W.MS1k100, W.RS11k210, W.RS11k300, W.NEWH10, W.RS11k311, W.RS11k201, W.MS1k111, W.MG1s, W.RS11k200,
    W.RS11k110, W.RS11k101, W.RS11k211, W.MG1h10, W.MG1h11, W.RS11k100, W.RS11k111, W.FO11, W.MG1h20, W.MG1h21,
    W.MID11, W.UP110, W.MG1h30, W.UP111, W.MG1h31, W.DOWN11, W.MG1h40, W.MG1h41, W.NEWH11,
)


def dot(a, b):
    return jnp.dot(a, b, preferred_element_type=F32)


def dot_by(a, b, left, right):
    return lax.dot_general(a, b, (((left,), (right,)), ((), ())), preferred_element_type=F32)


def exact_dot(x, onehot, right=A):
    high = x.astype(BF16)
    rest = x - high.astype(F32)
    mid = rest.astype(BF16)
    low = (rest - mid.astype(F32)).astype(BF16)
    out = dot_by(jnp.concatenate([high, mid, low], axis=A), onehot, B, right).reshape(FAR - 1, x.shape[A], -1)
    return out[A] + out[B] + out[PAIR]


def sums_to_rows(parts):
    axis = parts[A].ndim - PAIR
    sub = lax.broadcasted_iota(I32, parts[A].shape, axis)
    while len(parts) > 1:
        half = len(parts) // PAIR
        high = (sub & half) != 0
        parts = [
            jnp.where(high, a + pltpu.roll(a, half, axis), b + pltpu.roll(b, SUB - half, axis))
            for a, b in zip(parts[half:], parts[:half], strict=True)
        ]
    return parts[A]


def at_block(i, size):
    return pl.ds(pl.multiple_of(i * size, size), size)


def loop(count, body):
    def step(i, carry):
        body(i)
        return carry

    lax.fori_loop(A, count, step, A)


def takes(way, hop, half):
    return hop < FAR or way == half


def taken(hops=HOPS):
    return [(way, hop, half) for half in BOTH for way in BOTH for hop in hops if takes(way, hop, half)]


def mask_rows(ids, values, shape=None):
    out = jnp.zeros(shape or ids.shape, I32)
    for e in range(values.shape[A]):
        out = jnp.where(ids == values[e], 1, out)
    return out


def placed(ids, values, slots):
    entries = values.shape[A]
    row = lax.broadcasted_iota(I32, (entries, slots), A)
    out = jnp.zeros((entries, slots), F32)
    for e in range(entries):
        out = jnp.where(row == e, jnp.where(ids == values[e], 1.0, 0.0), out)
    return out.astype(BF16)


def main_kernel(
    n,
    src_ref, dst_ref, tab_ref, len_ref, x_ref, wq, wk, wv, wo, wu, wd, kp, vp,
    y_ref, knew_ref, vec_ref, mig_out,
    oh_ref, e_ref, es_ref, pres_ref, lane_ref, pick_ref, mg, mx, mr, mf,
    h_all, hsel, wbig, wk_v, wv_v, wo_v, wu_v, raw, kv_p, q_ref, kn_ref, kn_p, s_ref, oa, ob, a_ref, pd, rd,
    olhs, pf, rf, hm, act, ag_sent, ag_got, dd_sem, rs_sent, rs_got, x_sem, f_sem, m_sem, gs_sent, gs_got, gg_sent, gg_got,
    gp_sem, go_sem, p_sem, w_sem,
):
    me = lax.axis_index("kv")
    z, c = me // PAIR, lax.rem(me, PAIR)
    group = lax.axis_index("rep")
    peer = (group, z * PAIR + 1 - c)
    live = pl.ds(A, n.slots)
    half_d = n.d_model // PAIR
    heads_half = n.rep_heads // PAIR

    chips = {step: lax.rem(z + step + n.chips, n.chips) for step in range(-FAR, FAR + 1)}
    rings = {step: (group, PAIR * chips[step] + c) for step in (-1, 1)}
    h_rows = {step: (chips[step] * PAIR + c) * n.seqs for step in chips}

    def along(way, steps):
        return steps if way == A else -steps

    def on_ring(way, steps):
        return rings[along(way, steps)]

    def remote_by(src, dst, send, recv, target):
        return pltpu.make_async_remote_copy(
            src_ref=src, dst_ref=dst, send_sem=send, recv_sem=recv, device_id=target, device_id_type=MESH)

    def remote(src, dst, sems, at, target):
        return remote_by(src, dst, sems.at[(A, *at)], sems.at[(B, *at)], target)

    barrier = pltpu.get_barrier_semaphore()
    others = (peer, *rings.values())
    for target in others:
        pl.semaphore_signal(barrier, inc=1, device_id=target, device_id_type=MESH)
    pl.semaphore_wait(barrier, len(others))

    mine_o, mine_f = at_block(c, n.wide), at_block(c, n.ff_half)
    sources = {
        "q": lambda l: (wq.at[l], wbig.at[pl.ds(A, n.d_model), :]), "k": lambda l: (wk.at[l], wk_v), "v": lambda l: (wv.at[l], wv_v),
        "o": lambda l: (wo.at[l, mine_o, :], wo_v), "u": lambda l: (wu.at[l, :, mine_f], wu_v),
        "d": lambda l: (wd.at[l, mine_f, :], wbig.at[pl.ds(A, n.ff_half), :]),
    }
    follows = {"q": ("d", A), "d": ("q", B)} | {name: (name, B) for name in "kvou"}
    users = {name: PAIR for name in "qkvoud"}
    ready, used = set(), {}

    def load(name, l):
        src, dst = sources[name](l)
        return pltpu.make_async_copy(src, dst, w_sem.at[list(sources).index(name)])

    def need(names, l):
        for name in names:
            if (name, l) not in ready:
                ready.add((name, l))
                load(name, l).wait()

    def release(names, l):
        for name in names:
            used[name, l] = used.get((name, l), A) + 1
            after, more = follows[name]
            if used[name, l] == users[name] and l + more < n.layers:
                load(after, l + more).start()

    def gather(ref_of, sent, got, key):
        def copy(way, hop, half):
            ref = ref_of(along(way, 1 - hop), half)
            return remote_by(ref, ref, sent.at[key], got.at[key, way, hop - 1, half], on_ring(way, 1))

        return copy

    def gather_start(copy):
        for half in BOTH:
            for way in BOTH:
                copy(way, 1, half).start()

    def gather_hop(copy, hop, half, passed_on=None):
        for way in BOTH:
            if takes(way, hop, half):
                copy(way, hop, half).wait_recv()
                if hop < FAR and takes(way, hop + 1, half):
                    copy(way, hop + 1, half).start()
                if passed_on:
                    passed_on(way, hop, half).start()

    def total(src_of, got_of, sent, got, key):
        def copy(way, dist, half):
            return remote_by(
                src_of(along(way, dist), half), got_of(way, dist, half), sent.at[key], got.at[key, way, dist - 1, half],
                on_ring(way, 1))

        return copy

    def total_start(copy):
        for way in BOTH:
            copy(way, FAR, way).start()
        for way in BOTH:
            copy(way, FAR - 1, 1 - way).start()

    def total_hop(copy, add, dist, way, half):
        copy(way, dist, half).wait_recv()
        add(along(way, dist - 1), way, dist, half)
        if dist > 1:
            copy(way, dist - 1, half).start()

    ring_copies = len(taken())

    def all_sent(ref, sem):
        remote_by(ref, ref, sem, sem, peer).wait_send()

    def block(t, step, half):
        return h_all.at[t, pl.ds(pl.multiple_of(h_rows[step], n.seqs), n.seqs), pl.ds(half * half_d, half_d)]

    ag_copies = [gather(lambda step, half, t=t: block(t, step, half), ag_sent, ag_got, t) for t in BOTH]

    def to_peer(t):
        def copy(way, hop, half):
            ref = block(t, along(way, -hop), half)
            return remote(ref, ref, dd_sem, (t,), peer)

        return copy

    def ag_start(l, t):
        gather_start(ag_copies[t])
        for half in BOTH:
            to_peer(t)(A, A, half).start()

    def ag_hop(t, hop, half):
        gather_hop(ag_copies[t], hop, half, to_peer(t))

    def ag_finish(t):
        blocks = ring_copies // PAIR
        from_peer = h_all.at[t, pl.ds(A, (blocks + 1) * n.seqs), :]
        remote(from_peer, from_peer, dd_sem, (t,), peer).wait()
        all_sent(h_all.at[t, pl.ds(A, blocks * n.seqs), :], ag_sent.at[t])

    stats = pl.ds(n.sub, SUB)
    top_rows = lax.broadcasted_iota(I32, (SUB, LANES), A) < heads_half
    rs_copies = [
        total(lambda step, half, t=t: pd.at[t, chips[step], half], lambda way, d, half, t=t: rd.at[t, way, d - 1, half], rs_sent, rs_got, t)
        for t in BOTH
    ]

    def merge(t):
        def add(step, way, d, half):
            got, mine = rd.at[t, way, d - 1, half], pd.at[t, chips[step], half]
            s1, s2 = got[stats, :], mine[stats, :]
            m = jnp.maximum(s1, s2)
            a1, a2 = jnp.exp(s1 - m), jnp.exp(s2 - m)
            mine[stats, :] = jnp.where(top_rows, m, pltpu.roll(a1, heads_half, A) * s1 + pltpu.roll(a2, heads_half, A) * s2)
            at = pl.ds(A, n.sub)
            by_head = (heads_half, n.head, LANES)
            a1, a2 = (a[:heads_half][:, None] for a in (a1, a2))
            mine[at, :] = (a1 * got[at, :].reshape(by_head) + a2 * mine[at, :].reshape(by_head)).reshape(n.sub, LANES)

        return add

    def select(l, t):
        ag_finish(t)

        def body(i):
            cols = at_block(i, n.s_cols)
            hsel[:, cols] = dot(oh_ref[live, :], h_all[t, :, cols]).astype(BF16)

        loop(n.d_model // n.s_cols, body)

    def turned(w):
        rows = dot(hsel[...], w).astype(BF16).astype(F32)
        return jnp.concatenate([rows, jnp.zeros((LANES - n.slots, rows.shape[B]), F32)], axis=A).T

    units = (PAIR * (1 - c), PAIR * (1 - c) + 1, PAIR * c)
    spread_head = PAIR * c + 1
    first_part = LANES - n.slots

    def packed(u, own, other):
        rest = (other[..., :first_part], other[..., first_part:], own[..., n.slots :])[u]
        if rest.shape[-1] < first_part:
            pad = jnp.zeros((*own.shape[:-1], first_part - rest.shape[-1]), own.dtype)
            rest = jnp.concatenate([rest, pad], axis=-1) if rest.shape[-1] else pad
        return jnp.concatenate([own, rest], axis=-1)

    def project(l, t):
        need("qkv", l)

        def query(kvh):
            return turned(wbig[pl.ds(A, n.d_model), at_block(kvh, n.own_rows)])

        other = query(spread_head)[:, : n.slots]
        for u, kvh in enumerate(units):
            q_ref[u] = packed(u, query(kvh)[:, : n.slots], other)
        for i, w in enumerate((wk_v, wv_v)):
            kn_ref[t, i] = turned(w[...])
            knew_ref[l, t, i] = kn_ref[t, i].astype(BF16)
            for u, kvh in enumerate(units):
                own, other = (kn_ref[t, i, at_block(head, n.head), live] for head in (kvh, spread_head))
                kn_p[t, i, at_block(u, n.head), :] = packed(u, own, other)
        release("qkv", l)

    def attend(t, u):
        rows = at_block(u, n.head)
        scale = n.head ** -0.5
        out = oa.at[t, jnp.where(u < PAIR, 1 - c, c), jnp.where(u < PAIR, u, A)]
        heads = range(n.rep_heads)

        def pages(w, at):
            return kv_p[w, at, rows, :].astype(F32)

        def scores(keys):
            parts = []
            for h in heads:
                prods = q_ref[u, pl.ds(h * n.head, n.head), :][None] * keys
                acc = prods[:, :SUB]
                for d in range(SUB, n.head, SUB):
                    acc = acc + prods[:, d : d + SUB]
                parts.append(acc)
            return sums_to_rows(parts)

        def qk(i):
            at = pl.ds(i * FAR, FAR)
            s_ref[at, :, :] = scores(pages(A, at))

        loop(n.page // FAR, qk)
        fresh = range(t + 1)
        news = [scores(kn_p[i, A, rows, :][None])[A] for i in fresh]
        lim, has_new = lane_ref[pl.ds(PAIR * u, 1), :], lane_ref[pl.ds(PAIR * u + 1, 1), :] > 0
        news = [jnp.where(has_new, s * scale, NEG) for s in news]
        valid = lax.broadcasted_iota(I32, (n.page, n.rep_heads, lim.shape[B]), A) < lim[None]
        old = jnp.where(valid, s_ref[:, :, :] * scale, NEG)
        m = jnp.max(old, axis=A)
        for s in news:
            m = jnp.maximum(m, s)
        probs = jnp.where(valid, jnp.exp(old - m[None]), 0.0)
        s_ref[:, :, :] = probs
        news = [jnp.where(has_new, jnp.exp(s - m), 0.0) for s in news]
        count = jnp.sum(probs, axis=A)
        for p in news:
            count = count + p
        out[pl.ds(n.own_rows, SUB), :] = m
        out[pl.ds(n.own_rows + SUB, SUB), :] = count
        vals = [kn_p[i, B, rows, :] for i in fresh]
        for h in heads:
            acc = news[A][h : h + 1] * vals[A]
            for p, v in zip(news[1:], vals[1:], strict=True):
                acc = acc + p[h : h + 1] * v
            out[pl.ds(h * n.head, n.head), :] = acc

        def pv(i):
            vals = [v for v in pages(B, pl.ds(i * FAR, FAR))]
            ps = [s_ref[i * FAR + j, :, :] for j in range(FAR)]
            for h in heads:
                at = pl.ds(h * n.head, n.head)
                acc = out[at, :]
                for p, v in zip(ps, vals, strict=True):
                    acc = acc + p[h : h + 1] * v
                out[at, :] = acc

        loop(n.page // FAR, pv)

    def exchange(t):
        return remote(oa.at[t, 1 - c], ob.at[t], x_sem, (t,), peer)

    def attend_all(l, t, between):
        def body(u):
            attend(t, u)
            pl.when(u == B)(lambda: exchange(t).start())
            for at, work in between.items():
                pl.when(u == at)(work)

        loop(len(units), body)
        lane = lax.broadcasted_iota(I32, (1, LANES), B)
        near, far = (pltpu.roll(oa[t, 1 - c, v], first_part * (v + 1), B) for v in BOTH)
        oa[t, c, B] = jnp.where(lane < first_part, near, far)

    low_lanes = lax.broadcasted_iota(I32, (1, LANES), B) < n.pair

    def by_chip(parts, put):
        for zp in range(n.chips // PAIR):
            a, b = (p[:, zp * LANES : (zp + 1) * LANES] for p in parts)
            put(PAIR * zp, jnp.where(low_lanes, a, pltpu.roll(b, n.pair, B)))
            put(PAIR * zp + 1, jnp.where(low_lanes, pltpu.roll(a, n.pair, B), b))

    def scatter(l, t):
        exchange(t).wait()

        def both_cores(hh, at):
            return jnp.concatenate([oa[t, c, hh, at, :], ob[t, hh, at, :]], axis=B)

        top, count = (
            jnp.concatenate([both_cores(hh, pl.ds(n.own_rows + off, SUB)) for hh in BOTH], axis=A) for off in (A, SUB))
        m_page = [jnp.where(pres_ref[pl.ds(p, 1), :] > 0, exact_dot(top, e_ref[p]), NEG) for p in BOTH]
        m_seq = jnp.maximum(*m_page)
        a = jnp.exp(jnp.minimum(top - exact_dot(m_seq, es_ref[...], right=B), 0.0))
        a_ref[A], a_ref[B] = a[:SUB], a[SUB:]
        l_seq = exact_dot(count * a, es_ref[...])
        dense = {}
        for what, v in enumerate((m_seq, l_seq)):
            by_chip([v[:SUB], v[SUB:]], lambda zz, v, what=what: dense.update({(zz, what): v}))
        for zz in range(n.chips):
            m, l = dense[zz, A], dense[zz, B]
            pd[t, zz, A, stats, :] = jnp.where(top_rows, m, pltpu.roll(l, heads_half, A))
            pd[t, zz, B, stats, :] = jnp.where(top_rows, pltpu.roll(m, heads_half, A), l)

        def body(i):
            for half in BOTH:
                h = half * heads_half + i
                parts = [
                    exact_dot(both_cores(hh, at_block(h, n.head)) * a_ref[hh, pl.ds(h, 1), :], es_ref[...]) for hh in BOTH]

                def put(zz, v, half=half):
                    pd[t, zz, half, at_block(i, n.head), :] = v

                by_chip(parts, put)

        loop(heads_half, body)

    def f_copy(t, stage):
        return remote(pf.at[t, 1 - c], rf.at[t, stage], f_sem, (t, stage), peer)

    def m_copy(t):
        return remote(hm.at[t, c], hm.at[t, c], m_sem, (t,), peer)

    def product(t, lhs, w):
        def body(i):
            cols = at_block(i, n.d_cols)
            val = dot(lhs(), w(cols))
            pf[t, A, :, cols] = val[: n.seqs]
            pf[t, B, :, cols] = val[n.seqs :]

        loop(n.d_model // n.d_cols, body)

    own = pl.ds(pl.multiple_of(h_rows[A], n.seqs), n.seqs)

    def out_proj(l, t):
        all_sent(pd.at[t, pl.ds(A, ring_copies // PAIR)], rs_sent.at[t])
        for half in BOTH:
            mine = pd.at[t, z, half]
            inv = (1.0 / mine[stats, :])[heads_half:][:, None]
            flat = (mine[pl.ds(A, n.sub), :].reshape(heads_half, n.head, LANES) * inv).reshape(n.sub, LANES).T.astype(BF16)
            for hh in BOTH:
                olhs[:, pl.ds(hh * n.own_rows + half * n.sub, n.sub)] = flat[hh * n.pair : (hh + 1) * n.pair]
        need("o", l)
        product(t, lambda: olhs[...], lambda cols: wo_v[:, cols])
        release("o", l)
        f_copy(t, A).start()

    def mid(l, t):
        f_copy(t, A).wait()
        hm[t, c] = (h_all[t, own, :].astype(F32) + (pf[t, c] + rf[t, A])).astype(BF16)
        m_copy(t).start()

    def up(l, t, halfway):
        m_copy(t).wait()
        need("u", l)

        def body(i):
            cols = at_block(i, n.u_cols)
            u = dot(hm[t].reshape(n.pair, n.d_model), wu_v[:, cols]).astype(BF16).astype(F32)
            act[t, :, cols] = jax.nn.gelu(u, approximate=True).astype(BF16)
            for at, work in halfway.items():
                pl.when(i == at)(work)

        loop(n.ff_half // n.u_cols, body)
        release("u", l)

    def down(l, t):
        need("d", l)
        product(t, lambda: act[t], lambda cols: wbig[pl.ds(A, n.ff_half), cols])
        release("d", l)
        f_copy(t, B).start()

    def new_h(l, t):
        f_copy(t, B).wait()
        new = (hm[t, c].astype(F32) + (pf[t, c] + rf[t, B])).astype(BF16)
        h_all[t, own, :] = new
        y_ref[t] = new

    def ids_of(dev, axis):
        at = lax.broadcasted_iota(I32, (LANES, 1) if axis == A else (1, LANES), axis)
        return jnp.where(at < n.slots, dev * n.slots + at, -1)

    def tables():
        oa[...] = jnp.zeros_like(oa)
        for g, dev in enumerate((me, z * PAIR + 1 - c)):
            ids = ids_of(dev, A)
            target = ids
            for e in range(n.entries):
                target = jnp.where(ids == src_ref[e], dst_ref[e], target)
            stale = mask_rows(ids, dst_ref)
            hit = [jnp.where(tab_ref[pl.ds(p, 1), :] == target, 1.0, 0.0) for p in BOTH]
            now = [jnp.where(stale == 0, h, 0.0) for h in hit]
            at = pl.ds(g * LANES, LANES)
            for p in BOTH:
                e_ref[p, at, :] = now[p].astype(BF16)
            es_ref[at, :] = (now[A] + now[B]).astype(BF16)
            if g == A:
                oh_ref[...] = (hit[A] + hit[B]).astype(BF16)
                held = [h.astype(BF16) for h in (*now, hit[B])]
        for p in BOTH:
            pres_ref[pl.ds(p, 1), :] = jnp.sum(e_ref[p].astype(F32), axis=A, keepdims=True)
        lens = len_ref[...].astype(F32)
        rows = jnp.concatenate([lens, jnp.ones((SUB - 1, lens.shape[B]), F32)], axis=A).astype(BF16)
        first, last, fresh = (dot_by(rows, h, B, B) for h in held)
        at0, at1 = slice(A, 1), slice(B, PAIR)
        limit = jnp.where(first[at1] > 0, jnp.minimum(first[at0], n.page), jnp.where(last[at1] > 0, last[at0] - n.page, 0.0))
        for i, row in enumerate((limit, last[at1])):
            row = row[:, : n.slots]
            for u in range(len(units)):
                lane_ref[pl.ds(PAIR * u + i, 1), :] = packed(u, row, row).astype(I32)
        ids = ids_of(me, B)
        is_src, is_dst = mask_rows(ids, src_ref), mask_rows(ids, dst_ref)
        pick_ref[...] = placed(ids[:, : n.slots], src_ref, n.slots)
        on_last = jnp.where(is_src == 0, fresh[at1], 0.0) > 0
        start = fresh[at0] - n.page
        vec_ref[...] = jnp.where(is_src + is_dst == 0, 1.0, 0.0) * jnp.ones((SUB, LANES), F32)
        for t in BOTH:
            vec_ref[pl.ds(t, 1), :] = jnp.where(on_last, start + t, -1.0)

    m_cols = mf.shape[B] // n.chips // PAIR

    def mig_pair():
        return remote(mg.at[1 - c], mx, gp_sem, (), peer)

    def m_at(step, half):
        return at_block(chips[step] * PAIR + half, m_cols)

    ms_copies, mg_copies = [], []
    for l in range(n.layers):
        ms_copies.append(total(lambda step, half: mg.at[c, :, m_at(step, half)], lambda way, d, half: mr.at[way, d - 1, half], gs_sent, gs_got, l))
        mg_copies.append(gather(lambda step, half: mf.at[:, m_at(step, half)], gg_sent, gg_got, l))

    def mig_add(step, way, d, half):
        at = m_at(step, half)
        mg[c, :, at] = mg[c, :, at] + mr[way, d - 1, half]

    m_ring = pl.ds(A, ring_copies * m_cols)

    def mig_sent(l):
        all_sent(mg.at[c, :, m_ring], gs_sent.at[l])

    def mig_out_copies(l):
        return remote(mf, mig_out.at[l, c], go_sem, (l,), peer), pltpu.make_async_copy(mf, mig_out.at[l, c], go_sem.at[PAIR, l])

    def page_loads(l, i, slot):
        at = pl.ds(pl.multiple_of(i * SUB, SUB), SUB)
        return [pltpu.make_async_copy(pool.at[l, at], raw.at[slot, w], p_sem.at[slot, w]) for w, pool in enumerate((kp, vp))]

    def first_pages(l):
        for i in range(raw.shape[A]):
            for copy in page_loads(l, i, i):
                copy.start()

    def extract(l):
        if l > 0:
            mig_sent(l - 1)
        chunks, held = n.page // SUB, raw.shape[A]

        def body(i):
            slot = lax.rem(i, held)
            for copy in page_loads(l, i, slot):
                copy.wait()
            at = pl.ds(pl.multiple_of(i * SUB, SUB), SUB)
            for w in BOTH:
                rows = raw[slot, w].reshape(SUB * n.kv_cols, n.slots)
                mg[w, :, at_block(i, SUB * n.kv_cols)] = dot_by(pick_ref[...], rows, B, B).astype(BF16)
                other = raw[slot, w, :, at_block(spread_head, n.head), :]
                for u, kvh in enumerate(units):
                    kv_p[w, at, at_block(u, n.head), :] = packed(u, raw[slot, w, :, at_block(kvh, n.head), :], other)

            @pl.when(i + held < chunks)
            def _():
                for copy in page_loads(l, i + held, slot):
                    copy.start()

        loop(chunks, body)
        if l + 1 < n.layers:
            first_pages(l + 1)
        mig_pair().start()

    def mig_start(l):
        if l > 0:
            for copy in mig_out_copies(l - 1):
                copy.wait()
        mig_pair().wait()
        mg[c] = mg[c] + mx[...]
        total_start(ms_copies[l])

    def mig_gather(l):
        gather_start(mg_copies[l])

    def mig_own():
        for half in BOTH:
            mf[:, m_at(A, half)] = mg[c, :, m_at(A, half)]

    def mig_end(l):
        all_sent(mf.at[:, m_ring], gg_sent.at[l])
        for copy in mig_out_copies(l):
            copy.start()

    steps = {"TAB": tables}
    for l in range(n.layers):
        steps[f"EXT{l}"] = functools.partial(extract, l)
        steps[f"MS{l}s"] = functools.partial(mig_start, l)
        steps[f"MG{l}s"] = functools.partial(mig_gather, l)
        for hop in HOPS:
            for half in BOTH:
                steps[f"MG{l}h{hop}{half}"] = functools.partial(gather_hop, mg_copies[l], hop, half)
                for way in BOTH:
                    steps[f"MS{l}k{hop}{way}{half}"] = functools.partial(total_hop, ms_copies[l], mig_add, hop, way, half)
        for t in BOTH:
            for name, work in (
                ("SEL", select), ("PROJ", project), ("SCAT", scatter), ("FO", out_proj), ("MID", mid), ("DOWN", down), ("NEWH", new_h),
            ):
                steps[f"{name}{l}{t}"] = functools.partial(work, l, t)
            steps[f"AG{l}{t}s"] = functools.partial(ag_start, l, t)
            steps[f"RS{l}{t}s"] = functools.partial(total_start, rs_copies[t])
            for hop in HOPS:
                for half in BOTH:
                    steps[f"AG{l}{t}h{hop}{half}"] = functools.partial(ag_hop, t, hop, half)
                    for way in BOTH:
                        steps[f"RS{l}{t}k{hop}{way}{half}"] = functools.partial(total_hop, rs_copies[t], merge(t), hop, way, half)

    first_pages(A)
    for name in ("q", "k", "v", "o", "u"):
        load(name, A).start()
    for t in BOTH:
        h_all[t, own, :] = x_ref[t]

    todo = list(ORDER)
    on_way = {kind: len([name for name in todo if name.startswith(kind)]) for l in range(n.layers) for kind in (f"MS{l}k", f"MG{l}h")}

    def run(names):
        for name in names:
            steps[name]()
            kind = name[:FAR]
            if kind in on_way:
                on_way[kind] -= 1
                if on_way[kind] == 0:
                    mig_end(int(kind[PAIR])) if "h" in kind else mig_own()

    loops = {"ATT": (attend_all, len(units)), "UP": (up, n.ff_half // n.u_cols)}
    while todo:
        name = todo.pop(A)
        word = name.rstrip("0123456789")
        if word in loops:
            work, count = loops[word]
            l, t, _ = (int(ch) for ch in name[len(word) :])
            between = {}
            for i in range(count - 1):
                upto = todo.index(f"{word}{l}{t}{i + 1}")
                if upto:
                    between[i] = functools.partial(run, todo[:upto])
                todo = todo[upto + 1 :]
            work(l, t, between)
        else:
            run([name])
    for copy in mig_out_copies(n.layers - 1):
        copy.wait()
    mig_sent(n.layers - 1)


def pool_kernel(dst_ref, vec_ref, mig_ref, new_ref, y_ref, k_ref, v_ref, ko_ref, vo_ref, yo_ref, moved, move_ref):
    step, rows, slots = k_ref.shape[1:]
    live = slice(A, slots)
    group = moved.shape[1] // rows
    tab = vec_ref[...]
    at0, at1, keep = (tab[i : i + 1, live].astype(BF16) for i in range(PAIR + 1))
    keep = keep > 0
    base = pl.program_id(B) * step
    turns = [(which, g) for which in BOTH for g in range(step // group)]

    @pl.when((pl.program_id(A) == 0) & (pl.program_id(B) == 0))
    def _():
        yo_ref[...] = y_ref[...]
        ids = lax.axis_index("kv") * slots + lax.broadcasted_iota(I32, (1, slots), B)
        move_ref[...] = placed(ids, dst_ref, slots)

    def move(which, g, slot):
        moved[slot] = dot_by(mig_ref[A, which, :, g * group * rows : (g + 1) * group * rows], move_ref[...], A, A).astype(BF16)

    move(A, A, A)
    for i, (which, g) in enumerate(turns):
        if i + 1 < len(turns):
            move(*turns[i + 1], (i + 1) % PAIR)
        pool_ref, out_ref = ((k_ref, ko_ref), (v_ref, vo_ref))[which]
        for j in range(group):
            r = g * group + j
            pos = jnp.full((1, slots), (base + r).astype(F32), F32).astype(BF16)
            val = jnp.where(keep, pool_ref[A, r], moved[i % PAIR, j * rows : (j + 1) * rows, :])
            val = jnp.where(at0 == pos, new_ref[A, A, which, :, live], val)
            out_ref[A, r] = jnp.where(at1 == pos, new_ref[A, B, which, :, live], val)


def new_pools(pools, mig, knew, vec, dst, y):
    layers, page, rows, slots = pools[A].shape
    step, group = page // PAIR, FAR
    entries = mig.shape[PAIR]
    block = pl.BlockSpec((1, step, rows, slots), lambda l, i: (l, i, A, A))
    whole = pl.BlockSpec(y.shape, lambda l, i: (A, A, A))
    return pl.pallas_call(
        pool_kernel,
        out_shape=[jax.ShapeDtypeStruct(pools[A].shape, BF16)] * PAIR + [jax.ShapeDtypeStruct(y.shape, BF16)],
        grid=(layers, page // step),
        in_specs=[
            pl.BlockSpec(memory_space=pltpu.SMEM),
            pl.BlockSpec(vec.shape, lambda l, i: (A, A)),
            pl.BlockSpec((1, PAIR, entries, step * rows), lambda l, i: (l, A, A, i)),
            pl.BlockSpec((1, PAIR, PAIR, rows, LANES), lambda l, i: (l, A, A, A, A)),
            whole, block, block,
        ],
        out_specs=[block, block, whole],
        scratch_shapes=[pltpu.VMEM((PAIR, group * rows, slots), BF16), pltpu.VMEM((entries, slots), BF16)],
        compiler_params=pltpu.CompilerParams(dimension_semantics=("arbitrary",) * PAIR, vmem_limit_bytes=VMEM_BYTES),
        name="new_pools",
    )(dst, vec, mig, knew, y, *pools)


def solution(mesh):
    devs = mesh.shape["kv"]
    pool_spec = P(("rep", "kv"))
    tok_spec = P(None, ("rep", "kv"), None)

    def device_fn(embeds, w_query, w_key, w_value, w_out, w_up, w_down, k_pool, v_pool, new_table, seq_lens, mig_src, mig_dst):
        slots, layers, page, kv_heads, head = k_pool.shape
        seqs, d_model = embeds.shape[1:]
        rep_heads = w_query.shape[-1] // head // kv_heads
        own_rows = rep_heads * head
        n = SimpleNamespace(
            layers=layers, d_model=d_model, ff_half=w_up.shape[-1] // PAIR, chips=devs // PAIR, seqs=seqs, pair=PAIR * seqs,
            slots=slots, kv_heads=kv_heads, head=head, page=page, rep_heads=rep_heads, own_rows=own_rows, sub=own_rows // PAIR,
            wide=kv_heads // PAIR * own_rows, kv_cols=kv_heads * head, entries=mig_src.shape[A],
            s_cols=d_model // PAIR, d_cols=d_model // FAR, u_cols=w_up.shape[-1] // FAR)
        total = seqs * devs
        pages = page * n.kv_cols
        pools = [jnp.moveaxis(p, A, -1).reshape(layers, page, n.kv_cols, slots) for p in (k_pool, v_pool)]
        dma, two = pltpu.SemaphoreType.DMA, PAIR
        ring = (two, FAR, two)
        bf = lambda *shape: pltpu.VMEM(shape, BF16)
        f32 = lambda *shape: pltpu.VMEM(shape, F32)
        hbm, vmem, smem = (pl.BlockSpec(memory_space=m) for m in (pl.ANY, pltpu.VMEM, pltpu.SMEM))
        y, knew, vec, mig = pl.pallas_call(
            functools.partial(main_kernel, n),
            out_shape=[
                jax.ShapeDtypeStruct((two, seqs, d_model), BF16),
                jax.ShapeDtypeStruct((layers, two, two, n.kv_cols, LANES), BF16),
                jax.ShapeDtypeStruct((SUB, LANES), F32),
                jax.ShapeDtypeStruct((layers, two, n.entries, pages), BF16),
            ],
            in_specs=[smem] * two + [vmem] * (two + 1) + [hbm] * SUB,
            out_specs=[vmem] * (two + 1) + [hbm],
            scratch_shapes=[
                bf(LANES, total), bf(two, two * LANES, total), bf(two * LANES, total), f32(SUB, total), pltpu.VMEM((SUB, LANES), I32),
                bf(n.entries, slots), bf(two, n.entries, pages), bf(n.entries, pages),
                bf(two, FAR, two, n.entries, pages // devs), bf(n.entries, pages),
                bf(two, total, d_model), bf(slots, d_model), bf(max(d_model, n.ff_half), d_model), bf(d_model, n.kv_cols),
                bf(d_model, n.kv_cols), bf(n.wide, d_model), bf(d_model, n.ff_half), bf(two + 1, two, SUB, n.kv_cols, slots), bf(two, page, (kv_heads - 1) * head, LANES),
                f32(kv_heads - 1, own_rows, LANES), f32(two, two, n.kv_cols, LANES), f32(two, two, (kv_heads - 1) * head, LANES), f32(page, rep_heads, LANES),
                f32(two, two, two, own_rows + two * SUB, LANES), f32(two, two, own_rows + two * SUB, LANES),
                f32(two, rep_heads, two * LANES), f32(two, n.chips, two, n.sub + SUB, LANES),
                f32(two, two, FAR, two, n.sub + SUB, LANES), bf(n.pair, n.wide), f32(two, two, seqs, d_model),
                f32(two, two, seqs, d_model), bf(two, two, seqs, d_model), bf(two, n.pair, n.ff_half),
                dma((two,)), dma((two, *ring)), dma((two, two)), dma((two,)), dma((two, *ring)), dma((two, two)),
                dma((two, two, two)), dma((two, two)), dma((layers,)), dma((layers, *ring)), dma((layers,)), dma((layers, *ring)),
                dma((two,)), dma((two + 1, layers)), dma((two + 1, two)), dma((SUB,)),
            ],
            compiler_params=pltpu.CompilerParams(collective_id=A, has_side_effects=True, vmem_limit_bytes=VMEM_BYTES),
            name="decode",
        )(mig_src, mig_dst, new_table.T, seq_lens[None], embeds, w_query, w_key, w_value, w_out, w_up, w_down, *pools)
        *outs, y = new_pools(pools, mig, knew, vec, mig_dst, y)
        outs = [jnp.moveaxis(p.reshape(layers, page, kv_heads, head, slots), -1, A) for p in outs]
        return y, *outs

    return jax.shard_map(
        device_fn, mesh=mesh,
        in_specs=(tok_spec, *(P(),) * (SUB - PAIR), pool_spec, pool_spec, P("rep", None), *(P("rep"),) * (FAR - 1)),
        out_specs=(tok_spec, pool_spec, pool_spec), check_vma=False)
```

```python
import functools
from types import SimpleNamespace

import jax
import jax.numpy as jnp
from jax import lax
from jax.experimental import pallas as pl
from jax.experimental.pallas import tpu as pltpu
from jax.sharding import PartitionSpec as P

MESH = pl.DeviceIdType.MESH
F32, BF16, I32 = jnp.float32, jnp.bfloat16, jnp.int32
NEG = -1e30
LANES = 128
SUB = 8
A, B = BOTH = range(2)
PAIR = len(BOTH)
VMEM_BYTES = 67043328
FAR = 4
HOPS = range(1, FAR + 1)


class Names:
    def __getattr__(self, name):
        return name


W = Names()
ORDER = (
    W.AG00s, W.AG01s, W.TAB, W.EXT0, W.AG00h10, W.AG00h11, W.AG01h10, W.AG01h11, W.AG00h20, W.AG00h21, W.AG01h20,
    W.AG01h21, W.AG00h30, W.AG00h31, W.AG01h30, W.AG01h31, W.AG00h40, W.AG00h41, W.SEL00, W.AG01h40, W.PROJ00,
    W.AG01h41, W.ATT000, W.MS0s, W.ATT001, W.ATT002, W.MS0k400, W.MS0k411, W.MS0k310, W.MS0k301, W.SCAT00, W.RS00s,
    W.SEL01, W.MS0k300, W.MS0k311, W.PROJ01, W.MS0k210, W.MS0k201, W.ATT010, W.RS00k400, W.RS00k310, W.ATT011,
    W.RS00k411, W.RS00k301, W.MS0k200, W.MS0k211, W.ATT012, W.RS00k300, W.RS00k210, W.MS0k110, W.MS0k101, W.SCAT01,
    W.RS00k311, W.RS00k201, W.RS01s, W.MS0k100, W.MS0k111, W.EXT1, W.RS00k200, W.RS00k110, W.RS00k211, W.RS00k101,
    W.RS01k310, W.RS01k400, W.RS01k411, W.RS01k301, W.RS00k111, W.RS00k100, W.FO00, W.RS01k210, W.RS01k300, W.MID00,
    W.UP000, W.UP001, W.RS01k311, W.RS01k201, W.DOWN00, W.RS01k200, W.RS01k110, W.NEWH00, W.AG10s, W.RS01k211,
    W.RS01k101, W.RS01k100, W.AG10h10, W.AG10h11, W.RS01k111, W.FO01, W.AG10h20, W.MID01, W.AG10h21, W.UP010, W.UP011,
    W.AG10h30, W.DOWN01, W.AG10h31, W.NEWH01, W.AG11s, W.AG10h40, W.AG10h41, W.MG0s, W.SEL10, W.AG11h10, W.PROJ10,
    W.AG11h11, W.MG0h10, W.ATT100, W.AG11h20, W.MG0h11, W.ATT101, W.AG11h21, W.MG0h20, W.ATT102, W.AG11h30, W.MG0h21,
    W.SCAT10, W.RS10s, W.AG11h31, W.MG0h30, W.AG11h40, W.MG0h31, W.RS10k400, W.RS10k310, W.RS10k301, W.RS10k411,
    W.MG0h40, W.AG11h41, W.MG0h41, W.MS1s, W.SEL11, W.PROJ11, W.RS10k300, W.RS10k210, W.ATT110, W.RS10k311,
    W.RS10k201, W.MS1k400, W.MS1k310, W.MS1k301, W.ATT111, W.RS10k200, W.RS10k110, W.MS1k411, W.ATT112, W.RS10k211,
    W.RS10k101, W.MS1k300, W.MS1k210, W.SCAT11, W.RS11s, W.MS1k311, W.MS1k201, W.RS10k100, W.MS1k200, W.RS10k111,
    W.FO10, W.MS1k110, W.MID10, W.RS11k400, W.RS11k310, W.UP100, W.UP101, W.RS11k411, W.RS11k301, W.MS1k101, W.DOWN10,
    W.MS1k211, W.MS1k100, W.RS11k210, W.RS11k300, W.NEWH10, W.RS11k311, W.RS11k201, W.MS1k111, W.MG1s, W.RS11k200,
    W.RS11k110, W.RS11k101, W.RS11k211, W.MG1h10, W.MG1h11, W.RS11k100, W.RS11k111, W.FO11, W.MG1h20, W.MG1h21,
    W.MID11, W.UP110, W.MG1h30, W.UP111, W.MG1h31, W.DOWN11, W.MG1h40, W.MG1h41, W.NEWH11,
)


def dot(a, b):
    return jnp.dot(a, b, preferred_element_type=F32)


def dot_by(a, b, left, right):
    return lax.dot_general(a, b, (((left,), (right,)), ((), ())), preferred_element_type=F32)


def exact_dot(x, onehot, right=A):
    high = x.astype(BF16)
    rest = x - high.astype(F32)
    mid = rest.astype(BF16)
    low = (rest - mid.astype(F32)).astype(BF16)
    out = dot_by(jnp.concatenate([high, mid, low], axis=A), onehot, B, right).reshape(FAR - 1, x.shape[A], -1)
    return out[A] + out[B] + out[PAIR]


def sums_to_rows(parts):
    axis = parts[A].ndim - PAIR
    sub = lax.broadcasted_iota(I32, parts[A].shape, axis)
    while len(parts) > 1:
        half = len(parts) // PAIR
        high = (sub & half) != 0
        parts = [
            jnp.where(high, a + pltpu.roll(a, half, axis), b + pltpu.roll(b, SUB - half, axis))
            for a, b in zip(parts[half:], parts[:half], strict=True)
        ]
    return parts[A]


def at_block(i, size):
    return pl.ds(pl.multiple_of(i * size, size), size)


def loop(count, body):
    def step(i, carry):
        body(i)
        return carry

    lax.fori_loop(A, count, step, A)


def takes(way, hop, half):
    return hop < FAR or way == half


def taken(hops=HOPS):
    return [(way, hop, half) for half in BOTH for way in BOTH for hop in hops if takes(way, hop, half)]


def mask_rows(ids, values, shape=None):
    out = jnp.zeros(shape or ids.shape, I32)
    for e in range(values.shape[A]):
        out = jnp.where(ids == values[e], 1, out)
    return out


def placed(ids, values, slots):
    entries = values.shape[A]
    row = lax.broadcasted_iota(I32, (entries, slots), A)
    out = jnp.zeros((entries, slots), F32)
    for e in range(entries):
        out = jnp.where(row == e, jnp.where(ids == values[e], 1.0, 0.0), out)
    return out.astype(BF16)


def main_kernel(
    n,
    src_ref, dst_ref, tab_ref, len_ref, x_ref, wq, wk, wv, wo, wu, wd, kp, vp,
    y_ref, knew_ref, vec_ref, mig_out,
    oh_ref, e_ref, es_ref, pres_ref, lane_ref, pick_ref, mg, mx, mr, mf,
    h_all, hsel, wbig, wk_v, wv_v, wo_v, wu_v, raw, kv_p, q_ref, kn_ref, kn_p, s_ref, oa, ob, a_ref, pd, rd,
    olhs, pf, rf, hm, act, ag_sent, ag_got, dd_sem, rs_sent, rs_got, x_sem, f_sem, m_sem, gs_sent, gs_got, gg_sent, gg_got,
    gp_sem, go_sem, p_sem, w_sem,
):
    me = lax.axis_index("kv")
    z, c = me // PAIR, lax.rem(me, PAIR)
    group = lax.axis_index("rep")
    peer = (group, z * PAIR + 1 - c)
    live = pl.ds(A, n.slots)
    half_d = n.d_model // PAIR
    heads_half = n.rep_heads // PAIR

    chips = {step: lax.rem(z + step + n.chips, n.chips) for step in range(-FAR, FAR + 1)}
    rings = {step: (group, PAIR * chips[step] + c) for step in (-1, 1)}
    h_rows = {step: (chips[step] * PAIR + c) * n.seqs for step in chips}

    def along(way, steps):
        return steps if way == A else -steps

    def on_ring(way, steps):
        return rings[along(way, steps)]

    def remote_by(src, dst, send, recv, target):
        return pltpu.make_async_remote_copy(
            src_ref=src, dst_ref=dst, send_sem=send, recv_sem=recv, device_id=target, device_id_type=MESH)

    def remote(src, dst, sems, at, target):
        return remote_by(src, dst, sems.at[(A, *at)], sems.at[(B, *at)], target)

    mine_o, mine_f = at_block(c, n.wide), at_block(c, n.ff_half)
    sources = {
        "q": lambda l: (wq.at[l], wbig.at[pl.ds(A, n.d_model), :]), "k": lambda l: (wk.at[l], wk_v), "v": lambda l: (wv.at[l], wv_v),
        "o": lambda l: (wo.at[l, mine_o, :], wo_v), "u": lambda l: (wu.at[l, :, mine_f], wu_v),
        "d": lambda l: (wd.at[l, mine_f, :], wbig.at[pl.ds(A, n.ff_half), :]),
    }
    follows = {"q": ("d", A), "d": ("q", B)} | {name: (name, B) for name in "kvou"}
    users = {name: PAIR for name in "qkvoud"}
    ready, used = set(), {}

    def load(name, l):
        src, dst = sources[name](l)
        return pltpu.make_async_copy(src, dst, w_sem.at[list(sources).index(name)])

    def need(names, l):
        for name in names:
            if (name, l) not in ready:
                ready.add((name, l))
                load(name, l).wait()

    def release(names, l):
        for name in names:
            used[name, l] = used.get((name, l), A) + 1
            after, more = follows[name]
            if used[name, l] == users[name] and l + more < n.layers:
                load(after, l + more).start()

    def gather(ref_of, sent, got, key):
        def copy(way, hop, half):
            ref = ref_of(along(way, 1 - hop), half)
            return remote_by(ref, ref, sent.at[key], got.at[key, way, hop - 1, half], on_ring(way, 1))

        return copy

    def gather_start(copy):
        for half in BOTH:
            for way in BOTH:
                copy(way, 1, half).start()

    def gather_hop(copy, hop, half, passed_on=None):
        for way in BOTH:
            if takes(way, hop, half):
                copy(way, hop, half).wait_recv()
                if hop < FAR and takes(way, hop + 1, half):
                    copy(way, hop + 1, half).start()
                if passed_on:
                    passed_on(way, hop, half).start()

    def total(src_of, got_of, sent, got, key):
        def copy(way, dist, half):
            return remote_by(
                src_of(along(way, dist), half), got_of(way, dist, half), sent.at[key], got.at[key, way, dist - 1, half],
                on_ring(way, 1))

        return copy

    def total_start(copy):
        for way in BOTH:
            copy(way, FAR, way).start()
        for way in BOTH:
            copy(way, FAR - 1, 1 - way).start()

    def total_hop(copy, add, dist, way, half):
        copy(way, dist, half).wait_recv()
        add(along(way, dist - 1), way, dist, half)
        if dist > 1:
            copy(way, dist - 1, half).start()

    ring_copies = len(taken())

    def all_sent(ref, sem):
        remote_by(ref, ref, sem, sem, peer).wait_send()

    def block(t, step, half):
        return h_all.at[t, pl.ds(pl.multiple_of(h_rows[step], n.seqs), n.seqs), pl.ds(half * half_d, half_d)]

    ag_copies = [gather(lambda step, half, t=t: block(t, step, half), ag_sent, ag_got, t) for t in BOTH]

    def to_peer(t):
        def copy(way, hop, half):
            ref = block(t, along(way, -hop), half)
            return remote(ref, ref, dd_sem, (t,), peer)

        return copy

    def ag_start(l, t):
        gather_start(ag_copies[t])
        for half in BOTH:
            to_peer(t)(A, A, half).start()

    def ag_hop(t, hop, half):
        gather_hop(ag_copies[t], hop, half, to_peer(t))

    def ag_finish(t):
        blocks = ring_copies // PAIR
        from_peer = h_all.at[t, pl.ds(A, (blocks + 1) * n.seqs), :]
        remote(from_peer, from_peer, dd_sem, (t,), peer).wait()
        all_sent(h_all.at[t, pl.ds(A, blocks * n.seqs), :], ag_sent.at[t])

    stats = pl.ds(n.sub, SUB)
    top_rows = lax.broadcasted_iota(I32, (SUB, LANES), A) < heads_half
    rs_copies = [
        total(lambda step, half, t=t: pd.at[t, chips[step], half], lambda way, d, half, t=t: rd.at[t, way, d - 1, half], rs_sent, rs_got, t)
        for t in BOTH
    ]

    def merge(t):
        def add(step, way, d, half):
            got, mine = rd.at[t, way, d - 1, half], pd.at[t, chips[step], half]
            s1, s2 = got[stats, :], mine[stats, :]
            m = jnp.maximum(s1, s2)
            a1, a2 = jnp.exp(s1 - m), jnp.exp(s2 - m)
            mine[stats, :] = jnp.where(top_rows, m, pltpu.roll(a1, heads_half, A) * s1 + pltpu.roll(a2, heads_half, A) * s2)
            at = pl.ds(A, n.sub)
            by_head = (heads_half, n.head, LANES)
            a1, a2 = (a[:heads_half][:, None] for a in (a1, a2))
            mine[at, :] = (a1 * got[at, :].reshape(by_head) + a2 * mine[at, :].reshape(by_head)).reshape(n.sub, LANES)

        return add

    def select(l, t):
        ag_finish(t)

        def body(i):
            cols = at_block(i, n.s_cols)
            hsel[:, cols] = dot(oh_ref[live, :], h_all[t, :, cols]).astype(BF16)

        loop(n.d_model // n.s_cols, body)

    def turned(w):
        rows = dot(hsel[...], w).astype(BF16).astype(F32)
        return jnp.concatenate([rows, jnp.zeros((LANES - n.slots, rows.shape[B]), F32)], axis=A).T

    units = (PAIR * (1 - c), PAIR * (1 - c) + 1, PAIR * c)
    spread_head = PAIR * c + 1
    first_part = LANES - n.slots

    def packed(u, own, other):
        rest = (other[..., :first_part], other[..., first_part:], own[..., n.slots :])[u]
        if rest.shape[-1] < first_part:
            pad = jnp.zeros((*own.shape[:-1], first_part - rest.shape[-1]), own.dtype)
            rest = jnp.concatenate([rest, pad], axis=-1) if rest.shape[-1] else pad
        return jnp.concatenate([own, rest], axis=-1)

    def project(l, t):
        need("qkv", l)

        def query(kvh):
            return turned(wbig[pl.ds(A, n.d_model), at_block(kvh, n.own_rows)])

        other = query(spread_head)[:, : n.slots]
        for u, kvh in enumerate(units):
            q_ref[u] = packed(u, query(kvh)[:, : n.slots], other)
        for i, w in enumerate((wk_v, wv_v)):
            kn_ref[t, i] = turned(w[...])
            knew_ref[l, t, i] = kn_ref[t, i].astype(BF16)
            for u, kvh in enumerate(units):
                own, other = (kn_ref[t, i, at_block(head, n.head), live] for head in (kvh, spread_head))
                kn_p[t, i, at_block(u, n.head), :] = packed(u, own, other)
        release("qkv", l)

    def attend(t, u):
        rows = at_block(u, n.head)
        scale = n.head ** -0.5
        out = oa.at[t, jnp.where(u < PAIR, 1 - c, c), jnp.where(u < PAIR, u, A)]
        heads = range(n.rep_heads)

        def pages(w, at):
            return kv_p[w, at, rows, :].astype(F32)

        def scores(keys):
            parts = []
            for h in heads:
                prods = q_ref[u, pl.ds(h * n.head, n.head), :][None] * keys
                acc = prods[:, :SUB]
                for d in range(SUB, n.head, SUB):
                    acc = acc + prods[:, d : d + SUB]
                parts.append(acc)
            return sums_to_rows(parts)

        def qk(i):
            at = pl.ds(i * FAR, FAR)
            s_ref[at, :, :] = scores(pages(A, at))

        loop(n.page // FAR, qk)
        fresh = range(t + 1)
        news = [scores(kn_p[i, A, rows, :][None])[A] for i in fresh]
        lim, has_new = lane_ref[pl.ds(PAIR * u, 1), :], lane_ref[pl.ds(PAIR * u + 1, 1), :] > 0
        news = [jnp.where(has_new, s * scale, NEG) for s in news]
        valid = lax.broadcasted_iota(I32, (n.page, n.rep_heads, lim.shape[B]), A) < lim[None]
        old = jnp.where(valid, s_ref[:, :, :] * scale, NEG)
        m = jnp.max(old, axis=A)
        for s in news:
            m = jnp.maximum(m, s)
        probs = jnp.where(valid, jnp.exp(old - m[None]), 0.0)
        s_ref[:, :, :] = probs
        news = [jnp.where(has_new, jnp.exp(s - m), 0.0) for s in news]
        count = jnp.sum(probs, axis=A)
        for p in news:
            count = count + p
        out[pl.ds(n.own_rows, SUB), :] = m
        out[pl.ds(n.own_rows + SUB, SUB), :] = count
        vals = [kn_p[i, B, rows, :] for i in fresh]
        for h in heads:
            acc = news[A][h : h + 1] * vals[A]
            for p, v in zip(news[1:], vals[1:], strict=True):
                acc = acc + p[h : h + 1] * v
            out[pl.ds(h * n.head, n.head), :] = acc

        def pv(i):
            vals = [v for v in pages(B, pl.ds(i * FAR, FAR))]
            ps = [s_ref[i * FAR + j, :, :] for j in range(FAR)]
            for h in heads:
                at = pl.ds(h * n.head, n.head)
                acc = out[at, :]
                for p, v in zip(ps, vals, strict=True):
                    acc = acc + p[h : h + 1] * v
                out[at, :] = acc

        loop(n.page // FAR, pv)

    def exchange(t):
        return remote(oa.at[t, 1 - c], ob.at[t], x_sem, (t,), peer)

    def attend_all(l, t, between):
        def body(u):
            attend(t, u)
            pl.when(u == B)(lambda: exchange(t).start())
            for at, work in between.items():
                pl.when(u == at)(work)

        loop(len(units), body)
        lane = lax.broadcasted_iota(I32, (1, LANES), B)
        near, far = (pltpu.roll(oa[t, 1 - c, v], first_part * (v + 1), B) for v in BOTH)
        oa[t, c, B] = jnp.where(lane < first_part, near, far)

    low_lanes = lax.broadcasted_iota(I32, (1, LANES), B) < n.pair

    def by_chip(parts, put):
        for zp in range(n.chips // PAIR):
            a, b = (p[:, zp * LANES : (zp + 1) * LANES] for p in parts)
            put(PAIR * zp, jnp.where(low_lanes, a, pltpu.roll(b, n.pair, B)))
            put(PAIR * zp + 1, jnp.where(low_lanes, pltpu.roll(a, n.pair, B), b))

    def scatter(l, t):
        exchange(t).wait()

        def both_cores(hh, at):
            return jnp.concatenate([oa[t, c, hh, at, :], ob[t, hh, at, :]], axis=B)

        top, count = (
            jnp.concatenate([both_cores(hh, pl.ds(n.own_rows + off, SUB)) for hh in BOTH], axis=A) for off in (A, SUB))
        m_page = [jnp.where(pres_ref[pl.ds(p, 1), :] > 0, exact_dot(top, e_ref[p]), NEG) for p in BOTH]
        m_seq = jnp.maximum(*m_page)
        a = jnp.exp(jnp.minimum(top - exact_dot(m_seq, es_ref[...], right=B), 0.0))
        a_ref[A], a_ref[B] = a[:SUB], a[SUB:]
        l_seq = exact_dot(count * a, es_ref[...])
        dense = {}
        for what, v in enumerate((m_seq, l_seq)):
            by_chip([v[:SUB], v[SUB:]], lambda zz, v, what=what: dense.update({(zz, what): v}))
        for zz in range(n.chips):
            m, l = dense[zz, A], dense[zz, B]
            pd[t, zz, A, stats, :] = jnp.where(top_rows, m, pltpu.roll(l, heads_half, A))
            pd[t, zz, B, stats, :] = jnp.where(top_rows, pltpu.roll(m, heads_half, A), l)

        def body(k):
            for half in BOTH:
                for j in BOTH:
                    i = k * PAIR + j
                    h = half * heads_half + i
                    parts = [
                        exact_dot(both_cores(hh, at_block(h, n.head)) * a_ref[hh, pl.ds(h, 1), :], es_ref[...]) for hh in BOTH]

                    def put(zz, v, half=half, i=i):
                        pd[t, zz, half, at_block(i, n.head), :] = v

                    by_chip(parts, put)

        loop(heads_half // PAIR, body)

    def f_copy(t, stage):
        return remote(pf.at[t, 1 - c], rf.at[t, stage], f_sem, (t, stage), peer)

    def m_copy(t):
        return remote(hm.at[t, c], hm.at[t, c], m_sem, (t,), peer)

    def product(t, lhs, w):
        def body(i):
            cols = at_block(i, n.s_cols)
            val = dot(lhs(), w(cols))
            pf[t, A, :, cols] = val[: n.seqs]
            pf[t, B, :, cols] = val[n.seqs :]

        loop(n.d_model // n.s_cols, body)

    own = pl.ds(pl.multiple_of(h_rows[A], n.seqs), n.seqs)

    def out_proj(l, t):
        all_sent(pd.at[t, pl.ds(A, ring_copies // PAIR)], rs_sent.at[t])
        for half in BOTH:
            mine = pd.at[t, z, half]
            inv = (1.0 / mine[stats, :])[heads_half:][:, None]
            flat = (mine[pl.ds(A, n.sub), :].reshape(heads_half, n.head, LANES) * inv).reshape(n.sub, LANES).T.astype(BF16)
            for hh in BOTH:
                olhs[:, pl.ds(hh * n.own_rows + half * n.sub, n.sub)] = flat[hh * n.pair : (hh + 1) * n.pair]
        need("o", l)
        product(t, lambda: olhs[...], lambda cols: wo_v[:, cols])
        release("o", l)
        f_copy(t, A).start()

    def mid(l, t):
        f_copy(t, A).wait()
        hm[t, c] = (h_all[t, own, :].astype(F32) + (pf[t, c] + rf[t, A])).astype(BF16)
        m_copy(t).start()

    def up(l, t, halfway):
        m_copy(t).wait()
        need("u", l)

        def body(i):
            cols = at_block(i, n.u_cols)
            u = dot(hm[t].reshape(n.pair, n.d_model), wu_v[:, cols]).astype(BF16).astype(F32)
            act[t, :, cols] = jax.nn.gelu(u, approximate=True).astype(BF16)
            for at, work in halfway.items():
                pl.when(i == at)(work)

        loop(n.ff_half // n.u_cols, body)
        release("u", l)

    def down(l, t):
        need("d", l)
        product(t, lambda: act[t], lambda cols: wbig[pl.ds(A, n.ff_half), cols])
        release("d", l)
        f_copy(t, B).start()

    def new_h(l, t):
        f_copy(t, B).wait()
        new = (hm[t, c].astype(F32) + (pf[t, c] + rf[t, B])).astype(BF16)
        h_all[t, own, :] = new
        y_ref[t] = new

    def ids_of(dev, axis):
        at = lax.broadcasted_iota(I32, (LANES, 1) if axis == A else (1, LANES), axis)
        return jnp.where(at < n.slots, dev * n.slots + at, -1)

    def tables():
        oa[...] = jnp.zeros_like(oa)
        for g, dev in enumerate((me, z * PAIR + 1 - c)):
            ids = ids_of(dev, A)
            target = ids
            for e in range(n.entries):
                target = jnp.where(ids == src_ref[e], dst_ref[e], target)
            stale = mask_rows(ids, dst_ref)
            hit = [jnp.where(tab_ref[pl.ds(p, 1), :] == target, 1.0, 0.0) for p in BOTH]
            now = [jnp.where(stale == 0, h, 0.0) for h in hit]
            at = pl.ds(g * LANES, LANES)
            for p in BOTH:
                e_ref[p, at, :] = now[p].astype(BF16)
            es_ref[at, :] = (now[A] + now[B]).astype(BF16)
            if g == A:
                oh_ref[...] = (hit[A] + hit[B]).astype(BF16)
                held = [h.astype(BF16) for h in (*now, hit[B])]
        for p in BOTH:
            pres_ref[pl.ds(p, 1), :] = jnp.sum(e_ref[p].astype(F32), axis=A, keepdims=True)
        lens = len_ref[...].astype(F32)
        rows = jnp.concatenate([lens, jnp.ones((SUB - 1, lens.shape[B]), F32)], axis=A).astype(BF16)
        first, last, fresh = (dot_by(rows, h, B, B) for h in held)
        at0, at1 = slice(A, 1), slice(B, PAIR)
        limit = jnp.where(first[at1] > 0, jnp.minimum(first[at0], n.page), jnp.where(last[at1] > 0, last[at0] - n.page, 0.0))
        for i, row in enumerate((limit, last[at1])):
            row = row[:, : n.slots]
            for u in range(len(units)):
                lane_ref[pl.ds(PAIR * u + i, 1), :] = packed(u, row, row).astype(I32)
        ids = ids_of(me, B)
        is_src, is_dst = mask_rows(ids, src_ref), mask_rows(ids, dst_ref)
        pick_ref[...] = placed(ids[:, : n.slots], src_ref, n.slots)
        on_last = jnp.where(is_src == 0, fresh[at1], 0.0) > 0
        start = fresh[at0] - n.page
        vec_ref[...] = jnp.where(is_src + is_dst == 0, 1.0, 0.0) * jnp.ones((SUB, LANES), F32)
        for t in BOTH:
            vec_ref[pl.ds(t, 1), :] = jnp.where(on_last, start + t, -1.0)

    m_cols = mf.shape[B] // n.chips // PAIR

    def mig_pair():
        return remote(mg.at[1 - c], mx, gp_sem, (), peer)

    def m_at(step, half):
        return at_block(chips[step] * PAIR + half, m_cols)

    ms_copies, mg_copies = [], []
    for l in range(n.layers):
        ms_copies.append(total(lambda step, half: mg.at[c, :, m_at(step, half)], lambda way, d, half: mr.at[way, d - 1, half], gs_sent, gs_got, l))
        mg_copies.append(gather(lambda step, half: mf.at[:, m_at(step, half)], gg_sent, gg_got, l))

    def mig_add(step, way, d, half):
        at = m_at(step, half)
        mg[c, :, at] = mg[c, :, at] + mr[way, d - 1, half]

    m_ring = pl.ds(A, ring_copies * m_cols)

    def mig_sent(l):
        all_sent(mg.at[c, :, m_ring], gs_sent.at[l])

    def mig_out_copies(l):
        return remote(mf, mig_out.at[l, c], go_sem, (l,), peer), pltpu.make_async_copy(mf, mig_out.at[l, c], go_sem.at[PAIR, l])

    def page_loads(l, i, slot):
        at = pl.ds(pl.multiple_of(i * SUB, SUB), SUB)
        return [pltpu.make_async_copy(pool.at[l, at], raw.at[slot, w], p_sem.at[slot, w]) for w, pool in enumerate((kp, vp))]

    def first_pages(l):
        for i in range(raw.shape[A]):
            for copy in page_loads(l, i, i):
                copy.start()

    def extract(l):
        if l > 0:
            mig_sent(l - 1)
        chunks, held = n.page // SUB, raw.shape[A]

        def body(i):
            slot = lax.rem(i, held)
            for copy in page_loads(l, i, slot):
                copy.wait()
            at = pl.ds(pl.multiple_of(i * SUB, SUB), SUB)
            for w in BOTH:
                rows = raw[slot, w].reshape(SUB * n.kv_cols, n.slots)
                mg[w, :, at_block(i, SUB * n.kv_cols)] = dot_by(pick_ref[...], rows, B, B).astype(BF16)
                other = raw[slot, w, :, at_block(spread_head, n.head), :]
                for u, kvh in enumerate(units):
                    kv_p[w, at, at_block(u, n.head), :] = packed(u, raw[slot, w, :, at_block(kvh, n.head), :], other)

            @pl.when(i + held < chunks)
            def _():
                for copy in page_loads(l, i + held, slot):
                    copy.start()

        loop(chunks, body)
        if l + 1 < n.layers:
            first_pages(l + 1)
        mig_pair().start()

    def mig_start(l):
        if l > 0:
            for copy in mig_out_copies(l - 1):
                copy.wait()
        mig_pair().wait()
        mg[c] = mg[c] + mx[...]
        total_start(ms_copies[l])

    def mig_gather(l):
        gather_start(mg_copies[l])

    def mig_own():
        for half in BOTH:
            mf[:, m_at(A, half)] = mg[c, :, m_at(A, half)]

    def mig_end(l):
        all_sent(mf.at[:, m_ring], gg_sent.at[l])
        for copy in mig_out_copies(l):
            copy.start()

    steps = {"TAB": tables}
    for l in range(n.layers):
        steps[f"EXT{l}"] = functools.partial(extract, l)
        steps[f"MS{l}s"] = functools.partial(mig_start, l)
        steps[f"MG{l}s"] = functools.partial(mig_gather, l)
        for hop in HOPS:
            for half in BOTH:
                steps[f"MG{l}h{hop}{half}"] = functools.partial(gather_hop, mg_copies[l], hop, half)
                for way in BOTH:
                    steps[f"MS{l}k{hop}{way}{half}"] = functools.partial(total_hop, ms_copies[l], mig_add, hop, way, half)
        for t in BOTH:
            for name, work in (
                ("SEL", select), ("PROJ", project), ("SCAT", scatter), ("FO", out_proj), ("MID", mid), ("DOWN", down), ("NEWH", new_h),
            ):
                steps[f"{name}{l}{t}"] = functools.partial(work, l, t)
            steps[f"AG{l}{t}s"] = functools.partial(ag_start, l, t)
            steps[f"RS{l}{t}s"] = functools.partial(total_start, rs_copies[t])
            for hop in HOPS:
                for half in BOTH:
                    steps[f"AG{l}{t}h{hop}{half}"] = functools.partial(ag_hop, t, hop, half)
                    for way in BOTH:
                        steps[f"RS{l}{t}k{hop}{way}{half}"] = functools.partial(total_hop, rs_copies[t], merge(t), hop, way, half)

    for t in BOTH:
        h_all[t, own, :] = x_ref[t]
    first_pages(A)
    load("q", A).start()
    barrier = pltpu.get_barrier_semaphore()
    others = (peer, *rings.values())
    for target in others:
        pl.semaphore_signal(barrier, inc=1, device_id=target, device_id_type=MESH)
    pl.semaphore_wait(barrier, len(others))

    def later_loads():
        for name in ("k", "v", "o", "u"):
            load(name, A).start()


    steps["LOADS"] = later_loads
    todo = list(ORDER)
    todo.insert(PAIR, "LOADS")
    on_way = {kind: len([name for name in todo if name.startswith(kind)]) for l in range(n.layers) for kind in (f"MS{l}k", f"MG{l}h")}

    def run(names):
        for name in names:
            steps[name]()
            kind = name[:FAR]
            if kind in on_way:
                on_way[kind] -= 1
                if on_way[kind] == 0:
                    mig_end(int(kind[PAIR])) if "h" in kind else mig_own()

    loops = {"ATT": (attend_all, len(units)), "UP": (up, n.ff_half // n.u_cols)}
    while todo:
        name = todo.pop(A)
        word = name.rstrip("0123456789")
        if word in loops:
            work, count = loops[word]
            l, t, _ = (int(ch) for ch in name[len(word) :])
            between = {}
            for i in range(count - 1):
                upto = todo.index(f"{word}{l}{t}{i + 1}")
                if upto:
                    between[i] = functools.partial(run, todo[:upto])
                todo = todo[upto + 1 :]
            work(l, t, between)
        else:
            run([name])
    for copy in mig_out_copies(n.layers - 1):
        copy.wait()
    mig_sent(n.layers - 1)


def pool_kernel(dst_ref, vec_ref, mig_ref, new_ref, y_ref, k_ref, v_ref, ko_ref, vo_ref, yo_ref, moved, move_ref):
    step, rows, slots = k_ref.shape[1:]
    live = slice(A, slots)
    group = moved.shape[1] // rows
    tab = vec_ref[...]
    at0, at1, keep = (tab[i : i + 1, live].astype(BF16) for i in range(PAIR + 1))
    keep = keep > 0
    base = pl.program_id(B) * step
    turns = [(which, g) for which in BOTH for g in range(step // group)]

    @pl.when((pl.program_id(A) == 0) & (pl.program_id(B) == 0))
    def _():
        yo_ref[...] = y_ref[...]
        ids = lax.axis_index("kv") * slots + lax.broadcasted_iota(I32, (1, slots), B)
        move_ref[...] = placed(ids, dst_ref, slots)

    def move(which, g, slot):
        moved[slot] = dot_by(mig_ref[A, which, :, g * group * rows : (g + 1) * group * rows], move_ref[...], A, A).astype(BF16)

    move(A, A, A)
    for i, (which, g) in enumerate(turns):
        if i + 1 < len(turns):
            move(*turns[i + 1], (i + 1) % PAIR)
        pool_ref, out_ref = ((k_ref, ko_ref), (v_ref, vo_ref))[which]
        for j in range(group):
            r = g * group + j
            pos = jnp.full((1, slots), (base + r).astype(F32), F32).astype(BF16)
            val = jnp.where(keep, pool_ref[A, r], moved[i % PAIR, j * rows : (j + 1) * rows, :])
            val = jnp.where(at0 == pos, new_ref[A, A, which, :, live], val)
            out_ref[A, r] = jnp.where(at1 == pos, new_ref[A, B, which, :, live], val)


def new_pools(pools, mig, knew, vec, dst, y):
    layers, page, rows, slots = pools[A].shape
    step, group = page // PAIR, FAR
    entries = mig.shape[PAIR]
    block = pl.BlockSpec((1, step, rows, slots), lambda l, i: (l, i, A, A))
    whole = pl.BlockSpec(y.shape, lambda l, i: (A, A, A))
    return pl.pallas_call(
        pool_kernel,
        out_shape=[jax.ShapeDtypeStruct(pools[A].shape, BF16)] * PAIR + [jax.ShapeDtypeStruct(y.shape, BF16)],
        grid=(layers, page // step),
        in_specs=[
            pl.BlockSpec(memory_space=pltpu.SMEM),
            pl.BlockSpec(vec.shape, lambda l, i: (A, A)),
            pl.BlockSpec((1, PAIR, entries, step * rows), lambda l, i: (l, A, A, i)),
            pl.BlockSpec((1, PAIR, PAIR, rows, LANES), lambda l, i: (l, A, A, A, A)),
            whole, block, block,
        ],
        out_specs=[block, block, whole],
        scratch_shapes=[pltpu.VMEM((PAIR, group * rows, slots), BF16), pltpu.VMEM((entries, slots), BF16)],
        compiler_params=pltpu.CompilerParams(dimension_semantics=("arbitrary",) * PAIR, vmem_limit_bytes=VMEM_BYTES),
        name="new_pools",
    )(dst, vec, mig, knew, y, *pools)


def solution(mesh):
    devs = mesh.shape["kv"]
    pool_spec = P(("rep", "kv"))
    tok_spec = P(None, ("rep", "kv"), None)

    def device_fn(embeds, w_query, w_key, w_value, w_out, w_up, w_down, k_pool, v_pool, new_table, seq_lens, mig_src, mig_dst):
        slots, layers, page, kv_heads, head = k_pool.shape
        seqs, d_model = embeds.shape[1:]
        rep_heads = w_query.shape[-1] // head // kv_heads
        own_rows = rep_heads * head
        n = SimpleNamespace(
            layers=layers, d_model=d_model, ff_half=w_up.shape[-1] // PAIR, chips=devs // PAIR, seqs=seqs, pair=PAIR * seqs,
            slots=slots, kv_heads=kv_heads, head=head, page=page, rep_heads=rep_heads, own_rows=own_rows, sub=own_rows // PAIR,
            wide=kv_heads // PAIR * own_rows, kv_cols=kv_heads * head, entries=mig_src.shape[A],
            s_cols=d_model // PAIR, d_cols=d_model // FAR, u_cols=w_up.shape[-1] // FAR)
        total = seqs * devs
        pages = page * n.kv_cols
        pools = [jnp.moveaxis(p, A, -1).reshape(layers, page, n.kv_cols, slots) for p in (k_pool, v_pool)]
        dma, two = pltpu.SemaphoreType.DMA, PAIR
        ring = (two, FAR, two)
        bf = lambda *shape: pltpu.VMEM(shape, BF16)
        f32 = lambda *shape: pltpu.VMEM(shape, F32)
        hbm, vmem, smem = (pl.BlockSpec(memory_space=m) for m in (pl.ANY, pltpu.VMEM, pltpu.SMEM))
        y, knew, vec, mig = pl.pallas_call(
            functools.partial(main_kernel, n),
            out_shape=[
                jax.ShapeDtypeStruct((two, seqs, d_model), BF16),
                jax.ShapeDtypeStruct((layers, two, two, n.kv_cols, LANES), BF16),
                jax.ShapeDtypeStruct((SUB, LANES), F32),
                jax.ShapeDtypeStruct((layers, two, n.entries, pages), BF16),
            ],
            in_specs=[smem] * two + [vmem] * (two + 1) + [hbm] * SUB,
            out_specs=[vmem] * (two + 1) + [hbm],
            scratch_shapes=[
                bf(LANES, total), bf(two, two * LANES, total), bf(two * LANES, total), f32(SUB, total), pltpu.VMEM((SUB, LANES), I32),
                bf(n.entries, slots), bf(two, n.entries, pages), bf(n.entries, pages),
                bf(two, FAR, two, n.entries, pages // devs), bf(n.entries, pages),
                bf(two, total, d_model), bf(slots, d_model), bf(max(d_model, n.ff_half), d_model), bf(d_model, n.kv_cols),
                bf(d_model, n.kv_cols), bf(n.wide, d_model), bf(d_model, n.ff_half), bf(two + 1, two, SUB, n.kv_cols, slots), bf(two, page, (kv_heads - 1) * head, LANES),
                f32(kv_heads - 1, own_rows, LANES), f32(two, two, n.kv_cols, LANES), f32(two, two, (kv_heads - 1) * head, LANES), f32(page, rep_heads, LANES),
                f32(two, two, two, own_rows + two * SUB, LANES), f32(two, two, own_rows + two * SUB, LANES),
                f32(two, rep_heads, two * LANES), f32(two, n.chips, two, n.sub + SUB, LANES),
                f32(two, two, FAR, two, n.sub + SUB, LANES), bf(n.pair, n.wide), f32(two, two, seqs, d_model),
                f32(two, two, seqs, d_model), bf(two, two, seqs, d_model), bf(two, n.pair, n.ff_half),
                dma((two,)), dma((two, *ring)), dma((two, two)), dma((two,)), dma((two, *ring)), dma((two, two)),
                dma((two, two, two)), dma((two, two)), dma((layers,)), dma((layers, *ring)), dma((layers,)), dma((layers, *ring)),
                dma((two,)), dma((two + 1, layers)), dma((two + 1, two)), dma((SUB,)),
            ],
            compiler_params=pltpu.CompilerParams(collective_id=A, has_side_effects=True, vmem_limit_bytes=VMEM_BYTES),
            name="decode",
        )(mig_src, mig_dst, new_table.T, seq_lens[None], embeds, w_query, w_key, w_value, w_out, w_up, w_down, *pools)
        *outs, y = new_pools(pools, mig, knew, vec, mig_dst, y)
        outs = [jnp.moveaxis(p.reshape(layers, page, kv_heads, head, slots), -1, A) for p in outs]
        return y, *outs

    return jax.shard_map(
        device_fn, mesh=mesh,
        in_specs=(tok_spec, *(P(),) * (SUB - PAIR), pool_spec, pool_spec, P("rep", None), *(P("rep"),) * (FAR - 1)),
        out_specs=(tok_spec, pool_spec, pool_spec), check_vma=False)
```

```python
import functools
from types import SimpleNamespace

import jax
import jax.numpy as jnp
from jax import lax
from jax.experimental import pallas as pl
from jax.experimental.pallas import tpu as pltpu
from jax.sharding import PartitionSpec as P

MESH = pl.DeviceIdType.MESH
F32, BF16, I32 = jnp.float32, jnp.bfloat16, jnp.int32
NEG = -1e30
LANES = 128
SUB = 8
A, B = BOTH = range(2)
PAIR = len(BOTH)
VMEM_BYTES = 67043328
FAR = 4
HOPS = range(1, FAR + 1)


class Names:
    def __getattr__(self, name):
        return name


W = Names()
ORDER = (
    W.AG00s, W.AG01s, W.AG00h10, W.AG00h11, W.AG01h10, W.AG01h11, W.TAB, W.AG00h20, W.AG00h21, W.EXT0, W.AG01h21,
    W.AG00h30, W.AG00h31, W.AG00h40, W.AG01h20, W.AG00h41, W.SEL00, W.MS0s, W.PROJ00, W.ATT000, W.AG01h30, W.MS0k301,
    W.MS0k400, W.MS0k310, W.AG01h31, W.ATT001, W.ATT002, W.MS0k411, W.MS0k300, W.AG01h40, W.AG01h41, W.MS0k210,
    W.SCAT00, W.SCAU00, W.SEL01, W.PROJ01, W.MS0k200, W.MS0k311, W.ATT010, W.RS00k400, W.MS0k201, W.RS00k310,
    W.ATT011, W.RS00k301, W.RS00k411, W.ATT012, W.RS00k300, W.RS00k210, W.MS0k110, W.MS0k101, W.MS0k100, W.SCAT01,
    W.RS00k311, W.RS00k200, W.MS0k211, W.SCAU01, W.RS00k201, W.RS01k400, W.MS0k111, W.RS00k211, W.EXT1, W.RS01k310,
    W.RS00k100, W.RS00k110, W.RS01k411, W.RS00k101, W.RS00k111, W.RS01k301, W.FO00, W.MID00, W.MG0s, W.RS01k300,
    W.RS01k210, W.UP000, W.UP001, W.RS01k201, W.RS01k311, W.DOWN00, W.NEWH00, W.AG10s, W.RS01k200, W.RS01k110,
    W.RS01k211, W.AG10h10, W.AG10h11, W.RS01k100, W.RS01k101, W.MG0h10, W.RS01k111, W.FO01, W.AG10h20, W.AG10h21,
    W.MID01, W.UP010, W.MG0h11, W.UP011, W.AG10h30, W.AG10h31, W.MG0h20, W.DOWN01, W.NEWH01, W.AG11s, W.AG10h41,
    W.AG10h40, W.MG0h21, W.SEL10, W.MG0h30, W.PROJ10, W.AG11h10, W.ATT100, W.AG11h11, W.ATT101, W.AG11h20, W.MG0h31,
    W.ATT102, W.AG11h21, W.SCAT10, W.AG11h30, W.AG11h31, W.SCAU10, W.RS10k400, W.MG0h41, W.AG11h40, W.MG0h40, W.MS1s,
    W.AG11h41, W.SEL11, W.RS10k411, W.PROJ11, W.RS10k310, W.RS10k301, W.MS1k411, W.ATT110, W.MS1k400, W.RS10k300,
    W.RS10k311, W.ATT111, W.RS10k210, W.MS1k311, W.MS1k301, W.RS10k201, W.MS1k310, W.ATT112, W.MS1k300, W.RS10k211,
    W.RS10k200, W.SCAT11, W.SCAU11, W.MS1k200, W.MS1k210, W.RS10k110, W.RS11k310, W.RS10k100, W.RS11k400, W.RS10k111,
    W.RS10k101, W.FO10, W.MS1k211, W.MS1k201, W.RS11k301, W.RS11k411, W.RS11k210, W.MID10, W.RS11k300, W.RS11k311,
    W.RS11k201, W.MS1k101, W.MS1k111, W.MS1k110, W.UP100, W.MS1k100, W.MG1s, W.UP101, W.DOWN10, W.RS11k211,
    W.RS11k200, W.RS11k110, W.RS11k101, W.MG1h10, W.MG1h11, W.RS11k111, W.RS11k100, W.FO11, W.MG1h20, W.MID11,
    W.MG1h21, W.UP110, W.MG1h30, W.UP111, W.MG1h31, W.DOWN11, W.MG1h40, W.NEWH11, W.NEWH10, W.MG1h41,
)


def dot(a, b):
    return jnp.dot(a, b, preferred_element_type=F32)


def dot_by(a, b, left, right):
    return lax.dot_general(a, b, (((left,), (right,)), ((), ())), preferred_element_type=F32)


def exact_dot(x, onehot, right=A):
    high = x.astype(BF16)
    rest = x - high.astype(F32)
    mid = rest.astype(BF16)
    low = (rest - mid.astype(F32)).astype(BF16)
    out = dot_by(jnp.concatenate([high, mid, low], axis=A), onehot, B, right).reshape(FAR - 1, x.shape[A], -1)
    return out[A] + out[B] + out[PAIR]


def sums_to_rows(parts):
    axis = parts[A].ndim - PAIR
    sub = lax.broadcasted_iota(I32, parts[A].shape, axis)
    while len(parts) > 1:
        half = len(parts) // PAIR
        high = (sub & half) != 0
        parts = [
            jnp.where(high, a + pltpu.roll(a, half, axis), b + pltpu.roll(b, SUB - half, axis))
            for a, b in zip(parts[half:], parts[:half], strict=True)
        ]
    return parts[A]


def at_block(i, size):
    return pl.ds(pl.multiple_of(i * size, size), size)


def loop(count, body):
    def step(i, carry):
        body(i)
        return carry

    lax.fori_loop(A, count, step, A)


def takes(way, hop, half):
    return hop < FAR or way == half


def taken(hops=HOPS):
    return [(way, hop, half) for half in BOTH for way in BOTH for hop in hops if takes(way, hop, half)]


def mask_rows(ids, values, shape=None):
    out = jnp.zeros(shape or ids.shape, I32)
    for e in range(values.shape[A]):
        out = jnp.where(ids == values[e], 1, out)
    return out


def placed(ids, values, slots):
    entries = values.shape[A]
    row = lax.broadcasted_iota(I32, (entries, slots), A)
    out = jnp.zeros((entries, slots), F32)
    for e in range(entries):
        out = jnp.where(row == e, jnp.where(ids == values[e], 1.0, 0.0), out)
    return out.astype(BF16)


def main_kernel(
    n,
    src_ref, dst_ref, tab_ref, len_ref, x_ref, wq, wk, wv, wo, wu, wd, kp, vp,
    y_ref, knew_ref, vec_ref, mig_out,
    oh_ref, e_ref, es_ref, pres_ref, lane_ref, pick_ref, mg, mx, mr, mf,
    h_all, hsel, wbig, wk_v, wv_v, wo_v, wu_v, raw, kv_p, q_ref, kn_ref, kn_p, s_ref, oa, ob, a_ref, pd, rd,
    olhs, pf, rf, hm, act, ag_sent, ag_got, dd_sem, rs_sent, rs_got, x_sem, f_sem, m_sem, gs_sent, gs_got, gg_sent, gg_got,
    gp_sem, go_sem, p_sem, w_sem,
):
    me = lax.axis_index("kv")
    z, c = me // PAIR, lax.rem(me, PAIR)
    group = lax.axis_index("rep")
    peer = (group, z * PAIR + 1 - c)
    live = pl.ds(A, n.slots)
    half_d = n.d_model // PAIR
    heads_half = n.rep_heads // PAIR

    chips = {step: lax.rem(z + step + n.chips, n.chips) for step in range(-FAR, FAR + 1)}
    rings = {step: (group, PAIR * chips[step] + c) for step in (-1, 1)}
    h_rows = {step: (chips[step] * PAIR + c) * n.seqs for step in chips}

    def along(way, steps):
        return steps if way == A else -steps

    def on_ring(way, steps):
        return rings[along(way, steps)]

    def remote_by(src, dst, send, recv, target):
        return pltpu.make_async_remote_copy(
            src_ref=src, dst_ref=dst, send_sem=send, recv_sem=recv, device_id=target, device_id_type=MESH)

    def remote(src, dst, sems, at, target):
        return remote_by(src, dst, sems.at[(A, *at)], sems.at[(B, *at)], target)

    mine_o, mine_f = at_block(c, n.wide), at_block(c, n.ff_half)
    sources = {
        "q": lambda l: (wq.at[l], wbig.at[pl.ds(A, n.d_model), :]), "k": lambda l: (wk.at[l], wk_v), "v": lambda l: (wv.at[l], wv_v),
        "o": lambda l: (wo.at[l, mine_o, :], wo_v), "u": lambda l: (wu.at[l, :, mine_f], wu_v),
        "d": lambda l: (wd.at[l, mine_f, :], wbig.at[pl.ds(A, n.ff_half), :]),
    }
    follows = {"q": ("d", A), "d": ("q", B)} | {name: (name, B) for name in "kvou"}
    users = {name: PAIR for name in "qkvoud"}
    ready, used = set(), {}

    def load(name, l):
        src, dst = sources[name](l)
        return pltpu.make_async_copy(src, dst, w_sem.at[list(sources).index(name)])

    def need(names, l):
        for name in names:
            if (name, l) not in ready:
                ready.add((name, l))
                load(name, l).wait()

    def release(names, l):
        for name in names:
            used[name, l] = used.get((name, l), A) + 1
            after, more = follows[name]
            if used[name, l] == users[name] and l + more < n.layers:
                load(after, l + more).start()

    def gather(ref_of, sent, got, key):
        def copy(way, hop, half):
            ref = ref_of(along(way, 1 - hop), half)
            return remote_by(ref, ref, sent.at[key], got.at[key, way, hop - 1, half], on_ring(way, 1))

        return copy

    def gather_start(copy):
        for half in BOTH:
            for way in BOTH:
                copy(way, 1, half).start()

    def gather_hop(copy, hop, half, passed_on=None):
        for way in BOTH:
            if takes(way, hop, half):
                copy(way, hop, half).wait_recv()
                if hop < FAR and takes(way, hop + 1, half):
                    copy(way, hop + 1, half).start()
                if passed_on:
                    passed_on(way, hop, half).start()

    def total(src_of, got_of, sent, got, key):
        def copy(way, dist, half):
            return remote_by(
                src_of(along(way, dist), half), got_of(way, dist, half), sent.at[key], got.at[key, way, dist - 1, half],
                on_ring(way, 1))

        return copy

    def total_start(copy):
        for way in BOTH:
            copy(way, FAR, way).start()
        for way in BOTH:
            copy(way, FAR - 1, 1 - way).start()

    def total_hop(copy, add, dist, way, half):
        copy(way, dist, half).wait_recv()
        add(along(way, dist - 1), way, dist, half)
        if dist > 1:
            copy(way, dist - 1, half).start()

    ring_copies = len(taken())

    def all_sent(ref, sem):
        remote_by(ref, ref, sem, sem, peer).wait_send()

    def block(t, step, half):
        return h_all.at[t, pl.ds(pl.multiple_of(h_rows[step], n.seqs), n.seqs), pl.ds(half * half_d, half_d)]

    ag_copies = [gather(lambda step, half, t=t: block(t, step, half), ag_sent, ag_got, t) for t in BOTH]

    def to_peer(t):
        def copy(way, hop, half):
            ref = block(t, along(way, -hop), half)
            return remote(ref, ref, dd_sem, (t,), peer)

        return copy

    def ag_start(l, t):
        gather_start(ag_copies[t])
        for half in BOTH:
            to_peer(t)(A, A, half).start()

    def ag_hop(t, hop, half):
        gather_hop(ag_copies[t], hop, half, to_peer(t))

    def ag_finish(t):
        blocks = ring_copies // PAIR
        from_peer = h_all.at[t, pl.ds(A, (blocks + 1) * n.seqs), :]
        remote(from_peer, from_peer, dd_sem, (t,), peer).wait()
        all_sent(h_all.at[t, pl.ds(A, blocks * n.seqs), :], ag_sent.at[t])

    stats = pl.ds(n.sub, SUB)
    top_rows = lax.broadcasted_iota(I32, (SUB, LANES), A) < heads_half
    rs_copies = [
        total(lambda step, half, t=t: pd.at[t, chips[step], half], lambda way, d, half, t=t: rd.at[t, way, d - 1, half], rs_sent, rs_got, t)
        for t in BOTH
    ]

    def merge(t):
        def add(step, way, d, half):
            got, mine = rd.at[t, way, d - 1, half], pd.at[t, chips[step], half]
            s1, s2 = got[stats, :], mine[stats, :]
            m = jnp.maximum(s1, s2)
            a1, a2 = jnp.exp(s1 - m), jnp.exp(s2 - m)
            mine[stats, :] = jnp.where(top_rows, m, pltpu.roll(a1, heads_half, A) * s1 + pltpu.roll(a2, heads_half, A) * s2)
            at = pl.ds(A, n.sub)
            by_head = (heads_half, n.head, LANES)
            a1, a2 = (a[:heads_half][:, None] for a in (a1, a2))
            mine[at, :] = (a1 * got[at, :].reshape(by_head) + a2 * mine[at, :].reshape(by_head)).reshape(n.sub, LANES)

        return add

    def select(l, t):
        ag_finish(t)

        def body(i):
            cols = at_block(i, n.s_cols)
            hsel[:, cols] = dot(oh_ref[live, :], h_all[t, :, cols]).astype(BF16)

        loop(n.d_model // n.s_cols, body)

    def turned(w):
        rows = dot(hsel[...], w).astype(BF16).astype(F32)
        return jnp.concatenate([rows, jnp.zeros((LANES - n.slots, rows.shape[B]), F32)], axis=A).T

    units = (PAIR * (1 - c), PAIR * (1 - c) + 1, PAIR * c)
    spread_head = PAIR * c + 1
    first_part = LANES - n.slots

    def packed(u, own, other):
        rest = (other[..., :first_part], other[..., first_part:], own[..., n.slots :])[u]
        if rest.shape[-1] < first_part:
            pad = jnp.zeros((*own.shape[:-1], first_part - rest.shape[-1]), own.dtype)
            rest = jnp.concatenate([rest, pad], axis=-1) if rest.shape[-1] else pad
        return jnp.concatenate([own, rest], axis=-1)

    def project(l, t):
        need("qkv", l)

        def query(kvh):
            return turned(wbig[pl.ds(A, n.d_model), at_block(kvh, n.own_rows)])

        other = query(spread_head)[:, : n.slots]
        for u, kvh in enumerate(units):
            q_ref[u] = packed(u, query(kvh)[:, : n.slots], other)
        for i, w in enumerate((wk_v, wv_v)):
            kn_ref[t, i] = turned(w[...])
            knew_ref[l, t, i] = kn_ref[t, i].astype(BF16)
            for u, kvh in enumerate(units):
                own, other = (kn_ref[t, i, at_block(head, n.head), live] for head in (kvh, spread_head))
                kn_p[t, i, at_block(u, n.head), :] = packed(u, own, other)
        release("qkv", l)

    def attend(t, u):
        rows = at_block(u, n.head)
        scale = n.head ** -0.5
        out = oa.at[t, jnp.where(u < PAIR, 1 - c, c), jnp.where(u < PAIR, u, A)]
        heads = range(n.rep_heads)

        def pages(w, at):
            return kv_p[w, at, rows, :].astype(F32)

        def scores(keys):
            parts = []
            for h in heads:
                prods = q_ref[u, pl.ds(h * n.head, n.head), :][None] * keys
                acc = prods[:, :SUB]
                for d in range(SUB, n.head, SUB):
                    acc = acc + prods[:, d : d + SUB]
                parts.append(acc)
            return sums_to_rows(parts)

        def qk(i):
            at = pl.ds(i * FAR, FAR)
            s_ref[at, :, :] = scores(pages(A, at))

        loop(n.page // FAR, qk)
        fresh = range(t + 1)
        news = [scores(kn_p[i, A, rows, :][None])[A] for i in fresh]
        lim, has_new = lane_ref[pl.ds(PAIR * u, 1), :], lane_ref[pl.ds(PAIR * u + 1, 1), :] > 0
        news = [jnp.where(has_new, s * scale, NEG) for s in news]
        valid = lax.broadcasted_iota(I32, (n.page, n.rep_heads, lim.shape[B]), A) < lim[None]
        old = jnp.where(valid, s_ref[:, :, :] * scale, NEG)
        m = jnp.max(old, axis=A)
        for s in news:
            m = jnp.maximum(m, s)
        probs = jnp.where(valid, jnp.exp(old - m[None]), 0.0)
        s_ref[:, :, :] = probs
        news = [jnp.where(has_new, jnp.exp(s - m), 0.0) for s in news]
        count = jnp.sum(probs, axis=A)
        for p in news:
            count = count + p
        out[pl.ds(n.own_rows, SUB), :] = m
        out[pl.ds(n.own_rows + SUB, SUB), :] = count
        vals = [kn_p[i, B, rows, :] for i in fresh]
        for h in heads:
            acc = news[A][h : h + 1] * vals[A]
            for p, v in zip(news[1:], vals[1:], strict=True):
                acc = acc + p[h : h + 1] * v
            out[pl.ds(h * n.head, n.head), :] = acc

        def pv(i):
            vals = [v for v in pages(B, pl.ds(i * FAR, FAR))]
            ps = [s_ref[i * FAR + j, :, :] for j in range(FAR)]
            for h in heads:
                at = pl.ds(h * n.head, n.head)
                acc = out[at, :]
                for p, v in zip(ps, vals, strict=True):
                    acc = acc + p[h : h + 1] * v
                out[at, :] = acc

        loop(n.page // FAR, pv)

    def exchange(t):
        return remote(oa.at[t, 1 - c], ob.at[t], x_sem, (t,), peer)

    def attend_all(l, t, between):
        def body(u):
            attend(t, u)
            pl.when(u == B)(lambda: exchange(t).start())
            for at, work in between.items():
                pl.when(u == at)(work)

        loop(len(units), body)
        lane = lax.broadcasted_iota(I32, (1, LANES), B)
        near, far = (pltpu.roll(oa[t, 1 - c, v], first_part * (v + 1), B) for v in BOTH)
        oa[t, c, B] = jnp.where(lane < first_part, near, far)

    low_lanes = lax.broadcasted_iota(I32, (1, LANES), B) < n.pair

    def by_chip(parts, put):
        for zp in range(n.chips // PAIR):
            a, b = (p[:, zp * LANES : (zp + 1) * LANES] for p in parts)
            put(PAIR * zp, jnp.where(low_lanes, a, pltpu.roll(b, n.pair, B)))
            put(PAIR * zp + 1, jnp.where(low_lanes, pltpu.roll(a, n.pair, B), b))

    def both_cores(t, hh, at):
        return jnp.concatenate([oa[t, c, hh, at, :], ob[t, hh, at, :]], axis=B)

    def scatter(l, t):
        exchange(t).wait()
        top, count = (
            jnp.concatenate([both_cores(t, hh, pl.ds(n.own_rows + off, SUB)) for hh in BOTH], axis=A) for off in (A, SUB))
        m_page = [jnp.where(pres_ref[pl.ds(p, 1), :] > 0, exact_dot(top, e_ref[p]), NEG) for p in BOTH]
        m_seq = jnp.maximum(*m_page)
        a = jnp.exp(jnp.minimum(top - exact_dot(m_seq, es_ref[...], right=B), 0.0))
        a_ref[A], a_ref[B] = a[:SUB], a[SUB:]
        l_seq = exact_dot(count * a, es_ref[...])
        dense = {}
        for what, v in enumerate((m_seq, l_seq)):
            by_chip([v[:SUB], v[SUB:]], lambda zz, v, what=what: dense.update({(zz, what): v}))
        for zz in range(n.chips):
            m, l = dense[zz, A], dense[zz, B]
            pd[t, zz, A, stats, :] = jnp.where(top_rows, m, pltpu.roll(l, heads_half, A))
            pd[t, zz, B, stats, :] = jnp.where(top_rows, pltpu.roll(m, heads_half, A), l)

        scatter_half(A, l, t)

    def scatter_half(half, l, t):
        def body(k):
            for j in range(heads_half // PAIR):
                i = k * PAIR + j
                h = half * heads_half + i
                parts = [
                    exact_dot(both_cores(t, hh, at_block(h, n.head)) * a_ref[hh, pl.ds(h, 1), :], es_ref[...]) for hh in BOTH]

                def put(zz, v, i=i):
                    pd[t, zz, half, at_block(i, n.head), :] = v

                by_chip(parts, put)

        loop(PAIR, body)
        for way in BOTH:
            rs_copies[t](way, FAR if way == half else FAR - 1, half).start()

    def f_copy(t, stage):
        return remote(pf.at[t, 1 - c], rf.at[t, stage], f_sem, (t, stage), peer)

    def m_copy(t):
        return remote(hm.at[t, c], hm.at[t, c], m_sem, (t,), peer)

    def product(t, lhs, w):
        def body(i):
            cols = at_block(i, n.s_cols)
            val = dot(lhs(), w(cols))
            pf[t, A, :, cols] = val[: n.seqs]
            pf[t, B, :, cols] = val[n.seqs :]

        loop(n.d_model // n.s_cols, body)

    own = pl.ds(pl.multiple_of(h_rows[A], n.seqs), n.seqs)

    def out_proj(l, t):
        all_sent(pd.at[t, pl.ds(A, ring_copies // PAIR)], rs_sent.at[t])
        for half in BOTH:
            mine = pd.at[t, z, half]
            inv = (1.0 / mine[stats, :])[heads_half:][:, None]
            flat = (mine[pl.ds(A, n.sub), :].reshape(heads_half, n.head, LANES) * inv).reshape(n.sub, LANES).T.astype(BF16)
            for hh in BOTH:
                olhs[:, pl.ds(hh * n.own_rows + half * n.sub, n.sub)] = flat[hh * n.pair : (hh + 1) * n.pair]
        need("o", l)
        product(t, lambda: olhs[...], lambda cols: wo_v[:, cols])
        release("o", l)
        f_copy(t, A).start()

    def mid(l, t):
        f_copy(t, A).wait()
        hm[t, c] = (h_all[t, own, :].astype(F32) + (pf[t, c] + rf[t, A])).astype(BF16)
        m_copy(t).start()

    def up(l, t, halfway):
        m_copy(t).wait()
        need("u", l)

        def body(i):
            cols = at_block(i, n.u_cols)
            u = dot(hm[t].reshape(n.pair, n.d_model), wu_v[:, cols]).astype(BF16).astype(F32)
            act[t, :, cols] = jax.nn.gelu(u, approximate=True).astype(BF16)
            for at, work in halfway.items():
                pl.when(i == at)(work)

        loop(n.ff_half // n.u_cols, body)
        release("u", l)

    def down(l, t):
        need("d", l)
        product(t, lambda: act[t], lambda cols: wbig[pl.ds(A, n.ff_half), cols])
        release("d", l)
        f_copy(t, B).start()

    def new_h(l, t):
        f_copy(t, B).wait()
        new = (hm[t, c].astype(F32) + (pf[t, c] + rf[t, B])).astype(BF16)
        h_all[t, own, :] = new
        y_ref[t] = new

    def ids_of(dev, axis):
        at = lax.broadcasted_iota(I32, (LANES, 1) if axis == A else (1, LANES), axis)
        return jnp.where(at < n.slots, dev * n.slots + at, -1)

    def tables():
        oa[...] = jnp.zeros_like(oa)
        for g, dev in enumerate((me, z * PAIR + 1 - c)):
            ids = ids_of(dev, A)
            target = ids
            for e in range(n.entries):
                target = jnp.where(ids == src_ref[e], dst_ref[e], target)
            stale = mask_rows(ids, dst_ref)
            hit = [jnp.where(tab_ref[pl.ds(p, 1), :] == target, 1.0, 0.0) for p in BOTH]
            now = [jnp.where(stale == 0, h, 0.0) for h in hit]
            at = pl.ds(g * LANES, LANES)
            for p in BOTH:
                e_ref[p, at, :] = now[p].astype(BF16)
            es_ref[at, :] = (now[A] + now[B]).astype(BF16)
            if g == A:
                oh_ref[...] = (hit[A] + hit[B]).astype(BF16)
                held = [h.astype(BF16) for h in (*now, hit[B])]
        for p in BOTH:
            pres_ref[pl.ds(p, 1), :] = jnp.sum(e_ref[p].astype(F32), axis=A, keepdims=True)
        lens = len_ref[...].astype(F32)
        rows = jnp.concatenate([lens, jnp.ones((SUB - 1, lens.shape[B]), F32)], axis=A).astype(BF16)
        first, last, fresh = (dot_by(rows, h, B, B) for h in held)
        at0, at1 = slice(A, 1), slice(B, PAIR)
        limit = jnp.where(first[at1] > 0, jnp.minimum(first[at0], n.page), jnp.where(last[at1] > 0, last[at0] - n.page, 0.0))
        for i, row in enumerate((limit, last[at1])):
            row = row[:, : n.slots]
            for u in range(len(units)):
                lane_ref[pl.ds(PAIR * u + i, 1), :] = packed(u, row, row).astype(I32)
        ids = ids_of(me, B)
        is_src, is_dst = mask_rows(ids, src_ref), mask_rows(ids, dst_ref)
        pick_ref[...] = placed(ids[:, : n.slots], src_ref, n.slots)
        on_last = jnp.where(is_src == 0, fresh[at1], 0.0) > 0
        start = fresh[at0] - n.page
        vec_ref[...] = jnp.where(is_src + is_dst == 0, 1.0, 0.0) * jnp.ones((SUB, LANES), F32)
        for t in BOTH:
            vec_ref[pl.ds(t, 1), :] = jnp.where(on_last, start + t, -1.0)

    m_cols = mf.shape[B] // n.chips // PAIR

    def mig_pair():
        return remote(mg.at[1 - c], mx, gp_sem, (), peer)

    def m_at(step, half):
        return at_block(chips[step] * PAIR + half, m_cols)

    ms_copies, mg_copies = [], []
    for l in range(n.layers):
        ms_copies.append(total(lambda step, half: mg.at[c, :, m_at(step, half)], lambda way, d, half: mr.at[way, d - 1, half], gs_sent, gs_got, l))
        mg_copies.append(gather(lambda step, half: mf.at[:, m_at(step, half)], gg_sent, gg_got, l))

    def mig_add(step, way, d, half):
        at = m_at(step, half)
        mg[c, :, at] = mg[c, :, at] + mr[way, d - 1, half]

    m_ring = pl.ds(A, ring_copies * m_cols)

    def mig_sent(l):
        all_sent(mg.at[c, :, m_ring], gs_sent.at[l])

    def mig_out_copies(l):
        return remote(mf, mig_out.at[l, c], go_sem, (l,), peer), pltpu.make_async_copy(mf, mig_out.at[l, c], go_sem.at[PAIR, l])

    def page_loads(l, i, slot):
        at = pl.ds(pl.multiple_of(i * SUB, SUB), SUB)
        return [pltpu.make_async_copy(pool.at[l, at], raw.at[slot, w], p_sem.at[slot, w]) for w, pool in enumerate((kp, vp))]

    def first_pages(l):
        for i in range(raw.shape[A]):
            for copy in page_loads(l, i, i):
                copy.start()

    def extract(l):
        if l > 0:
            mig_sent(l - 1)
        chunks, held = n.page // SUB, raw.shape[A]

        def body(i):
            slot = lax.rem(i, held)
            for copy in page_loads(l, i, slot):
                copy.wait()
            at = pl.ds(pl.multiple_of(i * SUB, SUB), SUB)
            for w in BOTH:
                rows = raw[slot, w].reshape(SUB * n.kv_cols, n.slots)
                mg[w, :, at_block(i, SUB * n.kv_cols)] = dot_by(pick_ref[...], rows, B, B).astype(BF16)
                other = raw[slot, w, :, at_block(spread_head, n.head), :]
                for u, kvh in enumerate(units):
                    kv_p[w, at, at_block(u, n.head), :] = packed(u, raw[slot, w, :, at_block(kvh, n.head), :], other)

            @pl.when(i + held < chunks)
            def _():
                for copy in page_loads(l, i + held, slot):
                    copy.start()

        loop(chunks, body)
        if l + 1 < n.layers:
            first_pages(l + 1)
        mig_pair().start()

    def mig_start(l):
        if l > 0:
            for copy in mig_out_copies(l - 1):
                copy.wait()
        mig_pair().wait()
        mg[c] = mg[c] + mx[...]
        total_start(ms_copies[l])

    def mig_gather(l):
        gather_start(mg_copies[l])

    def mig_own():
        for half in BOTH:
            mf[:, m_at(A, half)] = mg[c, :, m_at(A, half)]

    def mig_end(l):
        all_sent(mf.at[:, m_ring], gg_sent.at[l])
        for copy in mig_out_copies(l):
            copy.start()

    steps = {"TAB": tables}
    for l in range(n.layers):
        steps[f"EXT{l}"] = functools.partial(extract, l)
        steps[f"MS{l}s"] = functools.partial(mig_start, l)
        steps[f"MG{l}s"] = functools.partial(mig_gather, l)
        for hop in HOPS:
            for half in BOTH:
                steps[f"MG{l}h{hop}{half}"] = functools.partial(gather_hop, mg_copies[l], hop, half)
                for way in BOTH:
                    steps[f"MS{l}k{hop}{way}{half}"] = functools.partial(total_hop, ms_copies[l], mig_add, hop, way, half)
        for t in BOTH:
            for name, work in (
                ("SEL", select), ("PROJ", project), ("SCAT", scatter), ("SCAU", functools.partial(scatter_half, B)), ("FO", out_proj), ("MID", mid), ("DOWN", down), ("NEWH", new_h),
            ):
                steps[f"{name}{l}{t}"] = functools.partial(work, l, t)
            steps[f"AG{l}{t}s"] = functools.partial(ag_start, l, t)
            for hop in HOPS:
                for half in BOTH:
                    steps[f"AG{l}{t}h{hop}{half}"] = functools.partial(ag_hop, t, hop, half)
                    for way in BOTH:
                        steps[f"RS{l}{t}k{hop}{way}{half}"] = functools.partial(total_hop, rs_copies[t], merge(t), hop, way, half)

    for t in BOTH:
        h_all[t, own, :] = x_ref[t]
    first_pages(A)
    load("q", A).start()
    barrier = pltpu.get_barrier_semaphore()
    others = (peer, *rings.values())
    for target in others:
        pl.semaphore_signal(barrier, inc=1, device_id=target, device_id_type=MESH)
    pl.semaphore_wait(barrier, len(others))

    def later_loads():
        for name in ("k", "v", "o", "u"):
            load(name, A).start()


    steps["LOADS"] = later_loads
    todo = list(ORDER)
    todo.insert(PAIR, "LOADS")
    on_way = {kind: len([name for name in todo if name.startswith(kind)]) for l in range(n.layers) for kind in (f"MS{l}k", f"MG{l}h")}

    def run(names):
        for name in names:
            steps[name]()
            kind = name[:FAR]
            if kind in on_way:
                on_way[kind] -= 1
                if on_way[kind] == 0:
                    mig_end(int(kind[PAIR])) if "h" in kind else mig_own()

    loops = {"ATT": (attend_all, len(units)), "UP": (up, n.ff_half // n.u_cols)}
    while todo:
        name = todo.pop(A)
        word = name.rstrip("0123456789")
        if word in loops:
            work, count = loops[word]
            l, t, _ = (int(ch) for ch in name[len(word) :])
            between = {}
            for i in range(count - 1):
                upto = todo.index(f"{word}{l}{t}{i + 1}")
                if upto:
                    between[i] = functools.partial(run, todo[:upto])
                todo = todo[upto + 1 :]
            work(l, t, between)
        else:
            run([name])
    for copy in mig_out_copies(n.layers - 1):
        copy.wait()
    mig_sent(n.layers - 1)


def pool_kernel(dst_ref, vec_ref, mig_ref, new_ref, y_ref, k_ref, v_ref, ko_ref, vo_ref, yo_ref, moved, move_ref):
    step, rows, slots = k_ref.shape[1:]
    live = slice(A, slots)
    group = moved.shape[1] // rows
    tab = vec_ref[...]
    at0, at1, keep = (tab[i : i + 1, live].astype(BF16) for i in range(PAIR + 1))
    keep = keep > 0
    base = pl.program_id(B) * step
    turns = [(which, g) for which in BOTH for g in range(step // group)]

    @pl.when((pl.program_id(A) == 0) & (pl.program_id(B) == 0))
    def _():
        yo_ref[...] = y_ref[...]
        ids = lax.axis_index("kv") * slots + lax.broadcasted_iota(I32, (1, slots), B)
        move_ref[...] = placed(ids, dst_ref, slots)

    def move(which, g, slot):
        moved[slot] = dot_by(mig_ref[A, which, :, g * group * rows : (g + 1) * group * rows], move_ref[...], A, A).astype(BF16)

    move(A, A, A)
    for i, (which, g) in enumerate(turns):
        if i + 1 < len(turns):
            move(*turns[i + 1], (i + 1) % PAIR)
        pool_ref, out_ref = ((k_ref, ko_ref), (v_ref, vo_ref))[which]
        for j in range(group):
            r = g * group + j
            pos = jnp.full((1, slots), (base + r).astype(F32), F32).astype(BF16)
            val = jnp.where(keep, pool_ref[A, r], moved[i % PAIR, j * rows : (j + 1) * rows, :])
            val = jnp.where(at0 == pos, new_ref[A, A, which, :, live], val)
            out_ref[A, r] = jnp.where(at1 == pos, new_ref[A, B, which, :, live], val)


def new_pools(pools, mig, knew, vec, dst, y):
    layers, page, rows, slots = pools[A].shape
    step, group = page // PAIR, FAR
    entries = mig.shape[PAIR]
    block = pl.BlockSpec((1, step, rows, slots), lambda l, i: (l, i, A, A))
    whole = pl.BlockSpec(y.shape, lambda l, i: (A, A, A))
    return pl.pallas_call(
        pool_kernel,
        out_shape=[jax.ShapeDtypeStruct(pools[A].shape, BF16)] * PAIR + [jax.ShapeDtypeStruct(y.shape, BF16)],
        grid=(layers, page // step),
        in_specs=[
            pl.BlockSpec(memory_space=pltpu.SMEM),
            pl.BlockSpec(vec.shape, lambda l, i: (A, A)),
            pl.BlockSpec((1, PAIR, entries, step * rows), lambda l, i: (l, A, A, i)),
            pl.BlockSpec((1, PAIR, PAIR, rows, LANES), lambda l, i: (l, A, A, A, A)),
            whole, block, block,
        ],
        out_specs=[block, block, whole],
        scratch_shapes=[pltpu.VMEM((PAIR, group * rows, slots), BF16), pltpu.VMEM((entries, slots), BF16)],
        compiler_params=pltpu.CompilerParams(dimension_semantics=("arbitrary",) * PAIR, vmem_limit_bytes=VMEM_BYTES),
        name="new_pools",
    )(dst, vec, mig, knew, y, *pools)


def solution(mesh):
    devs = mesh.shape["kv"]
    pool_spec = P(("rep", "kv"))
    tok_spec = P(None, ("rep", "kv"), None)

    def device_fn(embeds, w_query, w_key, w_value, w_out, w_up, w_down, k_pool, v_pool, new_table, seq_lens, mig_src, mig_dst):
        slots, layers, page, kv_heads, head = k_pool.shape
        seqs, d_model = embeds.shape[1:]
        rep_heads = w_query.shape[-1] // head // kv_heads
        own_rows = rep_heads * head
        n = SimpleNamespace(
            layers=layers, d_model=d_model, ff_half=w_up.shape[-1] // PAIR, chips=devs // PAIR, seqs=seqs, pair=PAIR * seqs,
            slots=slots, kv_heads=kv_heads, head=head, page=page, rep_heads=rep_heads, own_rows=own_rows, sub=own_rows // PAIR,
            wide=kv_heads // PAIR * own_rows, kv_cols=kv_heads * head, entries=mig_src.shape[A],
            s_cols=d_model // PAIR, d_cols=d_model // FAR, u_cols=w_up.shape[-1] // FAR)
        total = seqs * devs
        pages = page * n.kv_cols
        pools = [jnp.moveaxis(p, A, -1).reshape(layers, page, n.kv_cols, slots) for p in (k_pool, v_pool)]
        dma, two = pltpu.SemaphoreType.DMA, PAIR
        ring = (two, FAR, two)
        bf = lambda *shape: pltpu.VMEM(shape, BF16)
        f32 = lambda *shape: pltpu.VMEM(shape, F32)
        hbm, vmem, smem = (pl.BlockSpec(memory_space=m) for m in (pl.ANY, pltpu.VMEM, pltpu.SMEM))
        y, knew, vec, mig = pl.pallas_call(
            functools.partial(main_kernel, n),
            out_shape=[
                jax.ShapeDtypeStruct((two, seqs, d_model), BF16),
                jax.ShapeDtypeStruct((layers, two, two, n.kv_cols, LANES), BF16),
                jax.ShapeDtypeStruct((SUB, LANES), F32),
                jax.ShapeDtypeStruct((layers, two, n.entries, pages), BF16),
            ],
            in_specs=[smem] * two + [vmem] * (two + 1) + [hbm] * SUB,
            out_specs=[vmem] * (two + 1) + [hbm],
            scratch_shapes=[
                bf(LANES, total), bf(two, two * LANES, total), bf(two * LANES, total), f32(SUB, total), pltpu.VMEM((SUB, LANES), I32),
                bf(n.entries, slots), bf(two, n.entries, pages), bf(n.entries, pages),
                bf(two, FAR, two, n.entries, pages // devs), bf(n.entries, pages),
                bf(two, total, d_model), bf(slots, d_model), bf(max(d_model, n.ff_half), d_model), bf(d_model, n.kv_cols),
                bf(d_model, n.kv_cols), bf(n.wide, d_model), bf(d_model, n.ff_half), bf(two + 1, two, SUB, n.kv_cols, slots), bf(two, page, (kv_heads - 1) * head, LANES),
                f32(kv_heads - 1, own_rows, LANES), f32(two, two, n.kv_cols, LANES), f32(two, two, (kv_heads - 1) * head, LANES), f32(page, rep_heads, LANES),
                f32(two, two, two, own_rows + two * SUB, LANES), f32(two, two, own_rows + two * SUB, LANES),
                f32(two, rep_heads, two * LANES), f32(two, n.chips, two, n.sub + SUB, LANES),
                f32(two, two, FAR, two, n.sub + SUB, LANES), bf(n.pair, n.wide), f32(two, two, seqs, d_model),
                f32(two, two, seqs, d_model), bf(two, two, seqs, d_model), bf(two, n.pair, n.ff_half),
                dma((two,)), dma((two, *ring)), dma((two, two)), dma((two,)), dma((two, *ring)), dma((two, two)),
                dma((two, two, two)), dma((two, two)), dma((layers,)), dma((layers, *ring)), dma((layers,)), dma((layers, *ring)),
                dma((two,)), dma((two + 1, layers)), dma((two + 1, two)), dma((SUB,)),
            ],
            compiler_params=pltpu.CompilerParams(collective_id=A, has_side_effects=True, vmem_limit_bytes=VMEM_BYTES),
            name="decode",
        )(mig_src, mig_dst, new_table.T, seq_lens[None], embeds, w_query, w_key, w_value, w_out, w_up, w_down, *pools)
        *outs, y = new_pools(pools, mig, knew, vec, mig_dst, y)
        outs = [jnp.moveaxis(p.reshape(layers, page, kv_heads, head, slots), -1, A) for p in outs]
        return y, *outs

    return jax.shard_map(
        device_fn, mesh=mesh,
        in_specs=(tok_spec, *(P(),) * (SUB - PAIR), pool_spec, pool_spec, P("rep", None), *(P("rep"),) * (FAR - 1)),
        out_specs=(tok_spec, pool_spec, pool_spec), check_vma=False)
```

```python
import functools
from types import SimpleNamespace

import jax
import jax.numpy as jnp
from jax import lax
from jax.experimental import pallas as pl
from jax.experimental.pallas import tpu as pltpu
from jax.sharding import PartitionSpec as P

MESH = pl.DeviceIdType.MESH
F32, BF16, I32 = jnp.float32, jnp.bfloat16, jnp.int32
NEG = -1e30
LANES = 128
SUB = 8
A, B = BOTH = range(2)
PAIR = len(BOTH)
VMEM_BYTES = 67043328
FAR = 4
HOPS = range(1, FAR + 1)


class Names:
    def __getattr__(self, name):
        return name


W = Names()
ORDER = (
    W.AG00s, W.TAB, W.AG01s, W.AG00h10, W.AG00h11, W.AG01h11, W.AG00h20, W.AG00h21, W.AG01h10, W.EXT0, W.AG00h30,
    W.AG01h21, W.AG00h31, W.MS0s, W.AG01h20, W.AG01h31, W.AG00h40, W.AG00h41, W.SEL00, W.PROA00, W.MS0k301, W.PROJ00,
    W.ATT000, W.AG01h30, W.MS0k400, W.MS0k411, W.ATT001, W.ATT002, W.ATT003, W.MS0k311, W.ATT004, W.ATT005, W.MS0k300,
    W.AG01h41, W.AG01h40, W.MS0k310, W.SCAT00, W.SCAU00, W.SEL01, W.PROA01, W.MS0k200, W.PROJ01, W.ATT010, W.RS00k400,
    W.RS00k310, W.ATT011, W.RS00k301, W.RS00k411, W.MS0k211, W.ATT012, W.MS0k201, W.ATT013, W.RS00k210, W.MS0k100,
    W.RS00k300, W.ATT014, W.ATT015, W.RS00k311, W.RS00k201, W.SCAT01, W.RS00k211, W.RS00k101, W.RS00k200, W.SCAU01,
    W.MS0k210, W.MS0k111, W.RS01k310, W.RS00k100, W.RS00k110, W.RS01k400, W.RS00k111, W.MS0k101, W.FO00, W.RS01k411,
    W.RS01k301, W.MID00, W.MS0k110, W.MG0s, W.RS01k300, W.RS01k210, W.UP000, W.UP001, W.RS01k311, W.RS01k201,
    W.DOW000, W.DOW001, W.NEWH00, W.MG0h10, W.AG10s, W.EXT1, W.RS01k200, W.RS01k211, W.MG0h11, W.AG10h10, W.RS01k101,
    W.RS01k110, W.AG10h11, W.RS01k111, W.RS01k100, W.FO01, W.MG0h21, W.AG10h20, W.MID01, W.AG10h21, W.UP010, W.MG0h20,
    W.UP011, W.DOW010, W.DOW011, W.AG10h31, W.AG10h30, W.MG0h31, W.MG0h30, W.NEWH01, W.AG11s, W.AG10h41, W.AG10h40,
    W.SEL10, W.AG11h10, W.PROA10, W.AG11h11, W.MG0h41, W.MG0h40, W.PROJ10, W.ATT100, W.MS1s, W.ATT101, W.AG11h20,
    W.AG11h21, W.ATT102, W.ATT103, W.MS1k411, W.ATT104, W.AG11h30, W.MS1k400, W.AG11h31, W.ATT105, W.SCAT10,
    W.MS1k300, W.AG11h40, W.AG11h41, W.SCAU10, W.MS1k301, W.RS10k310, W.MS1k311, W.SEL11, W.PROA11, W.RS10k400,
    W.MS1k200, W.RS10k411, W.MS1k310, W.PROJ11, W.ATT110, W.RS10k301, W.ATT111, W.ATT112, W.RS10k300, W.RS10k311,
    W.ATT113, W.RS10k210, W.MS1k211, W.MS1k210, W.RS10k201, W.ATT114, W.MS1k201, W.ATT115, W.RS10k200, W.RS10k211,
    W.SCAT11, W.MS1k100, W.SCAU11, W.MS1k111, W.MS1k110, W.RS10k111, W.RS11k400, W.RS10k110, W.RS10k101, W.RS10k100,
    W.MS1k101, W.RS11k411, W.RS11k310, W.MG1s, W.FO10, W.RS11k301, W.MID10, W.RS11k300, W.RS11k311, W.UP100,
    W.RS11k210, W.UP101, W.RS11k201, W.DOW100, W.MG1h11, W.RS11k200, W.RS11k211, W.DOW101, W.RS11k101, W.NEWH10,
    W.MG1h10, W.RS11k110, W.MG1h21, W.RS11k111, W.RS11k100, W.FO11, W.MID11, W.MG1h20, W.MG1h31, W.UP110, W.UP111,
    W.MG1h30, W.MG1h41, W.DOW110, W.DOW111, W.NEWH11, W.MG1h40,
)


def dot(a, b):
    return jnp.dot(a, b, preferred_element_type=F32)


def dot_by(a, b, left, right):
    return lax.dot_general(a, b, (((left,), (right,)), ((), ())), preferred_element_type=F32)


def exact_dot(x, onehot, right=A):
    high = x.astype(BF16)
    rest = x - high.astype(F32)
    mid = rest.astype(BF16)
    low = (rest - mid.astype(F32)).astype(BF16)
    out = dot_by(jnp.concatenate([high, mid, low], axis=A), onehot, B, right).reshape(FAR - 1, x.shape[A], -1)
    return out[A] + out[B] + out[PAIR]


def sums_to_rows(parts):
    axis = parts[A].ndim - PAIR
    sub = lax.broadcasted_iota(I32, parts[A].shape, axis)
    while len(parts) > 1:
        half = len(parts) // PAIR
        high = (sub & half) != 0
        parts = [
            jnp.where(high, a + pltpu.roll(a, half, axis), b + pltpu.roll(b, SUB - half, axis))
            for a, b in zip(parts[half:], parts[:half], strict=True)
        ]
    return parts[A]


def at_block(i, size):
    return pl.ds(pl.multiple_of(i * size, size), size)


def loop(count, body):
    def step(i, carry):
        body(i)
        return carry

    lax.fori_loop(A, count, step, A)


def takes(way, hop, half):
    return hop < FAR or way == half


def taken(hops=HOPS):
    return [(way, hop, half) for half in BOTH for way in BOTH for hop in hops if takes(way, hop, half)]


def mask_rows(ids, values, shape=None):
    out = jnp.zeros(shape or ids.shape, I32)
    for e in range(values.shape[A]):
        out = jnp.where(ids == values[e], 1, out)
    return out


def placed(ids, values, slots):
    entries = values.shape[A]
    row = lax.broadcasted_iota(I32, (entries, slots), A)
    out = jnp.zeros((entries, slots), F32)
    for e in range(entries):
        out = jnp.where(row == e, jnp.where(ids == values[e], 1.0, 0.0), out)
    return out.astype(BF16)


def main_kernel(
    n,
    src_ref, dst_ref, tab_ref, len_ref, x_ref, wq, wk, wv, wo, wu, wd, kp, vp,
    y_ref, knew_ref, vec_ref, mig_out,
    oh_ref, e_ref, es_ref, pres_ref, lane_ref, pick_ref, mg, mx, mr, mf,
    h_all, hsel, wbig, wk_v, wv_v, wo_v, wu_v, raw, kv_p, q_ref, kn_ref, kn_p, s_ref, oa, ob, a_ref, pd, rd,
    olhs, pf, rf, hm, act, ag_sent, ag_got, dd_sem, rs_sent, rs_got, x_sem, f_sem, m_sem, gs_sent, gs_got, gg_sent, gg_got,
    gp_sem, go_sem, p_sem, w_sem,
):
    me = lax.axis_index("kv")
    z, c = me // PAIR, lax.rem(me, PAIR)
    group = lax.axis_index("rep")
    peer = (group, z * PAIR + 1 - c)
    live = pl.ds(A, n.slots)
    half_d = n.d_model // PAIR
    heads_half = n.rep_heads // PAIR

    chips = {step: lax.rem(z + step + n.chips, n.chips) for step in range(-FAR, FAR + 1)}
    rings = {step: (group, PAIR * chips[step] + c) for step in (-1, 1)}
    h_rows = {step: (chips[step] * PAIR + c) * n.seqs for step in chips}

    def along(way, steps):
        return steps if way == A else -steps

    def on_ring(way, steps):
        return rings[along(way, steps)]

    def remote_by(src, dst, send, recv, target):
        return pltpu.make_async_remote_copy(
            src_ref=src, dst_ref=dst, send_sem=send, recv_sem=recv, device_id=target, device_id_type=MESH)

    def remote(src, dst, sems, at, target):
        return remote_by(src, dst, sems.at[(A, *at)], sems.at[(B, *at)], target)

    mine_o, mine_f = at_block(c, n.wide), at_block(c, n.ff_half)
    sources = {
        "q": lambda l: (wq.at[l], wbig.at[pl.ds(A, n.d_model), :]), "k": lambda l: (wk.at[l], wk_v), "v": lambda l: (wv.at[l], wv_v),
        "o": lambda l: (wo.at[l, mine_o, :], wo_v), "u": lambda l: (wu.at[l, :, mine_f], wu_v),
        "d": lambda l: (wd.at[l, mine_f, :], wbig.at[pl.ds(A, n.ff_half), :]),
    }
    follows = {"q": ("d", A), "d": ("q", B)} | {name: (name, B) for name in "kvou"}
    users = {name: PAIR for name in "qkvoud"}
    ready, used = set(), {}

    def load(name, l):
        src, dst = sources[name](l)
        return pltpu.make_async_copy(src, dst, w_sem.at[list(sources).index(name)])

    def need(names, l):
        for name in names:
            if (name, l) not in ready:
                ready.add((name, l))
                load(name, l).wait()

    def release(names, l):
        for name in names:
            used[name, l] = used.get((name, l), A) + 1
            after, more = follows[name]
            if used[name, l] == users[name] and l + more < n.layers:
                load(after, l + more).start()

    def gather(ref_of, sent, got, key):
        def copy(way, hop, half):
            ref = ref_of(along(way, 1 - hop), half)
            return remote_by(ref, ref, sent.at[key], got.at[key, way, hop - 1, half], on_ring(way, 1))

        return copy

    def gather_start(copy):
        for half in BOTH:
            for way in BOTH:
                copy(way, 1, half).start()

    def gather_hop(copy, hop, half, passed_on=None):
        for way in BOTH:
            if takes(way, hop, half):
                copy(way, hop, half).wait_recv()
                if hop < FAR and takes(way, hop + 1, half):
                    copy(way, hop + 1, half).start()
                if passed_on:
                    passed_on(way, hop, half).start()

    def total(src_of, got_of, sent, got, key):
        def copy(way, dist, half):
            return remote_by(
                src_of(along(way, dist), half), got_of(way, dist, half), sent.at[key], got.at[key, way, dist - 1, half],
                on_ring(way, 1))

        return copy

    def total_start(copy):
        for way in BOTH:
            copy(way, FAR, way).start()
        for way in BOTH:
            copy(way, FAR - 1, 1 - way).start()

    def total_hop(copy, add, dist, way, half):
        copy(way, dist, half).wait_recv()
        add(along(way, dist - 1), way, dist, half)
        if dist > 1:
            copy(way, dist - 1, half).start()

    ring_copies = len(taken())

    def all_sent(ref, sem):
        remote_by(ref, ref, sem, sem, peer).wait_send()

    def block(t, step, half):
        return h_all.at[t, pl.ds(pl.multiple_of(h_rows[step], n.seqs), n.seqs), pl.ds(half * half_d, half_d)]

    ag_copies = [gather(lambda step, half, t=t: block(t, step, half), ag_sent, ag_got, t) for t in BOTH]

    def to_peer(t):
        def copy(way, hop, half):
            ref = block(t, along(way, -hop), half)
            return remote(ref, ref, dd_sem, (t,), peer)

        return copy

    def ag_start(l, t):
        gather_start(ag_copies[t])
        for half in BOTH:
            to_peer(t)(A, A, half).start()

    def ag_hop(t, hop, half):
        gather_hop(ag_copies[t], hop, half, to_peer(t))

    def ag_finish(t):
        blocks = ring_copies // PAIR
        from_peer = h_all.at[t, pl.ds(A, (blocks + 1) * n.seqs), :]
        remote(from_peer, from_peer, dd_sem, (t,), peer).wait()
        all_sent(h_all.at[t, pl.ds(A, blocks * n.seqs), :], ag_sent.at[t])

    stats = pl.ds(n.sub, SUB)
    top_rows = lax.broadcasted_iota(I32, (SUB, LANES), A) < heads_half
    rs_copies = [
        total(lambda step, half, t=t: pd.at[t, chips[step], half], lambda way, d, half, t=t: rd.at[t, way, d - 1, half], rs_sent, rs_got, t)
        for t in BOTH
    ]

    def merge(t):
        def add(step, way, d, half):
            got, mine = rd.at[t, way, d - 1, half], pd.at[t, chips[step], half]
            s1, s2 = got[stats, :], mine[stats, :]
            m = jnp.maximum(s1, s2)
            a1, a2 = jnp.exp(s1 - m), jnp.exp(s2 - m)
            mine[stats, :] = jnp.where(top_rows, m, pltpu.roll(a1, heads_half, A) * s1 + pltpu.roll(a2, heads_half, A) * s2)
            at = pl.ds(A, n.sub)
            by_head = (heads_half, n.head, LANES)
            a1, a2 = (a[:heads_half][:, None] for a in (a1, a2))
            mine[at, :] = (a1 * got[at, :].reshape(by_head) + a2 * mine[at, :].reshape(by_head)).reshape(n.sub, LANES)

        return add

    def select(l, t):
        ag_finish(t)

        def body(i):
            cols = at_block(i, n.s_cols)
            hsel[:, cols] = dot(oh_ref[live, :], h_all[t, :, cols]).astype(BF16)

        loop(n.d_model // n.s_cols, body)

    def turned(w):
        rows = dot(hsel[...], w).astype(BF16).astype(F32)
        return jnp.concatenate([rows, jnp.zeros((LANES - n.slots, rows.shape[B]), F32)], axis=A).T

    units = (PAIR * (1 - c), PAIR * (1 - c) + 1, PAIR * c)
    spread_head = PAIR * c + 1
    first_part = LANES - n.slots

    def packed(u, own, other):
        rest = (other[..., :first_part], other[..., first_part:], own[..., n.slots :])[u]
        if rest.shape[-1] < first_part:
            pad = jnp.zeros((*own.shape[:-1], first_part - rest.shape[-1]), own.dtype)
            rest = jnp.concatenate([rest, pad], axis=-1) if rest.shape[-1] else pad
        return jnp.concatenate([own, rest], axis=-1)

    def query(kvh):
        return turned(wbig[pl.ds(A, n.d_model), at_block(kvh, n.own_rows)])[:, : n.slots]

    def project_first(l, t):
        need("qkv", l)
        other = query(spread_head)
        for u in BOTH:
            q_ref[u] = packed(u, query(units[u]), other)

    def project(l, t):
        own = query(units[PAIR])
        q_ref[PAIR] = packed(PAIR, own, own)
        for i, w in enumerate((wk_v, wv_v)):
            kn_ref[t, i] = turned(w[...])
            knew_ref[l, t, i] = kn_ref[t, i].astype(BF16)
            for u, kvh in enumerate(units):
                own, other = (kn_ref[t, i, at_block(head, n.head), live] for head in (kvh, spread_head))
                kn_p[t, i, at_block(u, n.head), :] = packed(u, own, other)
        release("qkv", l)

    heads = range(n.rep_heads)

    def outputs(t, u):
        return oa.at[t, jnp.where(u < PAIR, 1 - c, c), jnp.where(u < PAIR, u, A)]

    def pages(w, at, u):
        return kv_p[w, at, at_block(u, n.head), :].astype(F32)

    def attend(t, u):
        rows = at_block(u, n.head)
        scale = n.head ** -0.5
        out = outputs(t, u)

        def scores(keys):
            parts = []
            for h in heads:
                prods = q_ref[u, pl.ds(h * n.head, n.head), :][None] * keys
                acc = prods[:, :SUB]
                for d in range(SUB, n.head, SUB):
                    acc = acc + prods[:, d : d + SUB]
                parts.append(acc)
            return sums_to_rows(parts)

        def qk(i):
            at = pl.ds(i * FAR, FAR)
            s_ref[at, :, :] = scores(pages(A, at, u))

        loop(n.page // FAR, qk)
        fresh = range(t + 1)
        news = [scores(kn_p[i, A, rows, :][None])[A] for i in fresh]
        lim, has_new = lane_ref[pl.ds(PAIR * u, 1), :], lane_ref[pl.ds(PAIR * u + 1, 1), :] > 0
        news = [jnp.where(has_new, s * scale, NEG) for s in news]
        valid = lax.broadcasted_iota(I32, (n.page, n.rep_heads, lim.shape[B]), A) < lim[None]
        old = jnp.where(valid, s_ref[:, :, :] * scale, NEG)
        m = jnp.max(old, axis=A)
        for s in news:
            m = jnp.maximum(m, s)
        probs = jnp.where(valid, jnp.exp(old - m[None]), 0.0)
        s_ref[:, :, :] = probs
        news = [jnp.where(has_new, jnp.exp(s - m), 0.0) for s in news]
        count = jnp.sum(probs, axis=A)
        for p in news:
            count = count + p
        out[pl.ds(n.own_rows, SUB), :] = m
        out[pl.ds(n.own_rows + SUB, SUB), :] = count
        vals = [kn_p[i, B, rows, :] for i in fresh]
        for h in heads:
            acc = news[A][h : h + 1] * vals[A]
            for p, v in zip(news[1:], vals[1:], strict=True):
                acc = acc + p[h : h + 1] * v
            out[pl.ds(h * n.head, n.head), :] = acc

    def attend_values(t, u):
        out = outputs(t, u)

        def pv(i):
            vals = [v for v in pages(B, pl.ds(i * FAR, FAR), u)]
            ps = [s_ref[i * FAR + j, :, :] for j in range(FAR)]
            for h in heads:
                at = pl.ds(h * n.head, n.head)
                acc = out[at, :]
                for p, v in zip(ps, vals, strict=True):
                    acc = acc + p[h : h + 1] * v
                out[at, :] = acc

        loop(n.page // FAR, pv)

    def exchange(t):
        return remote(oa.at[t, 1 - c], ob.at[t], x_sem, (t,), peer)

    def attend_all(l, t, between):
        def body(u):
            attend(t, u)
            for at, work in between.items():
                if at % PAIR == A:
                    pl.when(u == at // PAIR)(work)
            attend_values(t, u)
            pl.when(u == B)(lambda: exchange(t).start())
            for at, work in between.items():
                if at % PAIR == B:
                    pl.when(u == at // PAIR)(work)

        loop(len(units), body)
        lane = lax.broadcasted_iota(I32, (1, LANES), B)
        near, far = (pltpu.roll(oa[t, 1 - c, v], first_part * (v + 1), B) for v in BOTH)
        oa[t, c, B] = jnp.where(lane < first_part, near, far)

    low_lanes = lax.broadcasted_iota(I32, (1, LANES), B) < n.pair

    def by_chip(parts, put):
        for zp in range(n.chips // PAIR):
            a, b = (p[:, zp * LANES : (zp + 1) * LANES] for p in parts)
            put(PAIR * zp, jnp.where(low_lanes, a, pltpu.roll(b, n.pair, B)))
            put(PAIR * zp + 1, jnp.where(low_lanes, pltpu.roll(a, n.pair, B), b))

    def both_cores(t, hh, at):
        return jnp.concatenate([oa[t, c, hh, at, :], ob[t, hh, at, :]], axis=B)

    def scatter(l, t):
        exchange(t).wait()
        top, count = (
            jnp.concatenate([both_cores(t, hh, pl.ds(n.own_rows + off, SUB)) for hh in BOTH], axis=A) for off in (A, SUB))
        m_page = [jnp.where(pres_ref[pl.ds(p, 1), :] > 0, exact_dot(top, e_ref[p]), NEG) for p in BOTH]
        m_seq = jnp.maximum(*m_page)
        a = jnp.exp(jnp.minimum(top - exact_dot(m_seq, es_ref[...], right=B), 0.0))
        a_ref[A], a_ref[B] = a[:SUB], a[SUB:]
        l_seq = exact_dot(count * a, es_ref[...])
        dense = {}
        for what, v in enumerate((m_seq, l_seq)):
            by_chip([v[:SUB], v[SUB:]], lambda zz, v, what=what: dense.update({(zz, what): v}))
        for zz in range(n.chips):
            m, l = dense[zz, A], dense[zz, B]
            pd[t, zz, A, stats, :] = jnp.where(top_rows, m, pltpu.roll(l, heads_half, A))
            pd[t, zz, B, stats, :] = jnp.where(top_rows, pltpu.roll(m, heads_half, A), l)

        scatter_half(A, l, t)

    def scatter_half(half, l, t):
        def body(k):
            for j in range(heads_half // PAIR):
                i = k * PAIR + j
                h = half * heads_half + i
                parts = [
                    exact_dot(both_cores(t, hh, at_block(h, n.head)) * a_ref[hh, pl.ds(h, 1), :], es_ref[...]) for hh in BOTH]

                def put(zz, v, i=i):
                    pd[t, zz, half, at_block(i, n.head), :] = v

                by_chip(parts, put)

        loop(PAIR, body)
        for way in BOTH:
            rs_copies[t](way, FAR if way == half else FAR - 1, half).start()

    def f_copy(t, stage):
        return remote(pf.at[t, 1 - c], rf.at[t, stage], f_sem, (t, stage), peer)

    def m_copy(t):
        return remote(hm.at[t, c], hm.at[t, c], m_sem, (t,), peer)

    def product(t, lhs, w, between):
        def body(i):
            cols = at_block(i, n.s_cols)
            val = dot(lhs(), w(cols))
            pf[t, A, :, cols] = val[: n.seqs]
            pf[t, B, :, cols] = val[n.seqs :]
            for at, work in between.items():
                pl.when(i == at)(work)

        loop(n.d_model // n.s_cols, body)

    own = pl.ds(pl.multiple_of(h_rows[A], n.seqs), n.seqs)

    def out_proj(l, t):
        all_sent(pd.at[t, pl.ds(A, ring_copies // PAIR)], rs_sent.at[t])
        for half in BOTH:
            mine = pd.at[t, z, half]
            inv = (1.0 / mine[stats, :])[heads_half:][:, None]
            flat = (mine[pl.ds(A, n.sub), :].reshape(heads_half, n.head, LANES) * inv).reshape(n.sub, LANES).T.astype(BF16)
            for hh in BOTH:
                olhs[:, pl.ds(hh * n.own_rows + half * n.sub, n.sub)] = flat[hh * n.pair : (hh + 1) * n.pair]
        need("o", l)
        product(t, lambda: olhs[...], lambda cols: wo_v[:, cols], {})
        release("o", l)
        f_copy(t, A).start()

    def mid(l, t):
        f_copy(t, A).wait()
        hm[t, c] = (h_all[t, own, :].astype(F32) + (pf[t, c] + rf[t, A])).astype(BF16)
        m_copy(t).start()

    def up(l, t, halfway):
        m_copy(t).wait()
        need("u", l)

        def body(i):
            cols = at_block(i, n.u_cols)
            u = dot(hm[t].reshape(n.pair, n.d_model), wu_v[:, cols]).astype(BF16).astype(F32)
            act[t, :, cols] = jax.nn.gelu(u, approximate=True).astype(BF16)
            for at, work in halfway.items():
                pl.when(i == at)(work)

        loop(n.ff_half // n.u_cols, body)
        release("u", l)

    def down(l, t, between):
        need("d", l)
        product(t, lambda: act[t], lambda cols: wbig[pl.ds(A, n.ff_half), cols], between)
        release("d", l)
        f_copy(t, B).start()

    def new_h(l, t):
        f_copy(t, B).wait()
        new = (hm[t, c].astype(F32) + (pf[t, c] + rf[t, B])).astype(BF16)
        h_all[t, own, :] = new
        y_ref[t] = new

    def ids_of(dev, axis):
        at = lax.broadcasted_iota(I32, (LANES, 1) if axis == A else (1, LANES), axis)
        return jnp.where(at < n.slots, dev * n.slots + at, -1)

    def tables():
        oa[...] = jnp.zeros_like(oa)
        for g, dev in enumerate((me, z * PAIR + 1 - c)):
            ids = ids_of(dev, A)
            target = ids
            for e in range(n.entries):
                target = jnp.where(ids == src_ref[e], dst_ref[e], target)
            stale = mask_rows(ids, dst_ref)
            hit = [jnp.where(tab_ref[pl.ds(p, 1), :] == target, 1.0, 0.0) for p in BOTH]
            now = [jnp.where(stale == 0, h, 0.0) for h in hit]
            at = pl.ds(g * LANES, LANES)
            for p in BOTH:
                e_ref[p, at, :] = now[p].astype(BF16)
            es_ref[at, :] = (now[A] + now[B]).astype(BF16)
            if g == A:
                oh_ref[...] = (hit[A] + hit[B]).astype(BF16)
                held = [h.astype(BF16) for h in (*now, hit[B])]
        for p in BOTH:
            pres_ref[pl.ds(p, 1), :] = jnp.sum(e_ref[p].astype(F32), axis=A, keepdims=True)
        lens = len_ref[...].astype(F32)
        rows = jnp.concatenate([lens, jnp.ones((SUB - 1, lens.shape[B]), F32)], axis=A).astype(BF16)
        first, last, fresh = (dot_by(rows, h, B, B) for h in held)
        at0, at1 = slice(A, 1), slice(B, PAIR)
        limit = jnp.where(first[at1] > 0, jnp.minimum(first[at0], n.page), jnp.where(last[at1] > 0, last[at0] - n.page, 0.0))
        for i, row in enumerate((limit, last[at1])):
            row = row[:, : n.slots]
            for u in range(len(units)):
                lane_ref[pl.ds(PAIR * u + i, 1), :] = packed(u, row, row).astype(I32)
        ids = ids_of(me, B)
        is_src, is_dst = mask_rows(ids, src_ref), mask_rows(ids, dst_ref)
        pick_ref[...] = placed(ids[:, : n.slots], src_ref, n.slots)
        on_last = jnp.where(is_src == 0, fresh[at1], 0.0) > 0
        start = fresh[at0] - n.page
        vec_ref[...] = jnp.where(is_src + is_dst == 0, 1.0, 0.0) * jnp.ones((SUB, LANES), F32)
        for t in BOTH:
            vec_ref[pl.ds(t, 1), :] = jnp.where(on_last, start + t, -1.0)

    m_cols = mf.shape[B] // n.chips // PAIR

    def mig_pair():
        return remote(mg.at[1 - c], mx, gp_sem, (), peer)

    def m_at(step, half):
        return at_block(chips[step] * PAIR + half, m_cols)

    ms_copies, mg_copies = [], []
    for l in range(n.layers):
        ms_copies.append(total(lambda step, half: mg.at[c, :, m_at(step, half)], lambda way, d, half: mr.at[way, d - 1, half], gs_sent, gs_got, l))
        mg_copies.append(gather(lambda step, half: mf.at[:, m_at(step, half)], gg_sent, gg_got, l))

    def mig_add(step, way, d, half):
        at = m_at(step, half)
        mg[c, :, at] = mg[c, :, at] + mr[way, d - 1, half]

    m_ring = pl.ds(A, ring_copies * m_cols)

    def mig_sent(l):
        all_sent(mg.at[c, :, m_ring], gs_sent.at[l])

    def mig_out_copies(l):
        return remote(mf, mig_out.at[l, c], go_sem, (l,), peer), pltpu.make_async_copy(mf, mig_out.at[l, c], go_sem.at[PAIR, l])

    def page_loads(l, i, slot):
        at = pl.ds(pl.multiple_of(i * SUB, SUB), SUB)
        return [pltpu.make_async_copy(pool.at[l, at], raw.at[slot, w], p_sem.at[slot, w]) for w, pool in enumerate((kp, vp))]

    def first_pages(l):
        for i in range(raw.shape[A]):
            for copy in page_loads(l, i, i):
                copy.start()

    def extract(l):
        if l > 0:
            mig_sent(l - 1)
        chunks, held = n.page // SUB, raw.shape[A]

        def body(i):
            slot = lax.rem(i, held)
            for copy in page_loads(l, i, slot):
                copy.wait()
            at = pl.ds(pl.multiple_of(i * SUB, SUB), SUB)
            for w in BOTH:
                rows = raw[slot, w].reshape(SUB * n.kv_cols, n.slots)
                mg[w, :, at_block(i, SUB * n.kv_cols)] = dot_by(pick_ref[...], rows, B, B).astype(BF16)
                other = raw[slot, w, :, at_block(spread_head, n.head), :]
                for u, kvh in enumerate(units):
                    kv_p[w, at, at_block(u, n.head), :] = packed(u, raw[slot, w, :, at_block(kvh, n.head), :], other)

            @pl.when(i + held < chunks)
            def _():
                for copy in page_loads(l, i + held, slot):
                    copy.start()

        loop(chunks, body)
        if l + 1 < n.layers:
            first_pages(l + 1)
        mig_pair().start()

    def mig_start(l):
        if l > 0:
            for copy in mig_out_copies(l - 1):
                copy.wait()
        mig_pair().wait()
        mg[c] = mg[c] + mx[...]
        total_start(ms_copies[l])

    def mig_gather(l):
        gather_start(mg_copies[l])

    def mig_own():
        for half in BOTH:
            mf[:, m_at(A, half)] = mg[c, :, m_at(A, half)]

    def mig_end(l):
        all_sent(mf.at[:, m_ring], gg_sent.at[l])
        for copy in mig_out_copies(l):
            copy.start()

    steps = {"TAB": tables}
    for l in range(n.layers):
        steps[f"EXT{l}"] = functools.partial(extract, l)
        steps[f"MS{l}s"] = functools.partial(mig_start, l)
        steps[f"MG{l}s"] = functools.partial(mig_gather, l)
        for hop in HOPS:
            for half in BOTH:
                steps[f"MG{l}h{hop}{half}"] = functools.partial(gather_hop, mg_copies[l], hop, half)
                for way in BOTH:
                    steps[f"MS{l}k{hop}{way}{half}"] = functools.partial(total_hop, ms_copies[l], mig_add, hop, way, half)
        for t in BOTH:
            for name, work in (
                ("SEL", select), ("PROA", project_first), ("PROJ", project), ("SCAT", scatter), ("SCAU", functools.partial(scatter_half, B)), ("FO", out_proj), ("MID", mid), ("NEWH", new_h),
            ):
                steps[f"{name}{l}{t}"] = functools.partial(work, l, t)
            steps[f"AG{l}{t}s"] = functools.partial(ag_start, l, t)
            for hop in HOPS:
                for half in BOTH:
                    steps[f"AG{l}{t}h{hop}{half}"] = functools.partial(ag_hop, t, hop, half)
                    for way in BOTH:
                        steps[f"RS{l}{t}k{hop}{way}{half}"] = functools.partial(total_hop, rs_copies[t], merge(t), hop, way, half)

    for t in BOTH:
        h_all[t, own, :] = x_ref[t]
    first_pages(A)
    load("q", A).start()
    barrier = pltpu.get_barrier_semaphore()
    others = (peer, *rings.values())
    for target in others:
        pl.semaphore_signal(barrier, inc=1, device_id=target, device_id_type=MESH)
    pl.semaphore_wait(barrier, len(others))

    def later_loads():
        for name in ("k", "v", "o", "u"):
            load(name, A).start()


    steps["LOADS"] = later_loads
    todo = list(ORDER)
    todo.insert(PAIR, "LOADS")
    on_way = {kind: len([name for name in todo if name.startswith(kind)]) for l in range(n.layers) for kind in (f"MS{l}k", f"MG{l}h")}

    def run(names):
        for name in names:
            steps[name]()
            kind = name[:FAR]
            if kind in on_way:
                on_way[kind] -= 1
                if on_way[kind] == 0:
                    mig_end(int(kind[PAIR])) if "h" in kind else mig_own()

    loops = {"ATT": (attend_all, PAIR * len(units)), "UP": (up, n.ff_half // n.u_cols), "DOW": (down, n.d_model // n.s_cols)}
    while todo:
        name = todo.pop(A)
        word = name.rstrip("0123456789")
        if word in loops:
            work, count = loops[word]
            l, t, _ = (int(ch) for ch in name[len(word) :])
            between = {}
            for i in range(count - 1):
                upto = todo.index(f"{word}{l}{t}{i + 1}")
                if upto:
                    between[i] = functools.partial(run, todo[:upto])
                todo = todo[upto + 1 :]
            work(l, t, between)
        else:
            run([name])
    for copy in mig_out_copies(n.layers - 1):
        copy.wait()
    mig_sent(n.layers - 1)


def pool_kernel(dst_ref, vec_ref, mig_ref, new_ref, y_ref, k_ref, v_ref, ko_ref, vo_ref, yo_ref, moved, move_ref):
    step, rows, slots = k_ref.shape[1:]
    live = slice(A, slots)
    group = moved.shape[1] // rows
    tab = vec_ref[...]
    at0, at1, keep = (tab[i : i + 1, live].astype(BF16) for i in range(PAIR + 1))
    keep = keep > 0
    base = pl.program_id(B) * step
    turns = [(which, g) for which in BOTH for g in range(step // group)]

    @pl.when((pl.program_id(A) == 0) & (pl.program_id(B) == 0))
    def _():
        yo_ref[...] = y_ref[...]
        ids = lax.axis_index("kv") * slots + lax.broadcasted_iota(I32, (1, slots), B)
        move_ref[...] = placed(ids, dst_ref, slots)

    def move(which, g, slot):
        moved[slot] = dot_by(mig_ref[A, which, :, g * group * rows : (g + 1) * group * rows], move_ref[...], A, A).astype(BF16)

    move(A, A, A)
    for i, (which, g) in enumerate(turns):
        if i + 1 < len(turns):
            move(*turns[i + 1], (i + 1) % PAIR)
        pool_ref, out_ref = ((k_ref, ko_ref), (v_ref, vo_ref))[which]
        for j in range(group):
            r = g * group + j
            pos = jnp.full((1, slots), (base + r).astype(F32), F32).astype(BF16)
            val = jnp.where(keep, pool_ref[A, r], moved[i % PAIR, j * rows : (j + 1) * rows, :])
            val = jnp.where(at0 == pos, new_ref[A, A, which, :, live], val)
            out_ref[A, r] = jnp.where(at1 == pos, new_ref[A, B, which, :, live], val)


def new_pools(pools, mig, knew, vec, dst, y):
    layers, page, rows, slots = pools[A].shape
    step, group = page // PAIR, FAR
    entries = mig.shape[PAIR]
    block = pl.BlockSpec((1, step, rows, slots), lambda l, i: (l, i, A, A))
    whole = pl.BlockSpec(y.shape, lambda l, i: (A, A, A))
    return pl.pallas_call(
        pool_kernel,
        out_shape=[jax.ShapeDtypeStruct(pools[A].shape, BF16)] * PAIR + [jax.ShapeDtypeStruct(y.shape, BF16)],
        grid=(layers, page // step),
        in_specs=[
            pl.BlockSpec(memory_space=pltpu.SMEM),
            pl.BlockSpec(vec.shape, lambda l, i: (A, A)),
            pl.BlockSpec((1, PAIR, entries, step * rows), lambda l, i: (l, A, A, i)),
            pl.BlockSpec((1, PAIR, PAIR, rows, LANES), lambda l, i: (l, A, A, A, A)),
            whole, block, block,
        ],
        out_specs=[block, block, whole],
        scratch_shapes=[pltpu.VMEM((PAIR, group * rows, slots), BF16), pltpu.VMEM((entries, slots), BF16)],
        compiler_params=pltpu.CompilerParams(dimension_semantics=("arbitrary",) * PAIR, vmem_limit_bytes=VMEM_BYTES),
        name="new_pools",
    )(dst, vec, mig, knew, y, *pools)


def solution(mesh):
    devs = mesh.shape["kv"]
    pool_spec = P(("rep", "kv"))
    tok_spec = P(None, ("rep", "kv"), None)

    def device_fn(embeds, w_query, w_key, w_value, w_out, w_up, w_down, k_pool, v_pool, new_table, seq_lens, mig_src, mig_dst):
        slots, layers, page, kv_heads, head = k_pool.shape
        seqs, d_model = embeds.shape[1:]
        rep_heads = w_query.shape[-1] // head // kv_heads
        own_rows = rep_heads * head
        n = SimpleNamespace(
            layers=layers, d_model=d_model, ff_half=w_up.shape[-1] // PAIR, chips=devs // PAIR, seqs=seqs, pair=PAIR * seqs,
            slots=slots, kv_heads=kv_heads, head=head, page=page, rep_heads=rep_heads, own_rows=own_rows, sub=own_rows // PAIR,
            wide=kv_heads // PAIR * own_rows, kv_cols=kv_heads * head, entries=mig_src.shape[A],
            s_cols=d_model // PAIR, d_cols=d_model // FAR, u_cols=w_up.shape[-1] // FAR)
        total = seqs * devs
        pages = page * n.kv_cols
        pools = [jnp.moveaxis(p, A, -1).reshape(layers, page, n.kv_cols, slots) for p in (k_pool, v_pool)]
        dma, two = pltpu.SemaphoreType.DMA, PAIR
        ring = (two, FAR, two)
        bf = lambda *shape: pltpu.VMEM(shape, BF16)
        f32 = lambda *shape: pltpu.VMEM(shape, F32)
        hbm, vmem, smem = (pl.BlockSpec(memory_space=m) for m in (pl.ANY, pltpu.VMEM, pltpu.SMEM))
        y, knew, vec, mig = pl.pallas_call(
            functools.partial(main_kernel, n),
            out_shape=[
                jax.ShapeDtypeStruct((two, seqs, d_model), BF16),
                jax.ShapeDtypeStruct((layers, two, two, n.kv_cols, LANES), BF16),
                jax.ShapeDtypeStruct((SUB, LANES), F32),
                jax.ShapeDtypeStruct((layers, two, n.entries, pages), BF16),
            ],
            in_specs=[smem] * two + [vmem] * (two + 1) + [hbm] * SUB,
            out_specs=[vmem] * (two + 1) + [hbm],
            scratch_shapes=[
                bf(LANES, total), bf(two, two * LANES, total), bf(two * LANES, total), f32(SUB, total), pltpu.VMEM((SUB, LANES), I32),
                bf(n.entries, slots), bf(two, n.entries, pages), bf(n.entries, pages),
                bf(two, FAR, two, n.entries, pages // devs), bf(n.entries, pages),
                bf(two, total, d_model), bf(slots, d_model), bf(max(d_model, n.ff_half), d_model), bf(d_model, n.kv_cols),
                bf(d_model, n.kv_cols), bf(n.wide, d_model), bf(d_model, n.ff_half), bf(two + 1, two, SUB, n.kv_cols, slots), bf(two, page, (kv_heads - 1) * head, LANES),
                f32(kv_heads - 1, own_rows, LANES), f32(two, two, n.kv_cols, LANES), f32(two, two, (kv_heads - 1) * head, LANES), f32(page, rep_heads, LANES),
                f32(two, two, two, own_rows + two * SUB, LANES), f32(two, two, own_rows + two * SUB, LANES),
                f32(two, rep_heads, two * LANES), f32(two, n.chips, two, n.sub + SUB, LANES),
                f32(two, two, FAR, two, n.sub + SUB, LANES), bf(n.pair, n.wide), f32(two, two, seqs, d_model),
                f32(two, two, seqs, d_model), bf(two, two, seqs, d_model), bf(two, n.pair, n.ff_half),
                dma((two,)), dma((two, *ring)), dma((two, two)), dma((two,)), dma((two, *ring)), dma((two, two)),
                dma((two, two, two)), dma((two, two)), dma((layers,)), dma((layers, *ring)), dma((layers,)), dma((layers, *ring)),
                dma((two,)), dma((two + 1, layers)), dma((two + 1, two)), dma((SUB,)),
            ],
            compiler_params=pltpu.CompilerParams(collective_id=A, has_side_effects=True, vmem_limit_bytes=VMEM_BYTES),
            name="decode",
        )(mig_src, mig_dst, new_table.T, seq_lens[None], embeds, w_query, w_key, w_value, w_out, w_up, w_down, *pools)
        *outs, y = new_pools(pools, mig, knew, vec, mig_dst, y)
        outs = [jnp.moveaxis(p.reshape(layers, page, kv_heads, head, slots), -1, A) for p in outs]
        return y, *outs

    return jax.shard_map(
        device_fn, mesh=mesh,
        in_specs=(tok_spec, *(P(),) * (SUB - PAIR), pool_spec, pool_spec, P("rep", None), *(P("rep"),) * (FAR - 1)),
        out_specs=(tok_spec, pool_spec, pool_spec), check_vma=False)
```

```python
import functools
from types import SimpleNamespace

import jax
import jax.numpy as jnp
from jax import lax
from jax.experimental import pallas as pl
from jax.experimental.pallas import tpu as pltpu
from jax.sharding import PartitionSpec as P

MESH = pl.DeviceIdType.MESH
F32, BF16, I32 = jnp.float32, jnp.bfloat16, jnp.int32
NEG = -1e30
LANES = 128
SUB = 8
A, B = BOTH = range(2)
PAIR = len(BOTH)
VMEM_BYTES = 67043328
FAR = 4
HOPS = range(1, FAR + 1)


class Names:
    def __getattr__(self, name):
        return name


W = Names()
ORDER = (
    W.AG00s, W.AG01s, W.TAB, W.AG00h10, W.AG00h11, W.EXT0, W.AG00h20, W.AG00h21, W.AG01h10, W.MS0s, W.AG01h11,
    W.AG00h30, W.AG00h31, W.AG01h21, W.MS0k301, W.MS0k400, W.MS0k411, W.MS0k310, W.AG01h20, W.AG00h41, W.AG00h40,
    W.SEL00, W.PROA00, W.PROJ00, W.ATT000, W.MS0k311, W.ATT001, W.ATT002, W.AG01h31, W.AG01h30, W.ATT003, W.MS0k201,
    W.ATT004, W.MS0k300, W.MS0k210, W.ATT005, W.SCAT00, W.AG01h40, W.AG01h41, W.SCAU00, W.SEL01, W.PROA01, W.PROJ01,
    W.RS00k310, W.RS00k400, W.ATT010, W.ATT011, W.RS00k411, W.RS00k301, W.MS0k110, W.ATT012, W.MS0k211, W.RS00k210,
    W.MS0k200, W.RS00k300, W.ATT013, W.ATT014, W.RS00k201, W.RS00k311, W.ATT015, W.SCAT01, W.SCAU01, W.MS0k111,
    W.RS00k101, W.RS00k200, W.MS0k100, W.RS00k211, W.RS01k310, W.RS01k400, W.RS01k411, W.MS0k101, W.RS01k301, W.MG0s,
    W.RS00k100, W.RS00k111, W.RS00k110, W.FO00, W.MID00, W.RS01k300, W.RS01k210, W.UP000, W.RS01k311, W.UP001,
    W.RS01k201, W.DOW000, W.MG0h11, W.DOW001, W.NEWH00, W.AG10s, W.RS01k211, W.RS01k200, W.MG0h10, W.RS01k110, W.EXT1,
    W.AG10h11, W.AG10h10, W.RS01k101, W.RS01k100, W.MG0h21, W.RS01k111, W.FO01, W.MG0h20, W.AG10h21, W.MID01,
    W.AG10h20, W.UP010, W.MG0h31, W.UP011, W.AG10h31, W.MG0h30, W.DOW010, W.AG10h30, W.DOW011, W.NEWH01, W.AG11s,
    W.AG10h41, W.AG10h40, W.SEL10, W.PROA10, W.AG11h10, W.MG0h40, W.PROJ10, W.AG11h11, W.MG0h41, W.MS1s, W.ATT100,
    W.ATT101, W.AG11h20, W.ATT102, W.AG11h21, W.ATT103, W.ATT104, W.MS1k411, W.AG11h30, W.MS1k301, W.MS1k310,
    W.MS1k400, W.ATT105, W.AG11h31, W.SCAT10, W.SCAU10, W.AG11h41, W.AG11h40, W.SEL11, W.MS1k311, W.MS1k300, W.PROA11,
    W.RS10k310, W.RS10k400, W.MS1k210, W.PROJ11, W.MS1k201, W.ATT110, W.RS10k301, W.RS10k411, W.MS1k200, W.ATT111,
    W.ATT112, W.RS10k300, W.RS10k210, W.ATT113, W.ATT114, W.MS1k211, W.RS10k311, W.RS10k201, W.ATT115, W.SCAT11,
    W.RS10k200, W.MS1k101, W.SCAU11, W.RS10k110, W.MS1k111, W.RS10k101, W.RS10k211, W.RS11k411, W.RS11k400,
    W.RS10k100, W.MS1k110, W.RS11k301, W.RS11k310, W.MS1k100, W.RS10k111, W.FO10, W.MG1s, W.RS11k311, W.RS11k300,
    W.MID10, W.UP100, W.UP101, W.RS11k210, W.RS11k201, W.MG1h11, W.DOW100, W.RS11k200, W.RS11k211, W.MG1h10,
    W.RS11k110, W.RS11k101, W.RS11k100, W.MG1h21, W.RS11k111, W.FO11, W.MG1h20, W.DOW101, W.MID11, W.UP110, W.MG1h30,
    W.MG1h31, W.UP111, W.DOW110, W.DOW111, W.NEWH10, W.MG1h41, W.MG1h40, W.NEWH11,
)


def dot(a, b):
    return jnp.dot(a, b, preferred_element_type=F32)


def dot_by(a, b, left, right):
    return lax.dot_general(a, b, (((left,), (right,)), ((), ())), preferred_element_type=F32)


def exact_dot(x, onehot, right=A):
    high = x.astype(BF16)
    rest = x - high.astype(F32)
    mid = rest.astype(BF16)
    low = (rest - mid.astype(F32)).astype(BF16)
    out = dot_by(jnp.concatenate([high, mid, low], axis=A), onehot, B, right).reshape(FAR - 1, x.shape[A], -1)
    return out[A] + out[B] + out[PAIR]


def sums_to_rows(parts):
    axis = parts[A].ndim - PAIR
    sub = lax.broadcasted_iota(I32, parts[A].shape, axis)
    while len(parts) > 1:
        half = len(parts) // PAIR
        high = (sub & half) != 0
        parts = [
            jnp.where(high, a + pltpu.roll(a, half, axis), b + pltpu.roll(b, SUB - half, axis))
            for a, b in zip(parts[half:], parts[:half], strict=True)
        ]
    return parts[A]


def at_block(i, size):
    return pl.ds(pl.multiple_of(i * size, size), size)


def loop(count, body):
    def step(i, carry):
        body(i)
        return carry

    lax.fori_loop(A, count, step, A)


def takes(way, hop, half):
    return hop < FAR or way == half


def taken(hops=HOPS):
    return [(way, hop, half) for half in BOTH for way in BOTH for hop in hops if takes(way, hop, half)]


def mask_rows(ids, values, shape=None):
    out = jnp.zeros(shape or ids.shape, I32)
    for e in range(values.shape[A]):
        out = jnp.where(ids == values[e], 1, out)
    return out


def placed(ids, values, slots):
    entries = values.shape[A]
    row = lax.broadcasted_iota(I32, (entries, slots), A)
    out = jnp.zeros((entries, slots), F32)
    for e in range(entries):
        out = jnp.where(row == e, jnp.where(ids == values[e], 1.0, 0.0), out)
    return out.astype(BF16)


def main_kernel(
    n,
    src_ref, dst_ref, tab_ref, len_ref, x_ref, wq, wk, wv, wo, wu, wd, kp, vp,
    y_ref, knew_ref, vec_ref, mig_out,
    oh_ref, e_ref, es_ref, pres_ref, lane_ref, pick_ref, mg, mx, mr, mf,
    h_all, hsel, wbig, wk_v, wv_v, wo_v, wu_v, raw, kv_p, q_ref, kn_ref, kn_p, s_ref, oa, ob, a_ref, pd, rd,
    olhs, pf, rf, hm, act, ag_sent, ag_got, dd_sem, rs_sent, rs_got, x_sem, f_sem, m_sem, gs_sent, gs_got, gg_sent, gg_got,
    gp_sem, go_sem, p_sem, w_sem,
):
    me = lax.axis_index("kv")
    z, c = me // PAIR, lax.rem(me, PAIR)
    group = lax.axis_index("rep")
    peer = (group, z * PAIR + 1 - c)
    live = pl.ds(A, n.slots)
    half_d = n.d_model // PAIR
    heads_half = n.rep_heads // PAIR

    chips = {step: lax.rem(z + step + n.chips, n.chips) for step in range(-FAR, FAR + 1)}
    rings = {step: (group, PAIR * chips[step] + c) for step in (-1, 1)}
    h_rows = {step: (chips[step] * PAIR + c) * n.seqs for step in chips}

    def along(way, steps):
        return steps if way == A else -steps

    def on_ring(way, steps):
        return rings[along(way, steps)]

    def remote_by(src, dst, send, recv, target):
        return pltpu.make_async_remote_copy(
            src_ref=src, dst_ref=dst, send_sem=send, recv_sem=recv, device_id=target, device_id_type=MESH)

    def remote(src, dst, sems, at, target):
        return remote_by(src, dst, sems.at[(A, *at)], sems.at[(B, *at)], target)

    mine_o, mine_f = at_block(c, n.wide), at_block(c, n.ff_half)
    sources = {
        "q": lambda l: (wq.at[l], wbig.at[pl.ds(A, n.d_model), :]), "k": lambda l: (wk.at[l], wk_v), "v": lambda l: (wv.at[l], wv_v),
        "o": lambda l: (wo.at[l, mine_o, :], wo_v), "u": lambda l: (wu.at[l, :, mine_f], wu_v),
        "d": lambda l: (wd.at[l, mine_f, :], wbig.at[pl.ds(A, n.ff_half), :]),
    }
    follows = {"q": ("d", A), "d": ("q", B)} | {name: (name, B) for name in "kvou"}
    users = {name: PAIR for name in "qkvoud"}
    ready, used = set(), {}

    def load(name, l):
        src, dst = sources[name](l)
        return pltpu.make_async_copy(src, dst, w_sem.at[list(sources).index(name)])

    def need(names, l):
        for name in names:
            if (name, l) not in ready:
                ready.add((name, l))
                load(name, l).wait()

    def release(names, l):
        for name in names:
            used[name, l] = used.get((name, l), A) + 1
            after, more = follows[name]
            if used[name, l] == users[name] and l + more < n.layers:
                load(after, l + more).start()

    def gather(ref_of, sent, got, key):
        def copy(way, hop, half):
            ref = ref_of(along(way, 1 - hop), half)
            return remote_by(ref, ref, sent.at[key], got.at[key, way, hop - 1, half], on_ring(way, 1))

        return copy

    def gather_start(copy):
        for half in BOTH:
            for way in BOTH:
                copy(way, 1, half).start()

    def gather_hop(copy, hop, half, passed_on=None):
        for way in BOTH:
            if takes(way, hop, half):
                copy(way, hop, half).wait_recv()
                if hop < FAR and takes(way, hop + 1, half):
                    copy(way, hop + 1, half).start()
                if passed_on:
                    passed_on(way, hop, half).start()

    def total(src_of, got_of, sent, got, key):
        def copy(way, dist, half):
            return remote_by(
                src_of(along(way, dist), half), got_of(way, dist, half), sent.at[key], got.at[key, way, dist - 1, half],
                on_ring(way, 1))

        return copy

    def total_start(copy):
        for way in BOTH:
            copy(way, FAR, way).start()
        for way in BOTH:
            copy(way, FAR - 1, 1 - way).start()

    def total_hop(copy, add, dist, way, half):
        copy(way, dist, half).wait_recv()
        add(along(way, dist - 1), way, dist, half)
        if dist > 1:
            copy(way, dist - 1, half).start()

    ring_copies = len(taken())

    def all_sent(ref, sem):
        remote_by(ref, ref, sem, sem, peer).wait_send()

    def block(t, step, half):
        return h_all.at[t, pl.ds(pl.multiple_of(h_rows[step], n.seqs), n.seqs), pl.ds(half * half_d, half_d)]

    ag_copies = [gather(lambda step, half, t=t: block(t, step, half), ag_sent, ag_got, t) for t in BOTH]

    def to_peer(t):
        def copy(way, hop, half):
            ref = block(t, along(way, -hop), half)
            return remote(ref, ref, dd_sem, (t,), peer)

        return copy

    def ag_start(l, t):
        gather_start(ag_copies[t])
        for half in BOTH:
            to_peer(t)(A, A, half).start()

    def ag_hop(t, hop, half):
        gather_hop(ag_copies[t], hop, half, to_peer(t))

    def ag_finish(t):
        blocks = ring_copies // PAIR
        from_peer = h_all.at[t, pl.ds(A, (blocks + 1) * n.seqs), :]
        remote(from_peer, from_peer, dd_sem, (t,), peer).wait()
        all_sent(h_all.at[t, pl.ds(A, blocks * n.seqs), :], ag_sent.at[t])

    stats = pl.ds(n.sub, SUB)
    top_rows = lax.broadcasted_iota(I32, (SUB, LANES), A) < heads_half
    rs_copies = [
        total(lambda step, half, t=t: pd.at[t, chips[step], half], lambda way, d, half, t=t: rd.at[t, way, d - 1, half], rs_sent, rs_got, t)
        for t in BOTH
    ]

    def merge(t):
        def add(step, way, d, half):
            got, mine = rd.at[t, way, d - 1, half], pd.at[t, chips[step], half]
            s1, s2 = got[stats, :], mine[stats, :]
            m = jnp.maximum(s1, s2)
            a1, a2 = jnp.exp(s1 - m), jnp.exp(s2 - m)
            mine[stats, :] = jnp.where(top_rows, m, pltpu.roll(a1, heads_half, A) * s1 + pltpu.roll(a2, heads_half, A) * s2)
            at = pl.ds(A, n.sub)
            by_head = (heads_half, n.head, LANES)
            a1, a2 = (a[:heads_half][:, None] for a in (a1, a2))
            mine[at, :] = (a1 * got[at, :].reshape(by_head) + a2 * mine[at, :].reshape(by_head)).reshape(n.sub, LANES)

        return add

    def select(l, t):
        ag_finish(t)

        def body(i):
            cols = at_block(i, n.s_cols)
            hsel[:, cols] = dot(oh_ref[live, :], h_all[t, :, cols]).astype(BF16)

        loop(n.d_model // n.s_cols, body)

    def turned(w):
        rows = dot(hsel[...], w).astype(BF16).astype(F32)
        return jnp.concatenate([rows, jnp.zeros((LANES - n.slots, rows.shape[B]), F32)], axis=A).T

    units = (PAIR * (1 - c), PAIR * (1 - c) + 1, PAIR * c)
    spread_head = PAIR * c + 1
    first_part = LANES - n.slots

    def packed(u, own, other):
        rest = (other[..., :first_part], other[..., first_part:], own[..., n.slots :])[u]
        if rest.shape[-1] < first_part:
            pad = jnp.zeros((*own.shape[:-1], first_part - rest.shape[-1]), own.dtype)
            rest = jnp.concatenate([rest, pad], axis=-1) if rest.shape[-1] else pad
        return jnp.concatenate([own, rest], axis=-1)

    def query(kvh):
        return turned(wbig[pl.ds(A, n.d_model), at_block(kvh, n.own_rows)])[:, : n.slots]

    def project_first(l, t):
        need("qkv", l)
        other = query(spread_head)
        for u in BOTH:
            q_ref[u] = packed(u, query(units[u]), other)

    def project(l, t):
        own = query(units[PAIR])
        q_ref[PAIR] = packed(PAIR, own, own)
        for i, w in enumerate((wk_v, wv_v)):
            kn_ref[t, i] = turned(w[...])
            knew_ref[l, t, i] = kn_ref[t, i].astype(BF16)
            for u, kvh in enumerate(units):
                own, other = (kn_ref[t, i, at_block(head, n.head), live] for head in (kvh, spread_head))
                kn_p[t, i, at_block(u, n.head), :] = packed(u, own, other)
        release("qkv", l)

    heads = range(n.rep_heads)

    def outputs(t, u):
        return oa.at[t, jnp.where(u < PAIR, 1 - c, c), jnp.where(u < PAIR, u, A)]

    def pages(w, at, u):
        return kv_p[w, at, at_block(u, n.head), :].astype(F32)

    def attend(t, u):
        rows = at_block(u, n.head)
        scale = n.head ** -0.5
        out = outputs(t, u)

        def scores(keys):
            parts = []
            for h in heads:
                prods = q_ref[u, pl.ds(h * n.head, n.head), :][None] * keys
                acc = prods[:, :SUB]
                for d in range(SUB, n.head, SUB):
                    acc = acc + prods[:, d : d + SUB]
                parts.append(acc)
            return sums_to_rows(parts)

        def qk(i):
            at = pl.ds(i * FAR, FAR)
            s_ref[at, :, :] = scores(pages(A, at, u))

        loop(n.page // FAR, qk)
        fresh = range(t + 1)
        news = [scores(kn_p[i, A, rows, :][None])[A] for i in fresh]
        lim, has_new = lane_ref[pl.ds(PAIR * u, 1), :], lane_ref[pl.ds(PAIR * u + 1, 1), :] > 0
        news = [jnp.where(has_new, s * scale, NEG) for s in news]
        valid = lax.broadcasted_iota(I32, (n.page, n.rep_heads, lim.shape[B]), A) < lim[None]
        old = jnp.where(valid, s_ref[:, :, :] * scale, NEG)
        m = jnp.max(old, axis=A)
        for s in news:
            m = jnp.maximum(m, s)
        probs = jnp.where(valid, jnp.exp(old - m[None]), 0.0)
        s_ref[:, :, :] = probs
        news = [jnp.where(has_new, jnp.exp(s - m), 0.0) for s in news]
        count = jnp.sum(probs, axis=A)
        for p in news:
            count = count + p
        out[pl.ds(n.own_rows, SUB), :] = m
        out[pl.ds(n.own_rows + SUB, SUB), :] = count
        vals = [kn_p[i, B, rows, :] for i in fresh]
        for h in heads:
            acc = news[A][h : h + 1] * vals[A]
            for p, v in zip(news[1:], vals[1:], strict=True):
                acc = acc + p[h : h + 1] * v
            out[pl.ds(h * n.head, n.head), :] = acc

    def attend_values(t, u):
        out = outputs(t, u)

        def pv(i):
            vals = [v for v in pages(B, pl.ds(i * FAR, FAR), u)]
            ps = [s_ref[i * FAR + j, :, :] for j in range(FAR)]
            for h in heads:
                at = pl.ds(h * n.head, n.head)
                acc = out[at, :]
                for p, v in zip(ps, vals, strict=True):
                    acc = acc + p[h : h + 1] * v
                out[at, :] = acc

        loop(n.page // FAR, pv)

    def exchange(t):
        return remote(oa.at[t, 1 - c], ob.at[t], x_sem, (t,), peer)

    def attend_all(l, t, between):
        def body(u):
            attend(t, u)
            for at, work in between.items():
                if at % PAIR == A:
                    pl.when(u == at // PAIR)(work)
            attend_values(t, u)
            pl.when(u == B)(lambda: exchange(t).start())
            for at, work in between.items():
                if at % PAIR == B:
                    pl.when(u == at // PAIR)(work)

        loop(len(units), body)
        lane = lax.broadcasted_iota(I32, (1, LANES), B)
        near, far = (pltpu.roll(oa[t, 1 - c, v], first_part * (v + 1), B) for v in BOTH)
        oa[t, c, B] = jnp.where(lane < first_part, near, far)

    low_lanes = lax.broadcasted_iota(I32, (1, LANES), B) < n.pair

    def by_chip(parts, put):
        for zp in range(n.chips // PAIR):
            a, b = (p[:, zp * LANES : (zp + 1) * LANES] for p in parts)
            put(PAIR * zp, jnp.where(low_lanes, a, pltpu.roll(b, n.pair, B)))
            put(PAIR * zp + 1, jnp.where(low_lanes, pltpu.roll(a, n.pair, B), b))

    def both_cores(t, hh, at):
        return jnp.concatenate([oa[t, c, hh, at, :], ob[t, hh, at, :]], axis=B)

    def scatter(l, t):
        exchange(t).wait()
        top, count = (
            jnp.concatenate([both_cores(t, hh, pl.ds(n.own_rows + off, SUB)) for hh in BOTH], axis=A) for off in (A, SUB))
        m_page = [jnp.where(pres_ref[pl.ds(p, 1), :] > 0, exact_dot(top, e_ref[p]), NEG) for p in BOTH]
        m_seq = jnp.maximum(*m_page)
        a = jnp.exp(jnp.minimum(top - exact_dot(m_seq, es_ref[...], right=B), 0.0))
        a_ref[A], a_ref[B] = a[:SUB], a[SUB:]
        l_seq = exact_dot(count * a, es_ref[...])
        dense = {}
        for what, v in enumerate((m_seq, l_seq)):
            by_chip([v[:SUB], v[SUB:]], lambda zz, v, what=what: dense.update({(zz, what): v}))
        for zz in range(n.chips):
            m, l = dense[zz, A], dense[zz, B]
            pd[t, zz, A, stats, :] = jnp.where(top_rows, m, pltpu.roll(l, heads_half, A))
            pd[t, zz, B, stats, :] = jnp.where(top_rows, pltpu.roll(m, heads_half, A), l)

        scatter_half(A, l, t)

    def scatter_half(half, l, t):
        def body(k):
            for j in range(heads_half // PAIR):
                i = k * PAIR + j
                h = half * heads_half + i
                parts = [
                    exact_dot(both_cores(t, hh, at_block(h, n.head)) * a_ref[hh, pl.ds(h, 1), :], es_ref[...]) for hh in BOTH]

                def put(zz, v, i=i):
                    pd[t, zz, half, at_block(i, n.head), :] = v

                by_chip(parts, put)

        loop(PAIR, body)
        for way in BOTH:
            rs_copies[t](way, FAR if way == half else FAR - 1, half).start()

    def f_copy(t, stage):
        return remote(pf.at[t, 1 - c], rf.at[t, stage], f_sem, (t, stage), peer)

    def m_copy(t):
        return remote(hm.at[t, c], hm.at[t, c], m_sem, (t,), peer)

    def product(t, lhs, w, between):
        def body(i):
            cols = at_block(i, n.s_cols)
            val = dot(lhs(), w(cols))
            pf[t, A, :, cols] = val[: n.seqs]
            pf[t, B, :, cols] = val[n.seqs :]
            for at, work in between.items():
                pl.when(i == at)(work)

        loop(n.d_model // n.s_cols, body)

    own = pl.ds(pl.multiple_of(h_rows[A], n.seqs), n.seqs)

    def out_proj(l, t):
        all_sent(pd.at[t, pl.ds(A, ring_copies // PAIR)], rs_sent.at[t])
        for half in BOTH:
            mine = pd.at[t, z, half]
            inv = (1.0 / mine[stats, :])[heads_half:][:, None]
            flat = (mine[pl.ds(A, n.sub), :].reshape(heads_half, n.head, LANES) * inv).reshape(n.sub, LANES).T.astype(BF16)
            for hh in BOTH:
                olhs[:, pl.ds(hh * n.own_rows + half * n.sub, n.sub)] = flat[hh * n.pair : (hh + 1) * n.pair]
        need("o", l)
        product(t, lambda: olhs[...], lambda cols: wo_v[:, cols], {})
        release("o", l)
        f_copy(t, A).start()

    def mid(l, t):
        f_copy(t, A).wait()
        hm[t, c] = (h_all[t, own, :].astype(F32) + (pf[t, c] + rf[t, A])).astype(BF16)
        m_copy(t).start()

    def up(l, t, halfway):
        m_copy(t).wait()
        need("u", l)

        def body(i):
            cols = at_block(i, n.u_cols)
            u = dot(hm[t].reshape(n.pair, n.d_model), wu_v[:, cols]).astype(BF16).astype(F32)
            act[t, :, cols] = jax.nn.gelu(u, approximate=True).astype(BF16)
            for at, work in halfway.items():
                pl.when(i == at)(work)

        loop(n.ff_half // n.u_cols, body)
        release("u", l)

    def down(l, t, between):
        need("d", l)
        product(t, lambda: act[t], lambda cols: wbig[pl.ds(A, n.ff_half), cols], between)
        release("d", l)
        f_copy(t, B).start()

    def new_h(l, t):
        f_copy(t, B).wait()
        new = (hm[t, c].astype(F32) + (pf[t, c] + rf[t, B])).astype(BF16)
        h_all[t, own, :] = new
        y_ref[t] = new

    def ids_of(dev, axis):
        at = lax.broadcasted_iota(I32, (LANES, 1) if axis == A else (1, LANES), axis)
        return jnp.where(at < n.slots, dev * n.slots + at, -1)

    def tables():
        oa[...] = jnp.zeros_like(oa)
        for g, dev in enumerate((me, z * PAIR + 1 - c)):
            ids = ids_of(dev, A)
            target = ids
            for e in range(n.entries):
                target = jnp.where(ids == src_ref[e], dst_ref[e], target)
            stale = mask_rows(ids, dst_ref)
            hit = [jnp.where(tab_ref[pl.ds(p, 1), :] == target, 1.0, 0.0) for p in BOTH]
            now = [jnp.where(stale == 0, h, 0.0) for h in hit]
            at = pl.ds(g * LANES, LANES)
            for p in BOTH:
                e_ref[p, at, :] = now[p].astype(BF16)
            es_ref[at, :] = (now[A] + now[B]).astype(BF16)
            if g == A:
                oh_ref[...] = (hit[A] + hit[B]).astype(BF16)
                held = [h.astype(BF16) for h in (*now, hit[B])]
        for p in BOTH:
            pres_ref[pl.ds(p, 1), :] = jnp.sum(e_ref[p].astype(F32), axis=A, keepdims=True)
        lens = len_ref[...].astype(F32)
        rows = jnp.concatenate([lens, jnp.ones((SUB - 1, lens.shape[B]), F32)], axis=A).astype(BF16)
        first, last, fresh = (dot_by(rows, h, B, B) for h in held)
        at0, at1 = slice(A, 1), slice(B, PAIR)
        limit = jnp.where(first[at1] > 0, jnp.minimum(first[at0], n.page), jnp.where(last[at1] > 0, last[at0] - n.page, 0.0))
        for i, row in enumerate((limit, last[at1])):
            row = row[:, : n.slots]
            for u in range(len(units)):
                lane_ref[pl.ds(PAIR * u + i, 1), :] = packed(u, row, row).astype(I32)
        ids = ids_of(me, B)
        is_src, is_dst = mask_rows(ids, src_ref), mask_rows(ids, dst_ref)
        pick_ref[...] = placed(ids[:, : n.slots], src_ref, n.slots)
        on_last = jnp.where(is_src == 0, fresh[at1], 0.0) > 0
        start = fresh[at0] - n.page
        vec_ref[...] = jnp.where(is_src + is_dst == 0, 1.0, 0.0) * jnp.ones((SUB, LANES), F32)
        for t in BOTH:
            vec_ref[pl.ds(t, 1), :] = jnp.where(on_last, start + t, -1.0)

    m_cols = mf.shape[B] // n.chips // PAIR

    def mig_pair():
        return remote(mg.at[1 - c], mx, gp_sem, (), peer)

    def m_at(step, half):
        return at_block(chips[step] * PAIR + half, m_cols)

    ms_copies, mg_copies = [], []
    for l in range(n.layers):
        ms_copies.append(total(lambda step, half: mg.at[c, :, m_at(step, half)], lambda way, d, half: mr.at[way, d - 1, half], gs_sent, gs_got, l))
        mg_copies.append(gather(lambda step, half: mf.at[:, m_at(step, half)], gg_sent, gg_got, l))

    def mig_add(step, way, d, half):
        at = m_at(step, half)
        mg[c, :, at] = mg[c, :, at] + mr[way, d - 1, half]

    m_ring = pl.ds(A, ring_copies * m_cols)

    def mig_sent(l):
        all_sent(mg.at[c, :, m_ring], gs_sent.at[l])

    def mig_out_copies(l):
        return remote(mf, mig_out.at[l, c], go_sem, (l,), peer), pltpu.make_async_copy(mf, mig_out.at[l, c], go_sem.at[PAIR, l])

    def page_loads(l, i, slot):
        at = pl.ds(pl.multiple_of(i * SUB, SUB), SUB)
        return [pltpu.make_async_copy(pool.at[l, at], raw.at[slot, w], p_sem.at[slot, w]) for w, pool in enumerate((kp, vp))]

    def first_pages(l):
        for i in range(raw.shape[A]):
            for copy in page_loads(l, i, i):
                copy.start()

    def extract(l):
        if l > 0:
            mig_sent(l - 1)
        chunks, held = n.page // SUB, raw.shape[A]

        def body(i):
            slot = lax.rem(i, held)
            for copy in page_loads(l, i, slot):
                copy.wait()
            at = pl.ds(pl.multiple_of(i * SUB, SUB), SUB)
            for w in BOTH:
                rows = raw[slot, w].reshape(SUB * n.kv_cols, n.slots)
                mg[w, :, at_block(i, SUB * n.kv_cols)] = dot_by(pick_ref[...], rows, B, B).astype(BF16)
                other = raw[slot, w, :, at_block(spread_head, n.head), :]
                for u, kvh in enumerate(units):
                    kv_p[w, at, at_block(u, n.head), :] = packed(u, raw[slot, w, :, at_block(kvh, n.head), :], other)

            @pl.when(i + held < chunks)
            def _():
                for copy in page_loads(l, i + held, slot):
                    copy.start()

        loop(chunks, body)
        if l + 1 < n.layers:
            first_pages(l + 1)
        mig_pair().start()

    def mig_start(l):
        if l > 0:
            for copy in mig_out_copies(l - 1):
                copy.wait()
        mig_pair().wait()
        mg[c] = mg[c] + mx[...]
        total_start(ms_copies[l])

    def mig_gather(l):
        gather_start(mg_copies[l])

    def mig_own():
        for half in BOTH:
            mf[:, m_at(A, half)] = mg[c, :, m_at(A, half)]

    def mig_end(l):
        all_sent(mf.at[:, m_ring], gg_sent.at[l])
        for copy in mig_out_copies(l):
            copy.start()

    steps = {"TAB": tables}
    for l in range(n.layers):
        steps[f"EXT{l}"] = functools.partial(extract, l)
        steps[f"MS{l}s"] = functools.partial(mig_start, l)
        steps[f"MG{l}s"] = functools.partial(mig_gather, l)
        for hop in HOPS:
            for half in BOTH:
                steps[f"MG{l}h{hop}{half}"] = functools.partial(gather_hop, mg_copies[l], hop, half)
                for way in BOTH:
                    steps[f"MS{l}k{hop}{way}{half}"] = functools.partial(total_hop, ms_copies[l], mig_add, hop, way, half)
        for t in BOTH:
            for name, work in (
                ("SEL", select), ("PROA", project_first), ("PROJ", project), ("SCAT", scatter), ("SCAU", functools.partial(scatter_half, B)), ("FO", out_proj), ("MID", mid), ("NEWH", new_h),
            ):
                steps[f"{name}{l}{t}"] = functools.partial(work, l, t)
            steps[f"AG{l}{t}s"] = functools.partial(ag_start, l, t)
            for hop in HOPS:
                for half in BOTH:
                    steps[f"AG{l}{t}h{hop}{half}"] = functools.partial(ag_hop, t, hop, half)
                    for way in BOTH:
                        steps[f"RS{l}{t}k{hop}{way}{half}"] = functools.partial(total_hop, rs_copies[t], merge(t), hop, way, half)

    for t in BOTH:
        h_all[t, own, :] = x_ref[t]
    first_pages(A)
    load("q", A).start()
    barrier = pltpu.get_barrier_semaphore()
    others = (peer, *rings.values())
    for target in others:
        pl.semaphore_signal(barrier, inc=1, device_id=target, device_id_type=MESH)
    pl.semaphore_wait(barrier, len(others))

    def later_loads():
        for name in ("k", "v", "o", "u"):
            load(name, A).start()


    steps["LOADS"] = later_loads
    todo = list(ORDER)
    todo.insert(PAIR, "LOADS")
    on_way = {kind: len([name for name in todo if name.startswith(kind)]) for l in range(n.layers) for kind in (f"MS{l}k", f"MG{l}h")}

    def run(names):
        for name in names:
            steps[name]()
            kind = name[:FAR]
            if kind in on_way:
                on_way[kind] -= 1
                if on_way[kind] == 0:
                    mig_end(int(kind[PAIR])) if "h" in kind else mig_own()

    loops = {"ATT": (attend_all, PAIR * len(units)), "UP": (up, n.ff_half // n.u_cols), "DOW": (down, n.d_model // n.s_cols)}
    while todo:
        name = todo.pop(A)
        word = name.rstrip("0123456789")
        if word in loops:
            work, count = loops[word]
            l, t, _ = (int(ch) for ch in name[len(word) :])
            between = {}
            for i in range(count - 1):
                upto = todo.index(f"{word}{l}{t}{i + 1}")
                if upto:
                    between[i] = functools.partial(run, todo[:upto])
                todo = todo[upto + 1 :]
            work(l, t, between)
        else:
            run([name])
    for copy in mig_out_copies(n.layers - 1):
        copy.wait()
    mig_sent(n.layers - 1)


def pool_kernel(dst_ref, vec_ref, mig_ref, new_ref, y_ref, k_ref, v_ref, ko_ref, vo_ref, yo_ref, moved, move_ref):
    step, rows, slots = k_ref.shape[1:]
    live = slice(A, slots)
    group = moved.shape[1] // rows
    tab = vec_ref[...]
    at0, at1, keep = (tab[i : i + 1, live].astype(BF16) for i in range(PAIR + 1))
    keep = keep > 0
    base = pl.program_id(B) * step
    turns = [(which, g) for which in BOTH for g in range(step // group)]

    @pl.when((pl.program_id(A) == 0) & (pl.program_id(B) == 0))
    def _():
        yo_ref[...] = y_ref[...]
        ids = lax.axis_index("kv") * slots + lax.broadcasted_iota(I32, (1, slots), B)
        move_ref[...] = placed(ids, dst_ref, slots)

    def move(which, g, slot):
        moved[slot] = dot_by(mig_ref[A, which, :, g * group * rows : (g + 1) * group * rows], move_ref[...], A, A).astype(BF16)

    move(A, A, A)
    for i, (which, g) in enumerate(turns):
        if i + 1 < len(turns):
            move(*turns[i + 1], (i + 1) % PAIR)
        pool_ref, out_ref = ((k_ref, ko_ref), (v_ref, vo_ref))[which]
        for j in range(group):
            r = g * group + j
            pos = jnp.full((1, slots), (base + r).astype(F32), F32).astype(BF16)
            val = jnp.where(keep, pool_ref[A, r], moved[i % PAIR, j * rows : (j + 1) * rows, :])
            val = jnp.where(at0 == pos, new_ref[A, A, which, :, live], val)
            out_ref[A, r] = jnp.where(at1 == pos, new_ref[A, B, which, :, live], val)


def new_pools(pools, mig, knew, vec, dst, y):
    layers, page, rows, slots = pools[A].shape
    step, group = page // PAIR, FAR
    entries = mig.shape[PAIR]
    block = pl.BlockSpec((1, step, rows, slots), lambda l, i: (l, i, A, A))
    whole = pl.BlockSpec(y.shape, lambda l, i: (A, A, A))
    return pl.pallas_call(
        pool_kernel,
        out_shape=[jax.ShapeDtypeStruct(pools[A].shape, BF16)] * PAIR + [jax.ShapeDtypeStruct(y.shape, BF16)],
        grid=(layers, page // step),
        in_specs=[
            pl.BlockSpec(memory_space=pltpu.SMEM),
            pl.BlockSpec(vec.shape, lambda l, i: (A, A)),
            pl.BlockSpec((1, PAIR, entries, step * rows), lambda l, i: (l, A, A, i)),
            pl.BlockSpec((1, PAIR, PAIR, rows, LANES), lambda l, i: (l, A, A, A, A)),
            whole, block, block,
        ],
        out_specs=[block, block, whole],
        scratch_shapes=[pltpu.VMEM((PAIR, group * rows, slots), BF16), pltpu.VMEM((entries, slots), BF16)],
        compiler_params=pltpu.CompilerParams(dimension_semantics=("arbitrary",) * PAIR, vmem_limit_bytes=VMEM_BYTES),
        name="new_pools",
    )(dst, vec, mig, knew, y, *pools)


def solution(mesh):
    devs = mesh.shape["kv"]
    pool_spec = P(("rep", "kv"))
    tok_spec = P(None, ("rep", "kv"), None)

    def device_fn(embeds, w_query, w_key, w_value, w_out, w_up, w_down, k_pool, v_pool, new_table, seq_lens, mig_src, mig_dst):
        slots, layers, page, kv_heads, head = k_pool.shape
        seqs, d_model = embeds.shape[1:]
        rep_heads = w_query.shape[-1] // head // kv_heads
        own_rows = rep_heads * head
        n = SimpleNamespace(
            layers=layers, d_model=d_model, ff_half=w_up.shape[-1] // PAIR, chips=devs // PAIR, seqs=seqs, pair=PAIR * seqs,
            slots=slots, kv_heads=kv_heads, head=head, page=page, rep_heads=rep_heads, own_rows=own_rows, sub=own_rows // PAIR,
            wide=kv_heads // PAIR * own_rows, kv_cols=kv_heads * head, entries=mig_src.shape[A],
            s_cols=d_model // PAIR, d_cols=d_model // FAR, u_cols=w_up.shape[-1] // FAR)
        total = seqs * devs
        pages = page * n.kv_cols
        pools = [jnp.moveaxis(p, A, -1).reshape(layers, page, n.kv_cols, slots) for p in (k_pool, v_pool)]
        dma, two = pltpu.SemaphoreType.DMA, PAIR
        ring = (two, FAR, two)
        bf = lambda *shape: pltpu.VMEM(shape, BF16)
        f32 = lambda *shape: pltpu.VMEM(shape, F32)
        hbm, vmem, smem = (pl.BlockSpec(memory_space=m) for m in (pl.ANY, pltpu.VMEM, pltpu.SMEM))
        y, knew, vec, mig = pl.pallas_call(
            functools.partial(main_kernel, n),
            out_shape=[
                jax.ShapeDtypeStruct((two, seqs, d_model), BF16),
                jax.ShapeDtypeStruct((layers, two, two, n.kv_cols, LANES), BF16),
                jax.ShapeDtypeStruct((SUB, LANES), F32),
                jax.ShapeDtypeStruct((layers, two, n.entries, pages), BF16),
            ],
            in_specs=[smem] * two + [vmem] * (two + 1) + [hbm] * SUB,
            out_specs=[vmem] * (two + 1) + [hbm],
            scratch_shapes=[
                bf(LANES, total), bf(two, two * LANES, total), bf(two * LANES, total), f32(SUB, total), pltpu.VMEM((SUB, LANES), I32),
                bf(n.entries, slots), bf(two, n.entries, pages), bf(n.entries, pages),
                bf(two, FAR, two, n.entries, pages // devs), bf(n.entries, pages),
                bf(two, total, d_model), bf(slots, d_model), bf(max(d_model, n.ff_half), d_model), bf(d_model, n.kv_cols),
                bf(d_model, n.kv_cols), bf(n.wide, d_model), bf(d_model, n.ff_half), bf(two + 1, two, SUB, n.kv_cols, slots), bf(two, page, (kv_heads - 1) * head, LANES),
                f32(kv_heads - 1, own_rows, LANES), f32(two, two, n.kv_cols, LANES), f32(two, two, (kv_heads - 1) * head, LANES), f32(page, rep_heads, LANES),
                f32(two, two, two, own_rows + two * SUB, LANES), f32(two, two, own_rows + two * SUB, LANES),
                f32(two, rep_heads, two * LANES), f32(two, n.chips, two, n.sub + SUB, LANES),
                f32(two, two, FAR, two, n.sub + SUB, LANES), bf(n.pair, n.wide), f32(two, two, seqs, d_model),
                f32(two, two, seqs, d_model), bf(two, two, seqs, d_model), bf(two, n.pair, n.ff_half),
                dma((two,)), dma((two, *ring)), dma((two, two)), dma((two,)), dma((two, *ring)), dma((two, two)),
                dma((two, two, two)), dma((two, two)), dma((layers,)), dma((layers, *ring)), dma((layers,)), dma((layers, *ring)),
                dma((two,)), dma((two + 1, layers)), dma((two + 1, two)), dma((SUB,)),
            ],
            compiler_params=pltpu.CompilerParams(collective_id=A, has_side_effects=True, vmem_limit_bytes=VMEM_BYTES),
            name="decode",
        )(mig_src, mig_dst, new_table.T, seq_lens[None], embeds, w_query, w_key, w_value, w_out, w_up, w_down, *pools)
        *outs, y = new_pools(pools, mig, knew, vec, mig_dst, y)
        outs = [jnp.moveaxis(p.reshape(layers, page, kv_heads, head, slots), -1, A) for p in outs]
        return y, *outs

    return jax.shard_map(
        device_fn, mesh=mesh,
        in_specs=(tok_spec, *(P(),) * (SUB - PAIR), pool_spec, pool_spec, P("rep", None), *(P("rep"),) * (FAR - 1)),
        out_specs=(tok_spec, pool_spec, pool_spec), check_vma=False)
```
